512 devices in a mesh: obs: 16 (over x, y), patch: 32 (over z, core).
Axes of the slice: x: 4, y: 4, z: 16, core: 2. Of those that a mesh axis runs over, the one named last changes fastest.
Arguments:
- green: float32 [20480, 20480], P('obs', 'patch'), may hold values from -0.0390625 to 0.0390625
- data: float32 [20480, 128], P('obs'), may hold values from -6 to 6
- neighbours: int32 [3, 20480], P(None, 'patch'), may hold values from 0 to 20479, as said below
- reg_weight: float32 [128], replicated, may hold values from 0.5 to 2
Outputs:
- slip: float32 [20480, 128], P('patch')
The draws below stay inside these ranges and needn't reach their ends.
Inputs may be any that keep to these rules, and one draw needn't show every extreme that they name: `neighbours`: entry (k, i) is a patch within 128 of i; an entry equal to i is padding. Distance 128 is reached in every draw.
All inputs are finite; a program needn't handle non-finite values.
Results may differ from the reference program's by a relative error of at most 0.0001.
Values sent between devices are 32-bit elements; how exact they have to be, the bound alone decides.
A program may use at most 64 MiB of HBM per device.

```python
import math
import jax
import jax.numpy as jnp
from jax import lax

EPOCHS = 128
BAND = 128
ITERS = 3
OBS = 20480
NPATCH = 20480


def draw_neighbours(key, part):
    key_offsets = jax.random.fold_in(key, 11)
    key_padding = jax.random.fold_in(key, 12)
    offsets = jax.random.randint(key_offsets, (3, NPATCH), -BAND, BAND + 1)
    padding = jax.random.randint(key_padding, (3, NPATCH), 0, 4) == 0
    offsets = jnp.where(padding, 0, offsets)
    indices = jnp.arange(NPATCH, dtype=jnp.int32)
    marked = indices % 37 == 5
    offsets = offsets.at[0].set(jnp.where(marked, -BAND, offsets[0]))
    offsets = offsets.at[1].set(jnp.where(marked, BAND, offsets[1]))
    return jnp.clip(indices[None, :] + offsets, 0, NPATCH - 1).astype(jnp.int32)


def level_of(key, extent, split, least, largest):
    level = 1.0
    for position, parts in split:
        draws = jax.random.uniform(jax.random.fold_in(jax.random.fold_in(key, 6), position), (parts,), jnp.float32, least / len(split), largest / len(split))
        level = level * jnp.repeat(jnp.exp(draws), extent[position] // parts).reshape((-1,) + (1,) * (len(extent) - 1 - position))
    return level


def gaussian(stream_key, dims, spread, most, shards=(), kind=jnp.bfloat16):
    loudness = level_of(stream_key, dims, shards, -0.22, 0.18) if shards else 1.0
    array = jax.random.normal(stream_key, dims, jnp.float32) * spread * loudness
    return jnp.minimum(jnp.maximum(array, -most), most).astype(kind)


def setup_inputs(seed: int = 0) -> dict:
    seeds = jax.random.split(jax.random.key(seed), 5)
    green = gaussian(seeds[0], (OBS, NPATCH), NPATCH ** -0.5, 0.0390625, ((0, 16), (1, 32)), jnp.float32)
    data = gaussian(seeds[1], (OBS, EPOCHS), 1.0, 6.0, ((0, 16),), jnp.float32)
    neighbours = draw_neighbours(jax.random.fold_in(seeds[4], 71), 0)
    reg_weight = jnp.clip(jnp.exp(jax.random.uniform(seeds[3], (EPOCHS,), jnp.float32, math.log(0.5), math.log(2.0))), 0.5, 2.0)
    return {"green": green, "data": data, "neighbours": neighbours, "reg_weight": reg_weight}


def laplace(field, neighbours):
    return 4.0 * field - field[neighbours[0]] - field[neighbours[1]] - field[neighbours[2]]


def laplace_t(values, neighbours):
    result = 4.0 * values
    for slot in range(3):
        result = result.at[neighbours[slot]].add(-values)
    return result


def transposed(green, residual):
    return lax.dot_general(green, residual, (((0,), (0,)), ((), ())), precision=lax.Precision.HIGHEST, preferred_element_type=jnp.float32)


def reference(green, data, neighbours, reg_weight):
    slip = jnp.zeros((NPATCH, EPOCHS), jnp.float32)
    residual = data
    reg_resid = jnp.zeros((NPATCH, EPOCHS), jnp.float32)
    gradient = transposed(green, data)
    grad_norm = jnp.sum(gradient * gradient, axis=0)
    direction = gradient
    for iteration in range(ITERS):
        image = jnp.dot(green, direction, precision=lax.Precision.HIGHEST, preferred_element_type=jnp.float32)
        reg_image = reg_weight * laplace(direction, neighbours)
        curvature = jnp.sum(image * image, axis=0) + jnp.sum(reg_image * reg_image, axis=0)
        step_size = grad_norm / curvature
        slip = slip + step_size * direction
        if iteration + 1 < ITERS:
            residual = residual - step_size * image
            reg_resid = reg_resid - step_size * reg_image
            gradient = transposed(green, residual) + reg_weight * laplace_t(reg_resid, neighbours)
            next_norm = jnp.sum(gradient * gradient, axis=0)
            direction = gradient + (next_norm / grad_norm) * direction
            grad_norm = next_norm
    return slip
```

```python
import functools
import math

import jax
import jax.numpy as jnp
from jax import lax
from jax.experimental import pallas as pl
from jax.experimental.pallas import tpu as pltpu
from jax.sharding import PartitionSpec as P

BAND = 128
ITERS = 3
MESH = pl.DeviceIdType.MESH
F32 = jnp.float32
BF16 = jnp.bfloat16


def dot(a, b):
    return lax.dot_general(a, b, (((1,), (0,)), ((), ())), preferred_element_type=F32)


def split(x):
    hi = x.astype(BF16)
    return hi, (x - hi.astype(F32)).astype(BF16)


def kernel(n_obs, n_patch, green, data, nb, rw, out,
           ghi, glo, gthi, gtlo, lm, lmt, cat_d, cat_r, cat_e,
           d, g, a, wext, slip, hd, hg, qd, qg,
           pf, s, rd, zr, zrel, zfin, img, bs, br, ag, hal, wr, scs, scr, pls, plr, qls, qlr,
           sem_d, sem_z, sem_f, sem_g, sem_i, sem_b, sem_a, sem_h, sem_w, sem_s, sem_p, sem_q):
    rows, cols = green.shape
    E = data.shape[1]
    nz = n_patch // 2
    R = rows // 2 // nz
    BR = cols // n_obs
    half = rows // 2
    per = 4
    nch = n_obs // per
    nd = rd.shape[1]
    PD = nz // nd
    CB = cols // BAND
    Q = nz // 4
    plus = list(range(1, Q + 1))
    minus = list(range(1, Q))
    obs = lax.axis_index("obs")
    pat = lax.axis_index("patch")
    z = pat // 2
    c = pat % 2
    other = 1 - c
    partner = z * 2 + other
    has_l, has_r = pat > 0, pat < n_patch - 1
    weight = rw[...]

    def at(o, q):
        return (o, q)

    def rcopy(src, dst, sems, dev):
        return pltpu.make_async_remote_copy(
            src_ref=src, dst_ref=dst, send_sem=sems[0], recv_sem=sems[1],
            device_id=dev, device_id_type=MESH)

    def pair(sem, *idx):
        return sem.at[(0,) + idx], sem.at[(1,) + idx]

    barrier = pltpu.get_barrier_semaphore()

    @pl.loop(1, n_patch)
    def _(i):
        pl.semaphore_signal(barrier, inc=1, device_id=at(obs, (pat + i) % n_patch), device_id_type=MESH)

    @pl.loop(1, n_obs)
    def _(i):
        pl.semaphore_signal(barrier, inc=1, device_id=at((obs + i) % n_obs, pat), device_id_type=MESH)

    nblk = rows // BAND

    @pl.loop(0, nblk)
    def _(i):
        r0 = pl.multiple_of(i * BAND, BAND)
        block = green[pl.ds(r0, BAND), :]
        hi, lo = split(block)
        ghi[pl.ds(r0, BAND), :] = hi
        glo[pl.ds(r0, BAND), :] = lo
        hi, lo = split(block.T)
        gthi[:, pl.ds(r0, BAND)] = hi
        gtlo[:, pl.ds(r0, BAND)] = lo
        hi, lo = split(data[pl.ds(r0, BAND), :])
        cat_r[pl.ds(r0, BAND), 0:E] = hi
        cat_r[pl.ds(r0, BAND), E:2 * E] = lo

    scs[...] = jnp.zeros((ITERS, 8, E), F32)
    zero_h = jnp.zeros((BAND, E), F32)

    @pl.when(pat == 0)
    def _():
        for it in range(ITERS):
            hal[it, 0] = zero_h
        for it in range(ITERS - 1):
            wr[it, 0] = zero_h

    @pl.when(pat == n_patch - 1)
    def _():
        for it in range(ITERS):
            hal[it, 1] = zero_h
        for it in range(ITERS - 1):
            wr[it, 1] = zero_h

    def build_laplace():
        @pl.loop(0, CB + 2)
        def _(j):
            r0 = pl.multiple_of(j * BAND, BAND)
            col = lax.broadcasted_iota(jnp.int32, (BAND, cols), 0) + j * BAND
            own = lax.broadcasted_iota(jnp.int32, (BAND, cols), 1) + BAND
            m = jnp.where(col == own, 4.0, 0.0)
            col = col + (pat * cols - BAND)
            for k in range(3):
                m = m - jnp.where(col == nb[k:k + 1, :], 1.0, 0.0)
            lmt[pl.ds(r0, BAND), :] = m.astype(BF16)
            lm[:, pl.ds(r0, BAND)] = m.T.astype(BF16)

    pl.semaphore_wait(barrier, n_patch - 1 + n_obs - 1)

    def bcopy(b, o, slot):
        return rcopy(bs.at[b, o], br.at[b, slot], (sem_b.at[0, b, o], sem_b.at[1, b, slot]), at(o, pat))

    def acopy(b, o, slot):
        r0 = pl.multiple_of(slot * BR, BR)
        return rcopy(ag.at[b, pl.ds(r0, BR)], ag.at[b, pl.ds(r0, BR)],
                     (sem_a.at[0, b, o], sem_a.at[1, b, slot]), at(o, pat))

    def backward(b, hook):
        @pl.loop(1, nch + 1)
        def _(j):
            ch = (obs // per + j) % nch
            r0 = pl.multiple_of(ch * (per * BR), per * BR)
            y = dot(gthi[pl.ds(r0, per * BR), :], cat_r[...])
            y = y[:, :E] + y[:, E:] + dot(gtlo[pl.ds(r0, per * BR), :], cat_r[:, 0:E])
            bs[b, pl.ds(ch * per, per)] = y.reshape(per, BR, E)
            for i in range(per):
                o = ch * per + i

                @pl.when(o != obs)
                def _():
                    bcopy(b, o, obs).start()

        hook()

        def add(i, acc):
            o = (obs + i) % n_obs
            bcopy(b, o, o).wait_recv()
            return acc + br[b, o]

        total = lax.fori_loop(1, n_obs, add, bs[b, obs])
        ag[b, pl.ds(pl.multiple_of(obs * BR, BR), BR), :] = total

        @pl.loop(1, n_obs)
        def _(i):
            acopy(b, (obs + i) % n_obs, obs).start()

        @pl.loop(1, n_obs)
        def _(i):
            o = (obs + i) % n_obs
            acopy(b, o, o).wait_recv()

    def backward_end(b):
        @pl.loop(1, n_obs)
        def _(i):
            o = (obs + i) % n_obs
            bcopy(b, o, obs).wait_send()
            acopy(b, o, obs).wait_send()

    def dcopy(it, k):
        return rcopy(pf.at[pl.ds(k * PD, PD)], rd.at[it, k], pair(sem_d, it, k), at(obs, partner))

    def zat(k):
        return at(obs, ((z + k + nz) % nz) * 2 + c)

    def owner(k):
        return (z + k + 2 * nz) % nz

    first_step = ([(-k, -k - Q) for k in reversed(plus)] + [(k, k + Q) for k in reversed(minus)]
                  + [(-k, -k) for k in reversed(minus)] + [(k, k) for k in reversed(minus)])
    n_plus, n_minus = len(plus), len(minus)

    def zcopy(it, slot):
        k, o = first_step[slot]
        return rcopy(s.at[owner(o)], zr.at[it, slot], pair(sem_z, it, slot), zat(k))

    def fcopy(it, slot):
        return rcopy(zrel.at[slot], zfin.at[it, slot], pair(sem_f, it, slot), zat(-Q if slot == 0 else Q))

    near = [(k, 0) for k in (-Q, Q) ] + [(sgn * k, 0) for k in reversed(minus) for sgn in (1, -1)]
    relay_p = [(k, -Q) for k in reversed(plus)]
    relay_m = [(-k, Q) for k in reversed(minus)]
    gather = near + relay_p + relay_m

    def gcopy(it, m):
        k, o = gather[m]
        p = owner(o)
        return rcopy(img.at[it, c, p], img.at[it, c, p], (sem_g.at[0, it, m], sem_g.at[1, it, p]), zat(k))

    def gwait(it, p):
        rcopy(img.at[it, c, p], img.at[it, c, p], (sem_g.at[0, it, 0], sem_g.at[1, it, p]), zat(1)).wait_recv()

    def icopy(it, k):
        return rcopy(img.at[it, c, k], img.at[it, c, k], pair(sem_i, it, k), at(obs, partner))

    def fold(acc, it, slots):
        for slot in slots:
            zcopy(it, slot).wait_recv()
            acc = acc + zr[it, slot]
        return acc

    def hsrc(it):
        return a if it else ag.at[0]

    def hcopy_r(it):
        return rcopy(hsrc(it).at[pl.ds(cols - BAND, BAND)], hal.at[it, 0], pair(sem_h, it, 0), at(obs, pat + 1))

    def hcopy_l(it):
        return rcopy(hsrc(it).at[pl.ds(0, BAND)], hal.at[it, 1], pair(sem_h, it, 1), at(obs, pat - 1))

    def forward(it, sums, hook):
        last = it == ITERS - 1

        hi, lo = split(hsrc(it)[...])
        cat_d[:, 0:E] = hi
        cat_d[:, E:2 * E] = lo

        def part(h):
            r0 = pl.multiple_of(h * half, half)
            y = dot(ghi[pl.ds(r0, half), :], cat_d[...])
            y = y[:, :E] + y[:, E:] + dot(glo[pl.ds(r0, half), :], cat_d[:, 0:E])
            return y.reshape(nz, R, E)

        pf[...] = part(other)

        for k in range(nd):
            dcopy(it, k).start()

        @pl.when(has_r)
        def _():
            hcopy_r(it).start()

        @pl.when(has_l)
        def _():
            hcopy_l(it).start()

        s[...] = part(c)
        sums()

        for k in range(nd):
            dcopy(it, k).wait_recv()
            s[k * PD:(k + 1) * PD] += rd[it, k]

        for slot in range(len(first_step)):
            zcopy(it, slot).start()

        zrel[0] = fold(s[owner(-Q)], it, range(n_plus))
        fcopy(it, 0).start()
        zrel[1] = fold(s[owner(Q)], it, range(n_plus, n_plus + n_minus))
        fcopy(it, 1).start()

        scalars = hook()

        total = fold(s[z], it, range(n_plus + n_minus, len(first_step)))
        for slot in range(2):
            fcopy(it, slot).wait_recv()
            total = total + zfin[it, slot]

        if it:
            step, ratio = scalars
            rest = qg[...] - step * total
            total = rest + ratio * qd[...]
        else:
            rest = total
        if last:
            sq = jnp.sum((total * total).reshape(R // 8, 8, E), axis=0)
        else:
            sq = None
            qg[...] = rest
            qd[...] = total
            img[it, c, z] = total
            for m in range(len(near)):
                gcopy(it, m).start()
            icopy(it, z).start()
            gwait(it, owner(-Q))
            for m in range(len(near), len(near) + len(relay_p)):
                gcopy(it, m).start()
            gwait(it, owner(Q))
            for m in range(len(near) + len(relay_p), len(gather)):
                gcopy(it, m).start()
            icopy(it, owner(-Q)).start()
            icopy(it, owner(Q)).start()
            seen = {0, nz - Q, Q}
            for k in minus:
                for o in (-k, k):
                    gwait(it, owner(o))
                    icopy(it, owner(o)).start()
                    seen.add(o % nz)
            for o in range(nz):
                if o not in seen:
                    gwait(it, owner(o))
                    icopy(it, owner(o)).start()
            for o in range(nz):
                icopy(it, owner(o)).wait_recv()
            hi, lo = split(img[it].reshape(rows, E))
            cat_r[:, 0:E] = hi
            cat_r[:, E:2 * E] = lo

        return sq

    def forward_end(it):
        for k in range(nd):
            dcopy(it, k).wait_send()
        for slot in range(len(first_step)):
            zcopy(it, slot).wait_send()
        for slot in range(2):
            fcopy(it, slot).wait_send()
        if it < ITERS - 1:
            for m in range(len(gather)):
                gcopy(it, m).wait_send()

            @pl.loop(0, nz)
            def _(k):
                icopy(it, k).wait_send()

    def halo_wait(it):
        @pl.when(has_l)
        def _():
            hcopy_r(it).wait_recv()

        @pl.when(has_r)
        def _():
            hcopy_l(it).wait_recv()

        @pl.when(has_r)
        def _():
            hcopy_r(it).wait_send()

        @pl.when(has_l)
        def _():
            hcopy_l(it).wait_send()

    def laplace():
        for r0, n, v in ((0, BAND, hd[0]), (BAND, cols, d[...]), (BAND + cols, BAND, hd[1])):
            hi, lo = split(v)
            cat_e[r0:r0 + n, 0:E] = hi
            cat_e[r0:r0 + n, E:2 * E] = lo

    def lap_rows(i):
        r0 = pl.multiple_of(i * BAND, BAND)
        y = dot(lm[pl.ds(r0, BAND), :], cat_e[...])
        return r0, weight * (y[:, :E] + y[:, E:])

    def wcopy_l(it):
        return rcopy(wext.at[pl.ds(0, BAND)], wr.at[it, 1], pair(sem_w, it, 1), at(obs, pat - 1))

    def wcopy_r(it):
        return rcopy(wext.at[pl.ds(BAND + cols, BAND)], wr.at[it, 0], pair(sem_w, it, 0), at(obs, pat + 1))

    def reg_start(it):
        laplace()

        @pl.loop(0, CB)
        def _(i):
            r0, u = lap_rows(i)
            hi, lo = split(u)
            cat_d[pl.ds(r0, BAND), 0:E] = hi
            cat_d[pl.ds(r0, BAND), E:2 * E] = lo

        @pl.loop(0, CB + 2)
        def _(i):
            r0 = pl.multiple_of(i * BAND, BAND)
            y = dot(lmt[pl.ds(r0, BAND), :], cat_d[...])
            wext[pl.ds(r0, BAND), :] = weight * (y[:, :E] + y[:, E:])

        @pl.when(has_l)
        def _():
            wcopy_l(it).start()

        @pl.when(has_r)
        def _():
            wcopy_r(it).start()

    def reg_end(it):
        a[...] = ag[it + 1] + wext[BAND:BAND + cols, :]

        @pl.when(has_l)
        def _():
            wcopy_r(it).wait_recv()

        @pl.when(has_r)
        def _():
            wcopy_l(it).wait_recv()

        a[0:BAND, :] += wr[it, 0]
        a[cols - BAND:cols, :] += wr[it, 1]

    def reg_done(it):
        @pl.when(has_l)
        def _():
            wcopy_l(it).wait_send()

        @pl.when(has_r)
        def _():
            wcopy_r(it).wait_send()

    def scopy(it, slot, q):
        return rcopy(scs.at[it], scr.at[it, slot], (sem_s.at[0, it, q], sem_s.at[1, it, slot]), at(obs, q))

    def sums_start(it):
        scr[it, pat] = scs[it]

        @pl.loop(1, n_patch)
        def _(i):
            scopy(it, pat, (pat + i) % n_patch).start()

    def sums_end(it):
        @pl.loop(1, n_patch)
        def _(i):
            q = (pat + i) % n_patch
            scopy(it, q, q).wait_recv()

        @pl.loop(1, n_patch)
        def _(i):
            q = (pat + i) % n_patch
            scopy(it, pat, q).wait_send()

        return jnp.sum(scr[it], axis=0)

    def pcopy(q, slot):
        return rcopy(pls, plr.at[slot], (sem_p.at[0, q], sem_p.at[1, slot]), at(obs, q))

    def qcopy(o, slot):
        return rcopy(qls, qlr.at[slot], (sem_q.at[0, o], sem_q.at[1, slot]), at(o, pat))

    def rowsum(x):
        return jnp.sum(x, axis=0, keepdims=True)

    norms = []

    def dots(it):
        gv, dv, av = g[...], d[...], a[...]
        scs[it, 0:1, :] = rowsum(gv * gv)
        scs[it, 1:2, :] = rowsum(dv * av)
        scs[it, 2:3, :] = rowsum(gv * av)
        scs[it, 3:4, :] = rowsum(av * av)
        sums_start(it)

    def first():
        halo_wait(0)
        hg[...] = hal[0]
        hd[...] = hal[0]

    def advance(it):
        tot = sums_end(it - 1)
        if it == 1:
            norms.append(tot[0:1])
        norm = norms[-1]
        step = norm / tot[1:2]
        after = norm - 2.0 * step * tot[2:3] + step * step * tot[3:4]
        ratio = after / norm
        norms.append(after)
        halo_wait(it)
        if it == 1:
            slip[...] = step * d[...]
        else:
            slip[...] += step * d[...]
        g[...] = g[...] - step * a[...]
        d[...] = g[...] + ratio * d[...]
        hg[...] = hg[...] - step * hal[it]
        hd[...] = hg[...] + ratio * hd[...]
        if it == ITERS - 1:
            laplace()

            @pl.loop(0, CB)
            def _(i):
                _, u = lap_rows(i)
                scs[it] += jnp.sum((u * u).reshape(BAND // 8, 8, E), axis=0)

            sums_start(it)
        return step, ratio

    backward(0, build_laplace)
    g[...] = ag[0]
    d[...] = ag[0]
    forward(0, lambda: None, first)
    for it in range(1, ITERS):
        backward(it, functools.partial(reg_start, it - 1))
        forward_end(it - 1)
        reg_end(it - 1)
        sq = forward(it, functools.partial(dots, it - 1), functools.partial(advance, it))
        reg_done(it - 1)
    last = ITERS - 1
    norm = norms[-1]
    pls[...] = sq
    plr[pat] = sq

    @pl.loop(1, n_patch)
    def _(i):
        pcopy((pat + i) % n_patch, pat).start()

    reg = rowsum(sums_end(last))
    forward_end(last)
    for it in range(ITERS):
        backward_end(it)

    @pl.loop(1, n_patch)
    def _(i):
        q = (pat + i) % n_patch
        pcopy(q, q).wait_recv()

    part = jnp.sum(plr[...], axis=0)
    qls[...] = part
    qlr[obs] = part

    @pl.loop(1, n_obs)
    def _(i):
        qcopy((obs + i) % n_obs, obs).start()

    @pl.loop(1, n_patch)
    def _(i):
        pcopy((pat + i) % n_patch, pat).wait_send()

    @pl.loop(1, n_obs)
    def _(i):
        o = (obs + i) % n_obs
        qcopy(o, o).wait_recv()

    curvature = rowsum(jnp.sum(qlr[...], axis=0)) + reg
    out[...] = slip[...] + (norm / curvature) * d[...]

    @pl.loop(1, n_obs)
    def _(i):
        qcopy((obs + i) % n_obs, obs).wait_send()


def shards(green, data, neighbours, reg_weight):
    rows, cols = green.shape
    E = data.shape[1]
    n_obs, n_patch = lax.axis_size("obs"), lax.axis_size("patch")
    nz = n_patch // 2
    nd = 4
    R, BR, ext = rows // 2 // nz, cols // n_obs, cols + 2 * BAND
    first, messages = 4 * (nz // 4) - 3, nz - 1
    V = pltpu.VMEM
    D = pltpu.SemaphoreType.DMA
    scratch = [
        V((rows, cols), BF16), V((rows, cols), BF16),
        V((cols, rows), BF16), V((cols, rows), BF16),
        V((cols, ext), BF16), V((ext, cols), BF16),
        V((cols, 2 * E), BF16), V((rows, 2 * E), BF16), V((ext, 2 * E), BF16),
        V((cols, E), F32), V((cols, E), F32), V((cols, E), F32), V((ext, E), F32), V((cols, E), F32),
        V((2, BAND, E), F32), V((2, BAND, E), F32), V((R, E), F32), V((R, E), F32),
        V((nz, R, E), F32), V((nz, R, E), F32), V((ITERS, nd, nz // nd, R, E), F32),
        V((ITERS, first, R, E), F32), V((2, R, E), F32), V((ITERS, 2, R, E), F32),
        V((ITERS - 1, 2, nz, R, E), F32),
        V((ITERS, n_obs, BR, E), F32), V((ITERS, n_obs, BR, E), F32), V((ITERS, cols, E), F32),
        V((ITERS, 2, BAND, E), F32), V((ITERS - 1, 2, BAND, E), F32),
        V((ITERS, 8, E), F32), V((ITERS, n_patch, 8, E), F32),
        V((8, E), F32), V((n_patch, 8, E), F32), V((8, E), F32), V((n_obs, 8, E), F32),
        D((2, ITERS, nd)), D((2, ITERS, first)), D((2, ITERS, 2)), D((2, ITERS - 1, nz)), D((2, ITERS - 1, nz)),
        D((2, ITERS, n_obs)), D((2, ITERS, n_obs)), D((2, ITERS, 2)), D((2, ITERS - 1, 2)),
        D((2, ITERS, n_patch)), D((2, n_patch)), D((2, n_obs)),
    ]
    return pl.pallas_call(
        functools.partial(kernel, n_obs, n_patch),
        out_shape=jax.ShapeDtypeStruct((cols, E), F32),
        in_specs=[pl.BlockSpec(memory_space=pltpu.VMEM)] * 4,
        out_specs=pl.BlockSpec(memory_space=pltpu.VMEM),
        scratch_shapes=scratch,
        compiler_params=pltpu.CompilerParams(
            collective_id=0, has_side_effects=True, vmem_limit_bytes=56 * 1024 * 1024),
    )(green, data, neighbours, reg_weight.reshape(1, E))


def solution(mesh):
    in_specs = (P("obs", "patch"), P("obs", None), P(None, "patch"), P())
    return jax.shard_map(shards, mesh=mesh, in_specs=in_specs, out_specs=P("patch", None), check_vma=False)
```

```python
import functools
import math

import jax
import jax.numpy as jnp
from jax import lax
from jax.experimental import pallas as pl
from jax.experimental.pallas import tpu as pltpu
from jax.sharding import PartitionSpec as P

BAND = 128
ITERS = 3
MESH = pl.DeviceIdType.MESH
F32 = jnp.float32
BF16 = jnp.bfloat16


def dot(a, b):
    return lax.dot_general(a, b, (((1,), (0,)), ((), ())), preferred_element_type=F32)


def split(x):
    hi = x.astype(BF16)
    return hi, (x - hi.astype(F32)).astype(BF16)


def kernel(n_obs, n_patch, green_h, data_h, nb_h, rw_h, slip_h, d_h, scale,
           green, data, nb, rw,
           ghi, glo, gthi, gtlo, lm, lmt, cat_d, cat_r, cat_e,
           d, g, a, wext, slip, hd, hg, qd, qg,
           pf, s, rd, zr, zrel, zfin, img, bs, br, ag, hal, wr, scs, scp, scz, scr, pls, plr, qls, qlr,
           sem_l, sem_o, sem_d, sem_z, sem_f, sem_g, sem_i, sem_b, sem_a, sem_h, sem_w, sem_c, sem_s, sem_p, sem_q):
    rows, cols = green.shape
    E = data.shape[1]
    nz = n_patch // 2
    R = rows // 2 // nz
    BR = cols // n_obs
    half = rows // 2
    per = 4
    nch = n_obs // per
    nd = rd.shape[1]
    PD = nz // nd
    CB = cols // BAND
    Q = nz // 4
    plus = list(range(1, Q + 1))
    minus = list(range(1, Q))
    obs = lax.axis_index("obs")
    pat = lax.axis_index("patch")
    z = pat // 2
    c = pat % 2
    other = 1 - c
    partner = z * 2 + other
    has_l, has_r = pat > 0, pat < n_patch - 1

    def at(o, q):
        return (o, q)

    def rcopy(src, dst, sems, dev):
        return pltpu.make_async_remote_copy(
            src_ref=src, dst_ref=dst, send_sem=sems[0], recv_sem=sems[1],
            device_id=dev, device_id_type=MESH)

    def pair(sem, *idx):
        return sem.at[(0,) + idx], sem.at[(1,) + idx]

    nblk = rows // BAND

    def load(i):
        r0 = pl.multiple_of(i * BAND, BAND)
        return pltpu.make_async_copy(green_h.at[pl.ds(r0, BAND)], green.at[pl.ds(r0, BAND)], sem_l.at[i])

    small = [pltpu.make_async_copy(src, dst, sem_l.at[nblk + i])
             for i, (src, dst) in enumerate(((data_h, data), (nb_h, nb), (rw_h, rw)))]
    small[0].start()

    @pl.loop(0, nblk)
    def _(i):
        load(i).start()

    for copy in small[1:]:
        copy.start()

    barrier = pltpu.get_barrier_semaphore()

    @pl.loop(1, n_patch)
    def _(i):
        pl.semaphore_signal(barrier, inc=1, device_id=at(obs, (pat + i) % n_patch), device_id_type=MESH)

    @pl.loop(1, n_obs)
    def _(i):
        pl.semaphore_signal(barrier, inc=1, device_id=at((obs + i) % n_obs, pat), device_id_type=MESH)

    small[0].wait()

    @pl.loop(0, nblk)
    def _(i):
        r0 = pl.multiple_of(i * BAND, BAND)
        load(i).wait()
        block = green[pl.ds(r0, BAND), :]
        hi, lo = split(block)
        ghi[pl.ds(r0, BAND), :] = hi
        glo[pl.ds(r0, BAND), :] = lo
        hi, lo = split(block.T)
        gthi[:, pl.ds(r0, BAND)] = hi
        gtlo[:, pl.ds(r0, BAND)] = lo
        hi, lo = split(data[pl.ds(r0, BAND), :])
        cat_r[pl.ds(r0, BAND), 0:E] = hi
        cat_r[pl.ds(r0, BAND), E:2 * E] = lo

    for copy in small[1:]:
        copy.wait()
    weight = rw[...]

    zero_h = jnp.zeros((BAND, E), F32)

    @pl.when(pat == 0)
    def _():
        for it in range(ITERS):
            hal[it, 0] = zero_h
        for it in range(ITERS - 1):
            wr[it, 0] = zero_h

    @pl.when(pat == n_patch - 1)
    def _():
        for it in range(ITERS):
            hal[it, 1] = zero_h
        for it in range(ITERS - 1):
            wr[it, 1] = zero_h

    def build_laplace():
        @pl.loop(0, CB + 2)
        def _(j):
            r0 = pl.multiple_of(j * BAND, BAND)
            col = lax.broadcasted_iota(jnp.int32, (BAND, cols), 0) + j * BAND
            own = lax.broadcasted_iota(jnp.int32, (BAND, cols), 1) + BAND
            m = jnp.where(col == own, 4.0, 0.0)
            col = col + (pat * cols - BAND)
            for k in range(3):
                m = m - jnp.where(col == nb[k:k + 1, :], 1.0, 0.0)
            lmt[pl.ds(r0, BAND), :] = m.astype(BF16)
            lm[:, pl.ds(r0, BAND)] = m.T.astype(BF16)

    def bcopy(b, o, slot):
        return rcopy(bs.at[b, o], br.at[b, slot], (sem_b.at[0, b, o], sem_b.at[1, b, slot]), at(o, pat))

    def acopy(b, o, slot):
        r0 = pl.multiple_of(slot * BR, BR)
        return rcopy(ag.at[b, pl.ds(r0, BR)], ag.at[b, pl.ds(r0, BR)],
                     (sem_a.at[0, b, o], sem_a.at[1, b, slot]), at(o, pat))

    def backward(b, hook):
        @pl.loop(1, nch + 1)
        def _(j):
            ch = (obs // per + j) % nch
            r0 = pl.multiple_of(ch * (per * BR), per * BR)
            y = dot(gthi[pl.ds(r0, per * BR), :], cat_r[...])
            y = y[:, :E] + y[:, E:] + dot(gtlo[pl.ds(r0, per * BR), :], cat_r[:, 0:E])
            bs[b, pl.ds(ch * per, per)] = y.reshape(per, BR, E)
            if b == 0:
                return
            for i in range(per):
                o = ch * per + i

                @pl.when(o != obs)
                def _():
                    bcopy(b, o, obs).start()

        hook()

        if b == 0:
            pl.semaphore_wait(barrier, n_patch - 1 + n_obs - 1)

            @pl.loop(1, n_obs)
            def _(i):
                bcopy(b, (obs + i) % n_obs, obs).start()

        def add(i, acc):
            o = (obs + i) % n_obs
            bcopy(b, o, o).wait_recv()
            return acc + br[b, o]

        total = lax.fori_loop(1, n_obs, add, bs[b, obs])
        ag[b, pl.ds(pl.multiple_of(obs * BR, BR), BR), :] = total

        @pl.loop(1, n_obs)
        def _(i):
            acopy(b, (obs + i) % n_obs, obs).start()

        @pl.loop(1, n_obs)
        def _(i):
            o = (obs + i) % n_obs
            acopy(b, o, o).wait_recv()

    def backward_end(b):
        @pl.loop(1, n_obs)
        def _(i):
            o = (obs + i) % n_obs
            bcopy(b, o, obs).wait_send()
            acopy(b, o, obs).wait_send()

    def dcopy(it, k):
        return rcopy(pf.at[pl.ds(k * PD, PD)], rd.at[it, k], pair(sem_d, it, k), at(obs, partner))

    def zat(k):
        return at(obs, ((z + k + nz) % nz) * 2 + c)

    def owner(k):
        return (z + k + 2 * nz) % nz

    first_step = ([(-k, -k - Q) for k in reversed(plus)] + [(k, k + Q) for k in reversed(minus)]
                  + [(-k, -k) for k in reversed(minus)] + [(k, k) for k in reversed(minus)])
    n_plus, n_minus = len(plus), len(minus)

    def zcopy(it, slot):
        k, o = first_step[slot]
        return rcopy(s.at[owner(o)], zr.at[it, slot], pair(sem_z, it, slot), zat(k))

    def fcopy(it, slot):
        return rcopy(zrel.at[slot], zfin.at[it, slot], pair(sem_f, it, slot), zat(-Q if slot == 0 else Q))

    near = [(k, 0) for k in (-Q, Q) ] + [(sgn * k, 0) for k in reversed(minus) for sgn in (1, -1)]
    relay_p = [(k, -Q) for k in reversed(plus)]
    relay_m = [(-k, Q) for k in reversed(minus)]
    gather = near + relay_p + relay_m

    def gcopy(it, m):
        k, o = gather[m]
        p = owner(o)
        return rcopy(img.at[it, c, p], img.at[it, c, p], (sem_g.at[0, it, m], sem_g.at[1, it, p]), zat(k))

    def gwait(it, p):
        rcopy(img.at[it, c, p], img.at[it, c, p], (sem_g.at[0, it, 0], sem_g.at[1, it, p]), zat(1)).wait_recv()

    def icopy(it, k):
        return rcopy(img.at[it, c, k], img.at[it, c, k], pair(sem_i, it, k), at(obs, partner))

    def fold(acc, it, slots):
        for slot in slots:
            zcopy(it, slot).wait_recv()
            acc = acc + zr[it, slot]
        return acc

    def hsrc(it):
        return a if it else ag.at[0]

    def hcopy_r(it):
        return rcopy(hsrc(it).at[pl.ds(cols - BAND, BAND)], hal.at[it, 0], pair(sem_h, it, 0), at(obs, pat + 1))

    def hcopy_l(it):
        return rcopy(hsrc(it).at[pl.ds(0, BAND)], hal.at[it, 1], pair(sem_h, it, 1), at(obs, pat - 1))

    def forward(it, hook):
        last = it == ITERS - 1

        hi, lo = split(hsrc(it)[...])
        cat_d[:, 0:E] = hi
        cat_d[:, E:2 * E] = lo

        def part(h):
            r0 = pl.multiple_of(h * half, half)
            y = dot(ghi[pl.ds(r0, half), :], cat_d[...])
            y = y[:, :E] + y[:, E:] + dot(glo[pl.ds(r0, half), :], cat_d[:, 0:E])
            return y.reshape(nz, R, E)

        pf[...] = part(other)

        for k in range(nd):
            dcopy(it, k).start()

        if it:
            dots(it - 1)

        s[...] = part(c)

        for k in range(nd):
            dcopy(it, k).wait_recv()
            s[k * PD:(k + 1) * PD] += rd[it, k]

        for slot in range(n_plus + n_minus):
            zcopy(it, slot).start()

        if it:
            sums_mid(it - 1)

        @pl.when(has_r)
        def _():
            hcopy_r(it).start()

        @pl.when(has_l)
        def _():
            hcopy_l(it).start()

        for slot in range(n_plus + n_minus, len(first_step)):
            zcopy(it, slot).start()

        zrel[0] = fold(s[owner(-Q)], it, range(n_plus))
        fcopy(it, 0).start()
        zrel[1] = fold(s[owner(Q)], it, range(n_plus, n_plus + n_minus))
        fcopy(it, 1).start()

        scalars = hook()

        total = fold(s[z], it, range(n_plus + n_minus, len(first_step)))
        for slot in range(2):
            fcopy(it, slot).wait_recv()
            total = total + zfin[it, slot]

        if it:
            step, ratio = scalars
            rest = qg[...] - step * total
            total = rest + ratio * qd[...]
        else:
            rest = total

        if last:
            sq = jnp.sum(total * total, axis=0, keepdims=True)
        else:
            sq = None
            qg[...] = rest
            qd[...] = total
            img[it, c, z] = total
            for m in range(len(near)):
                gcopy(it, m).start()
            icopy(it, z).start()
            gwait(it, owner(-Q))
            for m in range(len(near), len(near) + len(relay_p)):
                gcopy(it, m).start()
            gwait(it, owner(Q))
            for m in range(len(near) + len(relay_p), len(gather)):
                gcopy(it, m).start()
            icopy(it, owner(-Q)).start()
            icopy(it, owner(Q)).start()
            seen = {0, nz - Q, Q}

            for k in minus:
                for o in (-k, k):
                    gwait(it, owner(o))
                    icopy(it, owner(o)).start()
                    seen.add(o % nz)
            for o in range(nz):
                if o not in seen:
                    gwait(it, owner(o))
                    icopy(it, owner(o)).start()

            for o in range(nz):
                icopy(it, owner(o)).wait_recv()
            hi, lo = split(img[it].reshape(rows, E))
            cat_r[:, 0:E] = hi
            cat_r[:, E:2 * E] = lo

        return sq

    def forward_end(it):
        for k in range(nd):
            dcopy(it, k).wait_send()
        for slot in range(len(first_step)):
            zcopy(it, slot).wait_send()
        for slot in range(2):
            fcopy(it, slot).wait_send()
        if it < ITERS - 1:
            for m in range(len(gather)):
                gcopy(it, m).wait_send()

            @pl.loop(0, nz)
            def _(k):
                icopy(it, k).wait_send()

    def halo_wait(it):
        @pl.when(has_l)
        def _():
            hcopy_r(it).wait_recv()

        @pl.when(has_r)
        def _():
            hcopy_l(it).wait_recv()

        @pl.when(has_r)
        def _():
            hcopy_r(it).wait_send()

        @pl.when(has_l)
        def _():
            hcopy_l(it).wait_send()

    def laplace():
        for r0, n, v in ((0, BAND, hd[0]), (BAND, cols, d[...]), (BAND + cols, BAND, hd[1])):
            hi, lo = split(v)
            cat_e[r0:r0 + n, 0:E] = hi
            cat_e[r0:r0 + n, E:2 * E] = lo

    def lap_rows(i):
        r0 = pl.multiple_of(i * BAND, BAND)
        y = dot(lm[pl.ds(r0, BAND), :], cat_e[...])
        return r0, weight * (y[:, :E] + y[:, E:])

    def wcopy_l(it):
        return rcopy(wext.at[pl.ds(0, BAND)], wr.at[it, 1], pair(sem_w, it, 1), at(obs, pat - 1))

    def wcopy_r(it):
        return rcopy(wext.at[pl.ds(BAND + cols, BAND)], wr.at[it, 0], pair(sem_w, it, 0), at(obs, pat + 1))

    def reg_start(it):
        laplace()

        @pl.loop(0, CB)
        def _(i):
            r0, u = lap_rows(i)
            hi, lo = split(u)
            cat_d[pl.ds(r0, BAND), 0:E] = hi
            cat_d[pl.ds(r0, BAND), E:2 * E] = lo

        @pl.loop(0, CB + 2)
        def _(i):
            r0 = pl.multiple_of(i * BAND, BAND)
            y = dot(lmt[pl.ds(r0, BAND), :], cat_d[...])
            wext[pl.ds(r0, BAND), :] = weight * (y[:, :E] + y[:, E:])

        @pl.when(has_l)
        def _():
            wcopy_l(it).start()

        @pl.when(has_r)
        def _():
            wcopy_r(it).start()

    def reg_end(it):
        a[...] = ag[it + 1] + wext[BAND:BAND + cols, :]

        @pl.when(has_l)
        def _():
            wcopy_r(it).wait_recv()

        @pl.when(has_r)
        def _():
            wcopy_l(it).wait_recv()

        a[0:BAND, :] += wr[it, 0]
        a[cols - BAND:cols, :] += wr[it, 1]

    def reg_done(it):
        @pl.when(has_l)
        def _():
            wcopy_l(it).wait_send()

        @pl.when(has_r)
        def _():
            wcopy_r(it).wait_send()

    def ccopy(it):
        return rcopy(scs.at[it], scp.at[it], pair(sem_c, it), at(obs, partner))

    def scopy(it, k, slot):
        return rcopy(scz.at[it], scr.at[it, slot], (sem_s.at[0, it, k], sem_s.at[1, it, slot]), zat(k))

    def sums_mid(it):
        ccopy(it).wait_recv()
        scz[it] = scs[it] + scp[it]
        scr[it, z] = scs[it] + scp[it]

        @pl.loop(1, nz)
        def _(k):
            scopy(it, k, z).start()

    def sums_end(it):
        @pl.loop(1, nz)
        def _(k):
            scopy(it, k, owner(k)).wait_recv()

        return jnp.sum(scr[it], axis=0)

    def sums_done(it):
        ccopy(it).wait_send()

        @pl.loop(1, nz)
        def _(k):
            scopy(it, k, z).wait_send()

    def pcopy(q, slot):
        return rcopy(pls, plr.at[slot], (sem_p.at[0, q], sem_p.at[1, slot]), at(obs, q))

    def qcopy(o, slot):
        return rcopy(qls, qlr.at[slot], (sem_q.at[0, o], sem_q.at[1, slot]), at(o, pat))

    def rowsum(x):
        return jnp.sum(x, axis=0, keepdims=True)

    norms, regs = [], []

    def dots(it):
        gv, dv, av = g[...], d[...], a[...]
        scs[it, 0:1, :] = rowsum(gv * gv)
        scs[it, 1:2, :] = rowsum(dv * av)
        scs[it, 2:3, :] = rowsum(gv * av)
        scs[it, 3:4, :] = rowsum(av * av)
        ccopy(it).start()

    def first():
        halo_wait(0)
        hg[...] = hal[0]
        hd[...] = hal[0]

    def advance(it):
        tot = sums_end(it - 1)
        if it == 1:
            norms.append(tot[0:1])
        norm = norms[-1]
        step = norm / tot[1:2]
        after = norm - 2.0 * step * tot[2:3] + step * step * tot[3:4]
        ratio = after / norm
        norms.append(after)
        halo_wait(it)
        if it == 1:
            slip[...] = step * d[...]
        else:
            slip[...] += step * d[...]
        g[...] = g[...] - step * a[...]
        d[...] = g[...] + ratio * d[...]
        hg[...] = hg[...] - step * hal[it]
        hd[...] = hg[...] + ratio * hd[...]
        if it == ITERS - 1:
            laplace()

            def energy(i, acc):
                _, u = lap_rows(i)
                return acc + jnp.sum((u * u).reshape(BAND // 8, 8, E), axis=0)

            regs.append(rowsum(lax.fori_loop(0, CB, energy, jnp.zeros((8, E), F32))))
            for k, (src, dst) in enumerate(((slip, slip_h), (d, d_h))):
                pltpu.make_async_copy(src, dst, sem_o.at[k]).start()
        return step, ratio

    backward(0, build_laplace)
    g[...] = ag[0]
    d[...] = ag[0]
    forward(0, first)
    for it in range(1, ITERS):
        backward(it, functools.partial(reg_start, it - 1))
        forward_end(it - 1)
        reg_end(it - 1)
        sq = forward(it, functools.partial(advance, it))
        reg_done(it - 1)
    last = ITERS - 1
    norm = norms[-1]
    sq = sq + jnp.where(obs == 0, regs[0], 0.0)
    pls[...] = sq
    plr[pat] = sq

    @pl.loop(1, n_patch)
    def _(i):
        pcopy((pat + i) % n_patch, pat).start()

    forward_end(last)
    for it in range(ITERS):
        backward_end(it)
    for it in range(ITERS - 1):
        sums_done(it)

    @pl.loop(1, n_patch)
    def _(i):
        q = (pat + i) % n_patch
        pcopy(q, q).wait_recv()

    line = jnp.sum(plr[...], axis=0)
    qls[...] = line
    qlr[obs] = line

    @pl.loop(1, n_obs)
    def _(i):
        qcopy((obs + i) % n_obs, obs).start()

    @pl.loop(1, n_patch)
    def _(i):
        pcopy((pat + i) % n_patch, pat).wait_send()

    for k, (src, dst) in enumerate(((slip, slip_h), (d, d_h))):
        pltpu.make_async_copy(src, dst, sem_o.at[k]).wait()

    @pl.loop(1, n_obs)
    def _(i):
        o = (obs + i) % n_obs
        qcopy(o, o).wait_recv()

    scale[...] = norm / jnp.sum(qlr[...], axis=0)

    @pl.loop(1, n_obs)
    def _(i):
        qcopy((obs + i) % n_obs, obs).wait_send()


def shards(green, data, neighbours, reg_weight):
    rows, cols = green.shape
    E = data.shape[1]
    n_obs, n_patch = lax.axis_size("obs"), lax.axis_size("patch")
    nz = n_patch // 2
    nd = 4
    R, BR, ext = rows // 2 // nz, cols // n_obs, cols + 2 * BAND
    first, messages = 4 * (nz // 4) - 3, nz - 1
    V = pltpu.VMEM
    D = pltpu.SemaphoreType.DMA
    scratch = [
        V((rows, cols), F32), V((rows, E), F32), V(neighbours.shape, jnp.int32), V((1, E), F32),
        V((rows, cols), BF16), V((rows, cols), BF16),
        V((cols, rows), BF16), V((cols, rows), BF16),
        V((cols, ext), BF16), V((ext, cols), BF16),
        V((cols, 2 * E), BF16), V((rows, 2 * E), BF16), V((ext, 2 * E), BF16),
        V((cols, E), F32), V((cols, E), F32), V((cols, E), F32), V((ext, E), F32), V((cols, E), F32),
        V((2, BAND, E), F32), V((2, BAND, E), F32), V((R, E), F32), V((R, E), F32),
        V((nz, R, E), F32), V((nz, R, E), F32), V((ITERS, nd, nz // nd, R, E), F32),
        V((ITERS, first, R, E), F32), V((2, R, E), F32), V((ITERS, 2, R, E), F32),
        V((ITERS - 1, 2, nz, R, E), F32),
        V((ITERS, n_obs, BR, E), F32), V((ITERS, n_obs, BR, E), F32), V((ITERS, cols, E), F32),
        V((ITERS, 2, BAND, E), F32), V((ITERS - 1, 2, BAND, E), F32),
        V((ITERS - 1, 4, E), F32), V((ITERS - 1, 4, E), F32), V((ITERS - 1, 4, E), F32), V((ITERS - 1, nz, 4, E), F32),
        V((1, E), F32), V((n_patch, 1, E), F32), V((1, E), F32), V((n_obs, 1, E), F32),
        D((rows // BAND + 3,)), D((2,)),
        D((2, ITERS, nd)), D((2, ITERS, first)), D((2, ITERS, 2)), D((2, ITERS - 1, nz)), D((2, ITERS - 1, nz)),
        D((2, ITERS, n_obs)), D((2, ITERS, n_obs)), D((2, ITERS, 2)), D((2, ITERS - 1, 2)),
        D((2, ITERS - 1)), D((2, ITERS - 1, nz)), D((2, n_patch)), D((2, n_obs)),
    ]
    anywhere = pl.BlockSpec(memory_space=pl.ANY)
    slip, d, scale = pl.pallas_call(
        functools.partial(kernel, n_obs, n_patch),
        out_shape=[jax.ShapeDtypeStruct((cols, E), F32)] * 2 + [jax.ShapeDtypeStruct((1, E), F32)],
        in_specs=[anywhere] * 4,
        out_specs=[anywhere, anywhere, pl.BlockSpec(memory_space=pltpu.VMEM)],
        scratch_shapes=scratch,
        compiler_params=pltpu.CompilerParams(
            collective_id=0, has_side_effects=True, vmem_limit_bytes=56 * 1024 * 1024),
    )(green, data, neighbours, reg_weight.reshape(1, E))
    return slip + scale * d


def solution(mesh):
    in_specs = (P("obs", "patch"), P("obs", None), P(None, "patch"), P())
    return jax.shard_map(shards, mesh=mesh, in_specs=in_specs, out_specs=P("patch", None), check_vma=False)
```

```python
import functools
import math

import jax
import jax.numpy as jnp
from jax import lax
from jax.experimental import pallas as pl
from jax.experimental.pallas import tpu as pltpu
from jax.sharding import PartitionSpec as P

BAND = 128
ITERS = 3
MESH = pl.DeviceIdType.MESH
F32 = jnp.float32
BF16 = jnp.bfloat16


def dot(a, b):
    return lax.dot_general(a, b, (((1,), (0,)), ((), ())), preferred_element_type=F32)


def split(x):
    hi = x.astype(BF16)
    return hi, (x - hi.astype(F32)).astype(BF16)


def kernel(n_obs, n_patch, green_h, data_h, nb_h, rw_h, slip_h, d_h, scale,
           green, data, nb, rw,
           ghi, glo, gthi, gtlo, lm, lmt, cat_d, cat_r, cat_e,
           d, g, a, wext, slip, hd, hg, qd, qg,
           pf, s, rd, zr, zrel, zfin, img, bs, br, ag, hal, wr, scs, scp, scz, scr, pls, plr, qls, qlr,
           sem_l, sem_o, sem_d, sem_z, sem_f, sem_g, sem_i, sem_b, sem_a, sem_h, sem_w, sem_c, sem_s, sem_p, sem_q):
    rows, cols = green.shape
    E = data.shape[1]
    nz = n_patch // 2
    R = rows // 2 // nz
    BR = cols // n_obs
    half = rows // 2
    per = nch = math.isqrt(n_obs)
    CB = cols // BAND
    Q = nz // 4
    plus = list(range(1, Q + 1))
    minus = list(range(1, Q))
    near = [0] + [sgn * k for k in minus for sgn in (1, -1)] + [Q]
    far = [2 * Q] + [sgn * k for k in range(2 * Q - 1, Q, -1) for sgn in (1, -1)] + [-Q]
    pieces = near + far
    NP = len(near)
    quarter = half // 2

    def wrapped(o):
        return (o + 2 * Q - 1) % nz - 2 * Q + 1

    def idx(o):
        return pieces.index(wrapped(o))
    obs = lax.axis_index("obs")
    pat = lax.axis_index("patch")
    z = pat // 2
    c = pat % 2
    other = 1 - c
    partner = z * 2 + other
    has_l, has_r = pat > 0, pat < n_patch - 1

    def at(o, q):
        return (o, q)

    def rcopy(src, dst, sems, dev):
        return pltpu.make_async_remote_copy(
            src_ref=src, dst_ref=dst, send_sem=sems[0], recv_sem=sems[1],
            device_id=dev, device_id_type=MESH)

    def pair(sem, *idx):
        return sem.at[(0,) + idx], sem.at[(1,) + idx]

    def load(n):
        part, h, r = n // (2 * NP), n // NP % 2, n % NP
        o = pieces[part * NP + r]
        src = pl.multiple_of(h * half + (z + (1 - 2 * h) * o + nz) % nz * R, R)
        return [pltpu.make_async_copy(a_.at[pl.ds(src, R)], b_.at[pl.ds(n * R, R)], sem_l.at[k, n])
                for k, (a_, b_) in enumerate(((green_h, green), (data_h, data)))]

    for n in range(2 * nz):
        for copy in load(n):
            copy.start()

    small = [pltpu.make_async_copy(src, dst, sem_l.at[i, 2 * nz])
             for i, (src, dst) in enumerate(((nb_h, nb), (rw_h, rw)))]
    for copy in small:
        copy.start()

    barrier = pltpu.get_barrier_semaphore()

    def greet(o, q):
        pl.semaphore_signal(barrier, inc=1, device_id=at(o, q), device_id_type=MESH)

    greet(obs, (pat + nz) % n_patch)

    @pl.loop(1, nz)
    def _(i):
        greet(obs, (pat + nz + i) % n_patch)
        greet(obs, (pat + nz - i) % n_patch)

    @pl.loop(1, n_obs)
    def _(i):
        greet((obs + i) % n_obs, pat)

    def put_cat(where, value):
        hi, lo = split(value)
        cat_r[where, 0:E] = hi
        cat_r[where, E:2 * E] = lo

    def product(m0, m1, k0, k1):
        y = dot(gthi[m0:m1, k0:k1], cat_r[k0:k1, :])
        y = y[:, :E] + y[:, E:] + dot(gtlo[m0:m1, k0:k1], cat_r[k0:k1, 0:E])
        return y.reshape((m1 - m0) // BR, BR, E)

    def first_product(r0):
        y = product(0, cols, r0, r0 + STEP)
        if r0 == 0:
            bs[0] = y
        else:
            bs[0] += y

    STEP = 2 * BAND
    loaded = 0
    for r0 in range(0, rows, STEP):
        while loaded * R < r0 + STEP:
            for copy in load(loaded):
                copy.wait()
            loaded += 1
        if r0:
            first_product(r0 - STEP)
        for r in range(r0, r0 + STEP, BAND):
            block = green[r:r + BAND, :]
            hi, lo = split(block)
            ghi[r:r + BAND, :] = hi
            glo[r:r + BAND, :] = lo
            hi, lo = split(block.T)
            gthi[:, r:r + BAND] = hi
            gtlo[:, r:r + BAND] = lo
            put_cat(slice(r, r + BAND), data[r:r + BAND, :])

    first_product(rows - STEP)

    for copy in small:
        copy.wait()
    weight = rw[...]

    zero_h = jnp.zeros((BAND, E), F32)

    @pl.when(pat == 0)
    def _():
        for it in range(ITERS):
            hal[it, 0] = zero_h
        for it in range(ITERS - 1):
            wr[it, 0] = zero_h

    @pl.when(pat == n_patch - 1)
    def _():
        for it in range(ITERS):
            hal[it, 1] = zero_h
        for it in range(ITERS - 1):
            wr[it, 1] = zero_h

    def build_laplace():
        @pl.loop(0, CB + 2)
        def _(j):
            r0 = pl.multiple_of(j * BAND, BAND)
            col = lax.broadcasted_iota(jnp.int32, (BAND, cols), 0) + j * BAND
            own = lax.broadcasted_iota(jnp.int32, (BAND, cols), 1) + BAND
            m = jnp.where(col == own, 4.0, 0.0)
            col = col + (pat * cols - BAND)
            for k in range(3):
                m = m - jnp.where(col == nb[k:k + 1, :], 1.0, 0.0)
            lmt[pl.ds(r0, BAND), :] = m.astype(BF16)
            lm[:, pl.ds(r0, BAND)] = m.T.astype(BF16)

    side = math.isqrt(n_obs)
    steps = sorted(range(side), key=lambda k: -min(k, side - k))
    far_first = sorted([(i, j) for i in steps for j in steps if i or j],
                       key=lambda ij: -sum(min(k, side - k) for k in ij))

    def shifted(i, j):
        return (obs // side + i) % side * side + (obs + j) % side

    def bcopy(b, o, slot):
        return rcopy(bs.at[b, o], br.at[b, slot], (sem_b.at[0, b, o], sem_b.at[1, b, slot]), at(o, pat))

    def acopy(b, o, slot):
        r0 = pl.multiple_of(slot * BR, BR)
        return rcopy(ag.at[b, pl.ds(r0, BR)], ag.at[b, pl.ds(r0, BR)],
                     (sem_a.at[0, b, o], sem_a.at[1, b, slot]), at(o, pat))

    def backward(b, hook):
        if b == 0:
            pl.semaphore_wait(barrier, n_patch - 1 + n_obs - 1)

            for i, j in far_first:
                bcopy(b, shifted(i, j), obs).start()
        else:
            for o in far:
                if o != -Q:
                    gwait(b - 1, o)
                    icopy(b - 1, o).start()

            for o in far:
                icopy(b - 1, o).wait_recv()

            for h in range(2):
                put_cat(slice(half + h * quarter, half + (h + 1) * quarter), img[b - 1, h, NP:].reshape(quarter, E))
            for i in steps:
                ch = (obs // side + i) % side
                r0 = pl.multiple_of(ch * (per * BR), per * BR)
                y = dot(gthi[pl.ds(r0, per * BR), half:], cat_r[half:, :])
                y = y[:, :E] + y[:, E:] + dot(gtlo[pl.ds(r0, per * BR), half:], cat_r[half:, 0:E])
                bs[b, pl.ds(ch * per, per)] += y.reshape(per, BR, E)
                for j in steps:
                    if i or j:
                        bcopy(b, shifted(i, j), obs).start()

        hook()

        def add(i, acc):
            o = (obs + i) % n_obs
            bcopy(b, o, o).wait_recv()
            return acc + br[b, o]

        total = lax.fori_loop(1, n_obs, add, bs[b, obs])
        ag[b, pl.ds(pl.multiple_of(obs * BR, BR), BR), :] = total

        for i, j in far_first:
            acopy(b, shifted(i, j), obs).start()

        @pl.loop(1, n_obs)
        def _(i):
            o = (obs + i) % n_obs
            acopy(b, o, o).wait_recv()

    def backward_end(b):
        @pl.loop(1, n_obs)
        def _(i):
            o = (obs + i) % n_obs
            bcopy(b, o, obs).wait_send()
            acopy(b, o, obs).wait_send()

    def dcopy(it, k):
        return rcopy(pf.at[pl.ds(k * NP, NP)], rd.at[it, k], pair(sem_d, it, k), at(obs, partner))

    turn = 1 - 2 * c

    def zat(k):
        return at(obs, ((z + turn * k + nz) % nz) * 2 + c)

    first_step = ([(-k, -k - Q) for k in reversed(plus)] + [(k, k + Q) for k in reversed(minus)]
                  + [(-k, -k) for k in reversed(minus)] + [(k, k) for k in reversed(minus)])
    n_plus, n_minus = len(plus), len(minus)

    def zcopy(it, slot):
        k, o = first_step[slot]
        return rcopy(s.at[idx(o)], zr.at[it, slot], pair(sem_z, it, slot), zat(k))

    def fcopy(it, slot):
        return rcopy(zrel.at[slot], zfin.at[it, slot], pair(sem_f, it, slot), zat(-Q if slot == 0 else Q))

    gather = ([(k, 0) for k in (-Q, Q)] + [(sgn * k, 0) for k in reversed(minus) for sgn in (1, -1)]
              + [(k, -Q) for k in reversed(plus)] + [(-k, Q) for k in reversed(minus)])
    n_own = 2 * Q

    def gcopy(it, m):
        k, o = gather[m]
        to = idx(o - k)
        return rcopy(img.at[it, c, idx(o)], img.at[it, c, to], (sem_g.at[0, it, m], sem_g.at[1, it, to]), zat(k))

    def gwait(it, o):
        piece = img.at[it, c, idx(o)]
        rcopy(piece, piece, (sem_g.at[0, it, 0], sem_g.at[1, it, idx(o)]), zat(1)).wait_recv()

    def icopy(it, o):
        piece = img.at[it, c, idx(o)]
        return rcopy(piece, piece, pair(sem_i, it, idx(o)), at(obs, partner))

    def fold(acc, it, slots):
        for slot in slots:
            zcopy(it, slot).wait_recv()
            acc = acc + zr[it, slot]
        return acc

    def hsrc(it):
        return a if it else ag.at[0]

    def hcopy_r(it):
        return rcopy(hsrc(it).at[pl.ds(cols - BAND, BAND)], hal.at[it, 0], pair(sem_h, it, 0), at(obs, pat + 1))

    def hcopy_l(it):
        return rcopy(hsrc(it).at[pl.ds(0, BAND)], hal.at[it, 1], pair(sem_h, it, 1), at(obs, pat - 1))

    def forward(it, hook):
        last = it == ITERS - 1

        hi, lo = split(hsrc(it)[...])
        cat_d[:, 0:E] = hi
        cat_d[:, E:2 * E] = lo

        def part(h, k):
            r0 = pl.multiple_of(k * half + h * quarter, quarter)
            y = dot(ghi[pl.ds(r0, quarter), :], cat_d[...])
            y = y[:, :E] + y[:, E:] + dot(glo[pl.ds(r0, quarter), :], cat_d[:, 0:E])
            return y.reshape(NP, R, E)

        for k in (1, 0):
            pf[k * NP:(k + 1) * NP] = part(other, k)
            dcopy(it, k).start()

        if it:
            dots(it - 1)

        for k in (1, 0):
            s[k * NP:(k + 1) * NP] = part(c, k)

        dcopy(it, 1).wait_recv()
        s[NP:] += rd[it, 1]
        for slot in range(n_plus + n_minus):
            zcopy(it, slot).start()
        dcopy(it, 0).wait_recv()
        s[:NP] += rd[it, 0]

        if it:
            sums_mid(it - 1)

        @pl.when(has_r)
        def _():
            hcopy_r(it).start()

        @pl.when(has_l)
        def _():
            hcopy_l(it).start()

        for slot in range(n_plus + n_minus, len(first_step)):
            zcopy(it, slot).start()

        zrel[0] = fold(s[idx(-Q)], it, range(n_plus))
        fcopy(it, 0).start()
        zrel[1] = fold(s[idx(Q)], it, range(n_plus, n_plus + n_minus))
        fcopy(it, 1).start()

        scalars = hook()

        total = fold(s[idx(0)], it, range(n_plus + n_minus, len(first_step)))
        for slot in range(2):
            fcopy(it, slot).wait_recv()
            total = total + zfin[it, slot]

        if it:
            step, ratio = scalars
            rest = qg[...] - step * total
            total = rest + ratio * qd[...]
        else:
            rest = total

        if last:
            sq = jnp.sum(total * total, axis=0, keepdims=True)
        else:
            sq = None
            qg[...] = rest
            qd[...] = total
            img[it, c, idx(0)] = total
            for m in range(n_own):
                gcopy(it, m).start()
            icopy(it, 0).start()
            gwait(it, -Q)
            for m in range(n_own, n_own + Q):
                gcopy(it, m).start()
            gwait(it, Q)
            for m in range(n_own + Q, len(gather)):
                gcopy(it, m).start()
            icopy(it, Q).start()
            icopy(it, -Q).start()
            for o in near[1:-1]:
                gwait(it, o)
                icopy(it, o).start()

            for o in near:
                icopy(it, o).wait_recv()
            for h in range(2):
                put_cat(slice(h * quarter, (h + 1) * quarter), img[it, h, :NP].reshape(quarter, E))

            @pl.loop(0, nch)
            def _(ch):
                r0 = pl.multiple_of(ch * (per * BR), per * BR)
                y = dot(gthi[pl.ds(r0, per * BR), :half], cat_r[:half, :])
                y = y[:, :E] + y[:, E:] + dot(gtlo[pl.ds(r0, per * BR), :half], cat_r[:half, 0:E])
                bs[it + 1, pl.ds(ch * per, per)] = y.reshape(per, BR, E)

        return sq

    def forward_end(it):
        for k in range(2):
            dcopy(it, k).wait_send()
        for slot in range(len(first_step)):
            zcopy(it, slot).wait_send()
        for slot in range(2):
            fcopy(it, slot).wait_send()
        if it < ITERS - 1:
            for m in range(len(gather)):
                gcopy(it, m).wait_send()

            for o in pieces:
                icopy(it, o).wait_send()

    def halo_wait(it):
        @pl.when(has_l)
        def _():
            hcopy_r(it).wait_recv()

        @pl.when(has_r)
        def _():
            hcopy_l(it).wait_recv()

        @pl.when(has_r)
        def _():
            hcopy_r(it).wait_send()

        @pl.when(has_l)
        def _():
            hcopy_l(it).wait_send()

    def laplace():
        for r0, n, v in ((0, BAND, hd[0]), (BAND, cols, d[...]), (BAND + cols, BAND, hd[1])):
            hi, lo = split(v)
            cat_e[r0:r0 + n, 0:E] = hi
            cat_e[r0:r0 + n, E:2 * E] = lo

    def lap_rows(i):
        r0 = pl.multiple_of(i * BAND, BAND)
        y = dot(lm[pl.ds(r0, BAND), :], cat_e[...])
        return r0, weight * (y[:, :E] + y[:, E:])

    def wcopy_l(it):
        return rcopy(wext.at[pl.ds(0, BAND)], wr.at[it, 1], pair(sem_w, it, 1), at(obs, pat - 1))

    def wcopy_r(it):
        return rcopy(wext.at[pl.ds(BAND + cols, BAND)], wr.at[it, 0], pair(sem_w, it, 0), at(obs, pat + 1))

    def reg_start(it):
        laplace()

        @pl.loop(0, CB)
        def _(i):
            r0, u = lap_rows(i)
            hi, lo = split(u)
            cat_d[pl.ds(r0, BAND), 0:E] = hi
            cat_d[pl.ds(r0, BAND), E:2 * E] = lo

        @pl.loop(0, CB + 2)
        def _(i):
            r0 = pl.multiple_of(i * BAND, BAND)
            y = dot(lmt[pl.ds(r0, BAND), :], cat_d[...])
            wext[pl.ds(r0, BAND), :] = weight * (y[:, :E] + y[:, E:])

        @pl.when(has_l)
        def _():
            wcopy_l(it).start()

        @pl.when(has_r)
        def _():
            wcopy_r(it).start()

    def reg_end(it):
        a[...] = ag[it + 1] + wext[BAND:BAND + cols, :]

        @pl.when(has_l)
        def _():
            wcopy_r(it).wait_recv()

        @pl.when(has_r)
        def _():
            wcopy_l(it).wait_recv()

        a[0:BAND, :] += wr[it, 0]
        a[cols - BAND:cols, :] += wr[it, 1]

    def reg_done(it):
        @pl.when(has_l)
        def _():
            wcopy_l(it).wait_send()

        @pl.when(has_r)
        def _():
            wcopy_r(it).wait_send()

    def ccopy(it):
        return rcopy(scs.at[it], scp.at[it], pair(sem_c, it), at(obs, partner))

    def scopy(it, k, slot):
        return rcopy(scz.at[it], scr.at[it, slot], (sem_s.at[0, it, k], sem_s.at[1, it, slot]), zat(k))

    def sums_mid(it):
        ccopy(it).wait_recv()
        scz[it] = scs[it] + scp[it]
        scr[it, z] = scs[it] + scp[it]

        @pl.loop(1, nz)
        def _(k):
            scopy(it, k, z).start()

    def sums_end(it):
        @pl.loop(1, nz)
        def _(k):
            scopy(it, k, (z - turn * k + nz) % nz).wait_recv()

        return jnp.sum(scr[it], axis=0)

    def sums_done(it):
        ccopy(it).wait_send()

        @pl.loop(1, nz)
        def _(k):
            scopy(it, k, z).wait_send()

    def pcopy(q, slot):
        return rcopy(pls, plr.at[slot], (sem_p.at[0, q], sem_p.at[1, slot]), at(obs, q))

    def qcopy(o, slot):
        return rcopy(qls, qlr.at[slot], (sem_q.at[0, o], sem_q.at[1, slot]), at(o, pat))

    def rowsum(x):
        return jnp.sum(x, axis=0, keepdims=True)

    norms, regs = [], []

    def dots(it):
        gv, dv, av = g[...], d[...], a[...]
        scs[it, 0:1, :] = rowsum(gv * gv)
        scs[it, 1:2, :] = rowsum(dv * av)
        scs[it, 2:3, :] = rowsum(gv * av)
        scs[it, 3:4, :] = rowsum(av * av)
        ccopy(it).start()

    def first():
        halo_wait(0)
        hg[...] = hal[0]
        hd[...] = hal[0]

    def advance(it):
        tot = sums_end(it - 1)
        if it == 1:
            norms.append(tot[0:1])
        norm = norms[-1]
        step = norm / tot[1:2]
        after = norm - 2.0 * step * tot[2:3] + step * step * tot[3:4]
        ratio = after / norm
        norms.append(after)
        halo_wait(it)
        if it == 1:
            slip[...] = step * d[...]
        else:
            slip[...] += step * d[...]
        g[...] = g[...] - step * a[...]
        d[...] = g[...] + ratio * d[...]
        hg[...] = hg[...] - step * hal[it]
        hd[...] = hg[...] + ratio * hd[...]
        if it == ITERS - 1:
            laplace()

            _, u = lap_rows(jnp.minimum(obs, CB - 1))
            regs.append(jnp.where(obs < CB, rowsum(u * u), 0.0))
            for k, (src, dst) in enumerate(((slip, slip_h), (d, d_h))):
                pltpu.make_async_copy(src, dst, sem_o.at[k]).start()
        return step, ratio

    backward(0, build_laplace)
    g[...] = ag[0]
    d[...] = ag[0]
    forward(0, first)
    for it in range(1, ITERS):
        backward(it, functools.partial(reg_start, it - 1))
        forward_end(it - 1)
        reg_end(it - 1)
        sq = forward(it, functools.partial(advance, it))
        reg_done(it - 1)
    last = ITERS - 1
    norm = norms[-1]
    sq = sq + regs[0]
    pls[...] = sq
    plr[pat] = sq

    @pl.loop(1, n_patch)
    def _(i):
        pcopy((pat + i) % n_patch, pat).start()

    forward_end(last)
    for it in range(ITERS):
        backward_end(it)
    for it in range(ITERS - 1):
        sums_done(it)

    @pl.loop(1, n_patch)
    def _(i):
        q = (pat + i) % n_patch
        pcopy(q, q).wait_recv()

    line = jnp.sum(plr[...], axis=0)
    qls[...] = line
    qlr[obs] = line

    @pl.loop(1, n_obs)
    def _(i):
        qcopy((obs + i) % n_obs, obs).start()

    @pl.loop(1, n_patch)
    def _(i):
        pcopy((pat + i) % n_patch, pat).wait_send()

    for k, (src, dst) in enumerate(((slip, slip_h), (d, d_h))):
        pltpu.make_async_copy(src, dst, sem_o.at[k]).wait()

    @pl.loop(1, n_obs)
    def _(i):
        o = (obs + i) % n_obs
        qcopy(o, o).wait_recv()

    scale[...] = norm / jnp.sum(qlr[...], axis=0)

    @pl.loop(1, n_obs)
    def _(i):
        qcopy((obs + i) % n_obs, obs).wait_send()


def shards(green, data, neighbours, reg_weight):
    rows, cols = green.shape
    E = data.shape[1]
    n_obs, n_patch = lax.axis_size("obs"), lax.axis_size("patch")
    nz = n_patch // 2
    nd = 2
    R, BR, ext = rows // 2 // nz, cols // n_obs, cols + 2 * BAND
    first = 4 * (nz // 4) - 3
    V = pltpu.VMEM
    D = pltpu.SemaphoreType.DMA
    scratch = [
        V((rows, cols), F32), V((rows, E), F32), V(neighbours.shape, jnp.int32), V((1, E), F32),
        V((rows, cols), BF16), V((rows, cols), BF16),
        V((cols, rows), BF16), V((cols, rows), BF16),
        V((cols, ext), BF16), V((ext, cols), BF16),
        V((cols, 2 * E), BF16), V((rows, 2 * E), BF16), V((ext, 2 * E), BF16),
        V((cols, E), F32), V((cols, E), F32), V((cols, E), F32), V((ext, E), F32), V((cols, E), F32),
        V((2, BAND, E), F32), V((2, BAND, E), F32), V((R, E), F32), V((R, E), F32),
        V((nz, R, E), F32), V((nz, R, E), F32), V((ITERS, nd, nz // nd, R, E), F32),
        V((ITERS, first, R, E), F32), V((2, R, E), F32), V((ITERS, 2, R, E), F32),
        V((ITERS - 1, 2, nz, R, E), F32),
        V((ITERS, n_obs, BR, E), F32), V((ITERS, n_obs, BR, E), F32), V((ITERS, cols, E), F32),
        V((ITERS, 2, BAND, E), F32), V((ITERS - 1, 2, BAND, E), F32),
        V((ITERS - 1, 4, E), F32), V((ITERS - 1, 4, E), F32), V((ITERS - 1, 4, E), F32), V((ITERS - 1, nz, 4, E), F32),
        V((1, E), F32), V((n_patch, 1, E), F32), V((1, E), F32), V((n_obs, 1, E), F32),
        D((2, n_patch + 1)), D((2,)),
        D((2, ITERS, nd)), D((2, ITERS, first)), D((2, ITERS, 2)), D((2, ITERS - 1, nz)), D((2, ITERS - 1, nz)),
        D((2, ITERS, n_obs)), D((2, ITERS, n_obs)), D((2, ITERS, 2)), D((2, ITERS - 1, 2)),
        D((2, ITERS - 1)), D((2, ITERS - 1, nz)), D((2, n_patch)), D((2, n_obs)),
    ]
    anywhere = pl.BlockSpec(memory_space=pl.ANY)
    slip, d, scale = pl.pallas_call(
        functools.partial(kernel, n_obs, n_patch),
        out_shape=[jax.ShapeDtypeStruct((cols, E), F32)] * 2 + [jax.ShapeDtypeStruct((1, E), F32)],
        in_specs=[anywhere] * 4,
        out_specs=[anywhere, anywhere, pl.BlockSpec(memory_space=pltpu.VMEM)],
        scratch_shapes=scratch,
        compiler_params=pltpu.CompilerParams(
            collective_id=0, has_side_effects=True, vmem_limit_bytes=56 * 1024 * 1024),
    )(green, data, neighbours, reg_weight.reshape(1, E))
    return slip + scale * d


def solution(mesh):
    in_specs = (P("obs", "patch"), P("obs", None), P(None, "patch"), P())
    return jax.shard_map(shards, mesh=mesh, in_specs=in_specs, out_specs=P("patch", None), check_vma=False)
```

```python
import functools
import math

import jax
import jax.numpy as jnp
from jax import lax
from jax.experimental import pallas as pl
from jax.experimental.pallas import tpu as pltpu
from jax.sharding import PartitionSpec as P

BAND = 128
ITERS = 3
MESH = pl.DeviceIdType.MESH
F32 = jnp.float32
BF16 = jnp.bfloat16


def dot(a, b):
    return lax.dot_general(a, b, (((1,), (0,)), ((), ())), preferred_element_type=F32)


def split(x):
    hi = x.astype(BF16)
    return hi, (x - hi.astype(F32)).astype(BF16)


def kernel(n_obs, n_patch, green_h, data_h, nb_h, rw_h, slip_h, d_h, scale,
           green, data, nb, rw,
           ghi, glo, gthi, gtlo, lm, lmt, cat_d, cat_r, cat_e,
           d, g, a, wext, slip, hd, hg, qd, qg,
           pf, s, rd, zr, zrel, zfin, img, bs, br, ag, hal, wr, scs, scp, scz, scr, pls, plr, qls, qlr,
           sem_l, sem_o, sem_d, sem_z, sem_f, sem_g, sem_i, sem_b, sem_a, sem_h, sem_w, sem_c, sem_s, sem_p, sem_q, go):
    rows, cols = green.shape
    E = data.shape[1]
    nz = n_patch // 2
    R = rows // 2 // nz
    BR = cols // n_obs
    half = rows // 2
    per = nch = math.isqrt(n_obs)
    CB = cols // BAND
    Q = nz // 4
    plus = list(range(1, Q + 1))
    minus = list(range(1, Q))
    near = [0] + [sgn * k for k in minus for sgn in (1, -1)] + [Q]
    far = [2 * Q] + [sgn * k for k in range(2 * Q - 1, Q, -1) for sgn in (1, -1)] + [-Q]
    pieces = near + far
    NP = len(near)
    quarter = half // 2

    def wrapped(o):
        return (o + 2 * Q - 1) % nz - 2 * Q + 1

    def idx(o):
        return pieces.index(wrapped(o))
    obs = lax.axis_index("obs")
    pat = lax.axis_index("patch")
    z = pat // 2
    c = pat % 2
    other = 1 - c
    partner = z * 2 + other
    has_l, has_r = pat > 0, pat < n_patch - 1

    def at(o, q):
        return (o, q)

    def rcopy(src, dst, sems, dev):
        return pltpu.make_async_remote_copy(
            src_ref=src, dst_ref=dst, send_sem=sems[0], recv_sem=sems[1],
            device_id=dev, device_id_type=MESH)

    def pair(sem, *idx):
        return sem.at[(0,) + idx], sem.at[(1,) + idx]

    STEP = 2 * BAND
    ends = [-(-(r0 + STEP) // R) for r0 in range(0, rows, STEP)]

    def load(n):
        part, h, r = n // (2 * NP), n // NP % 2, n % NP
        o = pieces[part * NP + r]
        src = pl.multiple_of(h * half + (z + (1 - 2 * h) * o + nz) % nz * R, R)
        return [pltpu.make_async_copy(a_.at[pl.ds(src, R)], b_.at[pl.ds(n * R, R)], sem_l.at[k, sum(n >= e for e in ends)])
                for k, (a_, b_) in enumerate(((green_h, green), (data_h, data)))]

    small = [pltpu.make_async_copy(src, dst, sem_l.at[i, len(ends)])
             for i, (src, dst) in enumerate(((nb_h, nb), (rw_h, rw)))]
    barrier = pltpu.get_barrier_semaphore()

    def greet(o, q):
        pl.semaphore_signal(barrier, inc=1, device_id=at(o, q), device_id_type=MESH)

    def tell(k):
        pl.semaphore_signal(go.at[k], inc=1, device_id=at(obs, partner), device_id_type=MESH)

    def plane_entered():
        @pl.when(c == 0)
        def _():
            pl.semaphore_wait(barrier, 2 * n_obs - 1)
            tell(0)

        @pl.when(c == 1)
        def _():
            pl.semaphore_wait(go.at[0], 1)

    def line_entered():
        @pl.when(c == 1)
        def _():
            pl.semaphore_wait(barrier, n_patch - 1)
            tell(1)

        @pl.when(c == 0)
        def _():
            pl.semaphore_wait(go.at[1], 1)

    for n in range(2 * nz):
        if n == nz // 2:
            greet(obs, partner)

            @pl.loop(1, n_obs)
            def _(i):
                greet((obs + i) % n_obs, z * 2)

            @pl.loop(1, nz)
            def _(k):
                greet(obs, (z + k) % nz * 2 + 1)

        for copy in load(n):
            copy.start()

    for copy in small:
        copy.start()

    def put_cat(where, value):
        hi, lo = split(value)
        cat_r[where, 0:E] = hi
        cat_r[where, E:2 * E] = lo

    def product(m0, m1, k0, k1):
        y = dot(gthi[m0:m1, k0:k1], cat_r[k0:k1, :])
        y = y[:, :E] + y[:, E:] + dot(gtlo[m0:m1, k0:k1], cat_r[k0:k1, 0:E])
        return y.reshape((m1 - m0) // BR, BR, E)

    def first_product(r0):
        y = product(0, cols, r0, r0 + STEP)
        if r0 == 0:
            bs[0] = y
        else:
            bs[0] += y

    loaded = 0
    for n, r0 in enumerate(range(0, rows, STEP)):
        span = pl.ds(loaded * R, (ends[n] - loaded) * R)
        for k, (a_, b_) in enumerate(((green_h, green), (data_h, data))):
            pltpu.make_async_copy(a_.at[span], b_.at[span], sem_l.at[k, n]).wait()
        loaded = ends[n]
        if r0:
            first_product(r0 - STEP)
        for r in range(r0, r0 + STEP, BAND):
            block = green[r:r + BAND, :]
            hi, lo = split(block)
            ghi[r:r + BAND, :] = hi
            glo[r:r + BAND, :] = lo
            hi, lo = split(block.T)
            gthi[:, r:r + BAND] = hi
            gtlo[:, r:r + BAND] = lo
            put_cat(slice(r, r + BAND), data[r:r + BAND, :])

    first_product(rows - STEP)

    for copy in small:
        copy.wait()
    weight = rw[...]

    zero_h = jnp.zeros((BAND, E), F32)

    @pl.when(pat == 0)
    def _():
        for it in range(ITERS):
            hal[it, 0] = zero_h
        for it in range(ITERS - 1):
            wr[it, 0] = zero_h

    @pl.when(pat == n_patch - 1)
    def _():
        for it in range(ITERS):
            hal[it, 1] = zero_h
        for it in range(ITERS - 1):
            wr[it, 1] = zero_h

    def build_laplace():
        @pl.loop(0, CB + 2)
        def _(j):
            r0 = pl.multiple_of(j * BAND, BAND)
            col = lax.broadcasted_iota(jnp.int32, (BAND, cols), 0) + j * BAND
            own = lax.broadcasted_iota(jnp.int32, (BAND, cols), 1) + BAND
            m = jnp.where(col == own, 4.0, 0.0)
            col = col + (pat * cols - BAND)
            for k in range(3):
                m = m - jnp.where(col == nb[k:k + 1, :], 1.0, 0.0)
            lmt[pl.ds(r0, BAND), :] = m.astype(BF16)
            lm[:, pl.ds(r0, BAND)] = m.T.astype(BF16)

    side = math.isqrt(n_obs)
    steps = sorted(range(side), key=lambda k: -min(k, side - k))
    far_first = sorted([(i, j) for i in steps for j in steps if i or j],
                       key=lambda ij: -sum(min(k, side - k) for k in ij))

    def shifted(i, j):
        return (obs // side + i) % side * side + (obs + j) % side

    def bcopy(b, o, slot):
        return rcopy(bs.at[b, o], br.at[b, slot], pair(sem_b, b), at(o, pat))

    def ball(b):
        return rcopy(bs.at[b, pl.ds(0, n_obs - 1)], br.at[b, pl.ds(0, n_obs - 1)], pair(sem_b, b), at(obs, partner))

    def acopy(b, o, slot):
        piece = ag.at[b, pl.ds(pl.multiple_of(slot * BR, BR), BR)]
        return rcopy(piece, piece, pair(sem_a, b), at(o, pat))

    def aall(b):
        block = ag.at[b, pl.ds(0, (n_obs - 1) * BR)]
        return rcopy(block, block, pair(sem_a, b), at(obs, partner))

    def backward(b, hook):
        if b == 0:
            plane_entered()

            for i, j in far_first:
                bcopy(b, shifted(i, j), obs).start()
        else:
            for i in range(NP, nz - 1):
                gall(b - 1, i, 1).wait_recv()
                icopy(b - 1, i).start()

            icopy(b - 1, NP, NP).wait_recv()

            for h in range(2):
                put_cat(slice(half + h * quarter, half + (h + 1) * quarter), img[b - 1, h, NP:].reshape(quarter, E))
            for i in steps:
                ch = (obs // side + i) % side
                r0 = pl.multiple_of(ch * (per * BR), per * BR)
                y = dot(gthi[pl.ds(r0, per * BR), half:], cat_r[half:, :])
                y = y[:, :E] + y[:, E:] + dot(gtlo[pl.ds(r0, per * BR), half:], cat_r[half:, 0:E])
                bs[b, pl.ds(ch * per, per)] += y.reshape(per, BR, E)
                for j in steps:
                    if i or j:
                        bcopy(b, shifted(i, j), obs).start()

        hook()

        ball(b).wait_recv()
        total = lax.fori_loop(1, n_obs, lambda i, acc: acc + br[b, (obs + i) % n_obs], bs[b, obs])
        ag[b, pl.ds(pl.multiple_of(obs * BR, BR), BR), :] = total

        for i, j in far_first:
            acopy(b, shifted(i, j), obs).start()

        if b == 0:
            line_entered()

        aall(b).wait_recv()

    def backward_end(b):
        ball(b).wait_send()
        aall(b).wait_send()

    def dcopy(it, k):
        return rcopy(pf.at[pl.ds(k * NP, NP)], rd.at[it, k], pair(sem_d, it, k), at(obs, partner))

    turn = 1 - 2 * c

    def zat(k):
        return at(obs, ((z + turn * k + nz) % nz) * 2 + c)

    first_step = ([(-k, -k - Q) for k in reversed(plus)] + [(k, k + Q) for k in reversed(minus)]
                  + [(-k, -k) for k in reversed(minus)] + [(k, k) for k in reversed(minus)])
    n_plus, n_minus = len(plus), len(minus)

    groups = [(0, n_plus), (n_plus, n_minus), (n_plus + n_minus, len(first_step) - n_plus - n_minus)]

    def zcopy(it, slot):
        k, o = first_step[slot]
        group = sum(slot >= first for first, _ in groups)
        return rcopy(s.at[idx(o)], zr.at[it, slot], (sem_z.at[it, 0], sem_z.at[it, group]), zat(k))

    def zall(it, group, first, n):
        block = zr.at[it, pl.ds(first, n)]
        return rcopy(block, block, (sem_z.at[it, 0], sem_z.at[it, group]), at(obs, partner))

    def fcopy(it, slot):
        return rcopy(zrel.at[slot], zfin.at[it, slot], pair(sem_f, it), zat(-Q if slot == 0 else Q))

    def fall(it):
        return rcopy(zrel, zfin.at[it], pair(sem_f, it), at(obs, partner))

    gather = ([(k, 0) for k in (-Q, Q)] + [(sgn * k, 0) for k in reversed(minus) for sgn in (1, -1)]
              + [(k, -Q) for k in reversed(plus)] + [(-k, Q) for k in reversed(minus)])
    n_own = 2 * Q

    def arrival(it, i):
        return sem_g.at[it, 1 if 0 < i < NP - 1 else i - NP + 3]

    def gcopy(it, m):
        k, o = gather[m]
        to = idx(o - k)
        return rcopy(img.at[it, c, idx(o)], img.at[it, c, to], (sem_g.at[it, 0], arrival(it, to)), zat(k))

    def gall(it, i, n):
        block = img.at[it, c, pl.ds(i, n)]
        return rcopy(block, block, (sem_g.at[it, 0], arrival(it, i)), at(obs, partner))

    def icopy(it, i, n=1):
        block = img.at[it, c, pl.ds(i, n)]
        return rcopy(block, block, (sem_i.at[it, 0], sem_i.at[it, 1 + i // NP]), at(obs, partner))

    def fold(acc, it, group):
        first, n = groups[group]
        zall(it, group + 1, first, n).wait_recv()
        for slot in range(first, first + n):
            acc = acc + zr[it, slot]
        return acc

    def hsrc(it):
        return a if it else ag.at[0]

    def hcopy_r(it):
        return rcopy(hsrc(it).at[pl.ds(cols - BAND, BAND)], hal.at[it, 0], pair(sem_h, it, 0), at(obs, pat + 1))

    def hcopy_l(it):
        return rcopy(hsrc(it).at[pl.ds(0, BAND)], hal.at[it, 1], pair(sem_h, it, 1), at(obs, pat - 1))

    def forward(it, hook):
        last = it == ITERS - 1

        hi, lo = split(hsrc(it)[...])
        cat_d[:, 0:E] = hi
        cat_d[:, E:2 * E] = lo

        def part(h, k):
            r0 = pl.multiple_of(k * half + h * quarter, quarter)
            y = dot(ghi[pl.ds(r0, quarter), :], cat_d[...])
            y = y[:, :E] + y[:, E:] + dot(glo[pl.ds(r0, quarter), :], cat_d[:, 0:E])
            return y.reshape(NP, R, E)

        for k in (1, 0):
            pf[k * NP:(k + 1) * NP] = part(other, k)
            dcopy(it, k).start()

        if it:
            dots(it - 1)

        for k in (1, 0):
            s[k * NP:(k + 1) * NP] = part(c, k)

        dcopy(it, 1).wait_recv()
        s[NP:] += rd[it, 1]
        for slot in range(n_plus + n_minus):
            zcopy(it, slot).start()
        dcopy(it, 0).wait_recv()
        s[:NP] += rd[it, 0]

        if it:
            sums_mid(it - 1)

        @pl.when(has_r)
        def _():
            hcopy_r(it).start()

        @pl.when(has_l)
        def _():
            hcopy_l(it).start()

        for slot in range(n_plus + n_minus, len(first_step)):
            zcopy(it, slot).start()

        zrel[0] = fold(s[idx(-Q)], it, 0)
        fcopy(it, 0).start()
        zrel[1] = fold(s[idx(Q)], it, 1)
        fcopy(it, 1).start()

        scalars = hook()

        total = fold(s[idx(0)], it, 2)
        fall(it).wait_recv()
        total = total + zfin[it, 0] + zfin[it, 1]

        if it:
            step, ratio = scalars
            rest = qg[...] - step * total
            total = rest + ratio * qd[...]
        else:
            rest = total

        if last:
            sq = jnp.sum(total * total, axis=0, keepdims=True)
        else:
            sq = None
            qg[...] = rest
            qd[...] = total
            img[it, c, idx(0)] = total
            for m in range(n_own):
                gcopy(it, m).start()
            icopy(it, 0).start()
            gall(it, idx(-Q), 1).wait_recv()
            for m in range(n_own, n_own + Q):
                gcopy(it, m).start()
            gall(it, idx(Q), 1).wait_recv()
            for m in range(n_own + Q, len(gather)):
                gcopy(it, m).start()
            icopy(it, idx(Q)).start()
            icopy(it, idx(-Q)).start()
            gall(it, 1, NP - 2).wait_recv()
            icopy(it, 1, NP - 2).start()

            icopy(it, 0, NP).wait_recv()
            for h in range(2):
                put_cat(slice(h * quarter, (h + 1) * quarter), img[it, h, :NP].reshape(quarter, E))

            @pl.loop(0, nch)
            def _(ch):
                r0 = pl.multiple_of(ch * (per * BR), per * BR)
                y = dot(gthi[pl.ds(r0, per * BR), :half], cat_r[:half, :])
                y = y[:, :E] + y[:, E:] + dot(gtlo[pl.ds(r0, per * BR), :half], cat_r[:half, 0:E])
                bs[it + 1, pl.ds(ch * per, per)] = y.reshape(per, BR, E)

        return sq

    def forward_end(it):
        for k in range(2):
            dcopy(it, k).wait_send()
        zall(it, 1, 0, len(first_step)).wait_send()
        fall(it).wait_send()
        if it < ITERS - 1:
            gall(it, 0, nz - 1).wait_send()
            icopy(it, 0, nz).wait_send()

    def halo_wait(it):
        @pl.when(has_l)
        def _():
            hcopy_r(it).wait_recv()

        @pl.when(has_r)
        def _():
            hcopy_l(it).wait_recv()

        @pl.when(has_r)
        def _():
            hcopy_r(it).wait_send()

        @pl.when(has_l)
        def _():
            hcopy_l(it).wait_send()

    def laplace():
        for r0, n, v in ((0, BAND, hd[0]), (BAND, cols, d[...]), (BAND + cols, BAND, hd[1])):
            hi, lo = split(v)
            cat_e[r0:r0 + n, 0:E] = hi
            cat_e[r0:r0 + n, E:2 * E] = lo

    def lap_rows(i):
        r0 = pl.multiple_of(i * BAND, BAND)
        y = dot(lm[pl.ds(r0, BAND), :], cat_e[...])
        return r0, weight * (y[:, :E] + y[:, E:])

    def wcopy_l(it):
        return rcopy(wext.at[pl.ds(0, BAND)], wr.at[it, 1], pair(sem_w, it, 1), at(obs, pat - 1))

    def wcopy_r(it):
        return rcopy(wext.at[pl.ds(BAND + cols, BAND)], wr.at[it, 0], pair(sem_w, it, 0), at(obs, pat + 1))

    def reg_start(it):
        laplace()

        @pl.loop(0, CB)
        def _(i):
            r0, u = lap_rows(i)
            hi, lo = split(u)
            cat_d[pl.ds(r0, BAND), 0:E] = hi
            cat_d[pl.ds(r0, BAND), E:2 * E] = lo

        @pl.loop(0, CB + 2)
        def _(i):
            r0 = pl.multiple_of(i * BAND, BAND)
            y = dot(lmt[pl.ds(r0, BAND), :], cat_d[...])
            wext[pl.ds(r0, BAND), :] = weight * (y[:, :E] + y[:, E:])

        @pl.when(has_l)
        def _():
            wcopy_l(it).start()

        @pl.when(has_r)
        def _():
            wcopy_r(it).start()

    def reg_end(it):
        a[...] = ag[it + 1] + wext[BAND:BAND + cols, :]

        @pl.when(has_l)
        def _():
            wcopy_r(it).wait_recv()

        @pl.when(has_r)
        def _():
            wcopy_l(it).wait_recv()

        a[0:BAND, :] += wr[it, 0]
        a[cols - BAND:cols, :] += wr[it, 1]

    def reg_done(it):
        @pl.when(has_l)
        def _():
            wcopy_l(it).wait_send()

        @pl.when(has_r)
        def _():
            wcopy_r(it).wait_send()

    def ccopy(it):
        return rcopy(scs.at[it], scp.at[it], pair(sem_c, it), at(obs, partner))

    def scopy(it, k, slot):
        return rcopy(scz.at[it], scr.at[it, slot], pair(sem_s, it), zat(k))

    def sall(it):
        block = scr.at[it, pl.ds(0, nz - 1)]
        return rcopy(block, block, pair(sem_s, it), at(obs, partner))

    def sums_mid(it):
        ccopy(it).wait_recv()
        scz[it] = scs[it] + scp[it]
        scr[it, z] = scs[it] + scp[it]

        @pl.loop(1, nz)
        def _(k):
            scopy(it, k, z).start()

    def sums_end(it):
        sall(it).wait_recv()
        return jnp.sum(scr[it], axis=0)

    def sums_done(it):
        ccopy(it).wait_send()
        sall(it).wait_send()

    def pcopy(q, slot):
        return rcopy(pls, plr.at[slot], pair(sem_p), at(obs, q))

    def qcopy(o, core, slot):
        return rcopy(qls, qlr.at[slot], pair(sem_q), at(o, 2 * z + core))

    def rows_of(sem, n):
        block = plr.at[pl.ds(0, n)]
        return rcopy(block, block, pair(sem), at(obs, partner))

    def rowsum(x):
        return jnp.sum(x, axis=0, keepdims=True)

    norms, regs = [], []

    def dots(it):
        gv, dv, av = g[...], d[...], a[...]
        scs[it, 0:1, :] = rowsum(gv * gv)
        scs[it, 1:2, :] = rowsum(dv * av)
        scs[it, 2:3, :] = rowsum(gv * av)
        scs[it, 3:4, :] = rowsum(av * av)
        ccopy(it).start()

    def first():
        halo_wait(0)
        hg[...] = hal[0]
        hd[...] = hal[0]

    def advance(it):
        tot = sums_end(it - 1)
        if it == 1:
            norms.append(tot[0:1])
        norm = norms[-1]
        step = norm / tot[1:2]
        after = norm - 2.0 * step * tot[2:3] + step * step * tot[3:4]
        ratio = after / norm
        norms.append(after)
        halo_wait(it)
        if it == 1:
            slip[...] = step * d[...]
        else:
            slip[...] += step * d[...]
        g[...] = g[...] - step * a[...]
        d[...] = g[...] + ratio * d[...]
        hg[...] = hg[...] - step * hal[it]
        hd[...] = hg[...] + ratio * hd[...]
        if it == ITERS - 1:
            laplace()

            _, u = lap_rows(jnp.minimum(obs, CB - 1))
            regs.append(jnp.where(obs < CB, rowsum(u * u), 0.0))
            for k, (src, dst) in enumerate(((slip, slip_h), (d, d_h))):
                pltpu.make_async_copy(src, dst, sem_o.at[k]).start()
        return step, ratio

    backward(0, build_laplace)
    g[...] = ag[0]
    d[...] = ag[0]
    forward(0, first)
    for it in range(1, ITERS):
        backward(it, functools.partial(reg_start, it - 1))
        forward_end(it - 1)
        reg_end(it - 1)
        sq = forward(it, functools.partial(advance, it))
        reg_done(it - 1)
    last = ITERS - 1
    norm = norms[-1]
    sq = sq + regs[0]
    pls[...] = sq

    @pl.loop(c, nz)
    def _(k):
        pcopy((z + k) % nz * 2 + 1, pat).start()

    forward_end(last)
    for it in range(ITERS):
        backward_end(it)
    for it in range(ITERS - 1):
        sums_done(it)

    @pl.when(c == 1)
    def _():
        plr[pat] = sq

        rows_of(sem_p, n_patch - 1).wait_recv()

    @pl.when(c == 1)
    def _():
        line = jnp.sum(plr[...], axis=0)
        qls[...] = line
        qlr[obs] = line
        for i, j in far_first:
            for core in range(2):
                qcopy(shifted(i, j), core, obs).start()
        qcopy(obs, 0, obs).start()

    for core in range(2):
        @pl.when(c == core)
        def _():
            rows_of(sem_p, nz - core).wait_send()

    for k, (src, dst) in enumerate(((slip, slip_h), (d, d_h))):
        pltpu.make_async_copy(src, dst, sem_o.at[k]).wait()

    for core in range(2):
        @pl.when(c == core)
        def _():
            rows_of(sem_q, n_obs - core).wait_recv()

    scale[...] = norm / jnp.sum(qlr[...], axis=0)

    @pl.when(c == 1)
    def _():
        rows_of(sem_q, 2 * n_obs - 1).wait_send()


def shards(green, data, neighbours, reg_weight):
    rows, cols = green.shape
    E = data.shape[1]
    n_obs, n_patch = lax.axis_size("obs"), lax.axis_size("patch")
    nz = n_patch // 2
    nd = 2
    R, BR, ext = rows // 2 // nz, cols // n_obs, cols + 2 * BAND
    first = 4 * (nz // 4) - 3
    V = pltpu.VMEM
    D = pltpu.SemaphoreType.DMA
    scratch = [
        V((rows, cols), F32), V((rows, E), F32), V(neighbours.shape, jnp.int32), V((1, E), F32),
        V((rows, cols), BF16), V((rows, cols), BF16),
        V((cols, rows), BF16), V((cols, rows), BF16),
        V((cols, ext), BF16), V((ext, cols), BF16),
        V((cols, 2 * E), BF16), V((rows, 2 * E), BF16), V((ext, 2 * E), BF16),
        V((cols, E), F32), V((cols, E), F32), V((cols, E), F32), V((ext, E), F32), V((cols, E), F32),
        V((2, BAND, E), F32), V((2, BAND, E), F32), V((R, E), F32), V((R, E), F32),
        V((nz, R, E), F32), V((nz, R, E), F32), V((ITERS, nd, nz // nd, R, E), F32),
        V((ITERS, first, R, E), F32), V((2, R, E), F32), V((ITERS, 2, R, E), F32),
        V((ITERS - 1, 2, nz, R, E), F32),
        V((ITERS, n_obs, BR, E), F32), V((ITERS, n_obs, BR, E), F32), V((ITERS, cols, E), F32),
        V((ITERS, 2, BAND, E), F32), V((ITERS - 1, 2, BAND, E), F32),
        V((ITERS - 1, 4, E), F32), V((ITERS - 1, 4, E), F32), V((ITERS - 1, 4, E), F32), V((ITERS - 1, nz, 4, E), F32),
        V((1, E), F32), V((n_patch, 1, E), F32), V((1, E), F32), V((n_obs, 1, E), F32),
        D((2, rows // (2 * BAND) + 1)), D((2,)),
        D((2, ITERS, nd)), D((ITERS, 4)), D((2, ITERS)), D((ITERS - 1, nz - nz // 2 + 3)), D((ITERS - 1, 3)),
        D((2, ITERS)), D((2, ITERS)), D((2, ITERS, 2)), D((2, ITERS - 1, 2)),
        D((2, ITERS - 1)), D((2, ITERS - 1)), D((2,)), D((2,)), pltpu.SemaphoreType.REGULAR((2,)),
    ]
    anywhere = pl.BlockSpec(memory_space=pl.ANY)
    slip, d, scale = pl.pallas_call(
        functools.partial(kernel, n_obs, n_patch),
        out_shape=[jax.ShapeDtypeStruct((cols, E), F32)] * 2 + [jax.ShapeDtypeStruct((1, E), F32)],
        in_specs=[anywhere] * 4,
        out_specs=[anywhere, anywhere, pl.BlockSpec(memory_space=pltpu.VMEM)],
        scratch_shapes=scratch,
        compiler_params=pltpu.CompilerParams(
            collective_id=0, has_side_effects=True, vmem_limit_bytes=56 * 1024 * 1024),
    )(green, data, neighbours, reg_weight.reshape(1, E))
    return slip + scale * d


def solution(mesh):
    in_specs = (P("obs", "patch"), P("obs", None), P(None, "patch"), P())
    return jax.shard_map(shards, mesh=mesh, in_specs=in_specs, out_specs=P("patch", None), check_vma=False)
```

```python
import functools
import math

import jax
import jax.numpy as jnp
from jax import lax
from jax.experimental import pallas as pl
from jax.experimental.pallas import tpu as pltpu
from jax.sharding import PartitionSpec as P

BAND = 128
ITERS = 3
MESH = pl.DeviceIdType.MESH
F32 = jnp.float32
BF16 = jnp.bfloat16


def dot(a, b):
    return lax.dot_general(a, b, (((1,), (0,)), ((), ())), preferred_element_type=F32)


def split(x):
    hi = x.astype(BF16)
    return hi, (x - hi.astype(F32)).astype(BF16)


def kernel(n_obs, n_patch, green_h, data_h, nb_h, rw_h, slip_h, d_h, scale,
           green, data, nb, rw,
           ghi, glo, gthi, gtlo, lm, lmt, cat_d, cat_r, cat_e,
           d, g, a, wext, slip, hd, hg, qd, qg,
           pf, s, rd, zr, zrel, zfin, img, bs, br, ag, hal, wr, scs, scp, scz, scr, tots, pls, plr, qls, qlr,
           sem_l, sem_o, sem_d, sem_z, sem_f, sem_g, sem_i, sem_b, sem_a, sem_h, sem_w, sem_c, sem_s, sem_t, sem_p, sem_q, go):
    rows, cols = green.shape
    E = data.shape[1]
    nz = n_patch // 2
    R = rows // 2 // nz
    BR = cols // n_obs
    half = rows // 2
    per = nch = math.isqrt(n_obs)
    CB = cols // BAND
    Q = nz // 4
    plus = list(range(1, Q + 1))
    minus = list(range(1, Q))
    near = [0] + [sgn * k for k in minus for sgn in (1, -1)] + [Q]
    far = [2 * Q] + [sgn * k for k in range(2 * Q - 1, Q, -1) for sgn in (1, -1)] + [-Q]
    pieces = near + far
    NP = len(near)
    quarter = half // 2

    def wrapped(o):
        return (o + 2 * Q - 1) % nz - 2 * Q + 1

    def idx(o):
        return pieces.index(wrapped(o))
    obs = lax.axis_index("obs")
    pat = lax.axis_index("patch")
    z = pat // 2
    c = pat % 2
    other = 1 - c
    partner = z * 2 + other
    has_l, has_r = pat > 0, pat < n_patch - 1

    def at(o, q):
        return (o, q)

    def rcopy(src, dst, sems, dev):
        return pltpu.make_async_remote_copy(
            src_ref=src, dst_ref=dst, send_sem=sems[0], recv_sem=sems[1],
            device_id=dev, device_id_type=MESH)

    def pair(sem, *idx):
        return sem.at[(0,) + idx], sem.at[(1,) + idx]

    STEP = 2 * BAND
    ends = [-(-(r0 + STEP) // R) for r0 in range(0, rows, STEP)]

    def load(n):
        part, h, r = n // (2 * NP), n // NP % 2, n % NP
        o = pieces[part * NP + r]
        src = pl.multiple_of(h * half + (z + (1 - 2 * h) * o + nz) % nz * R, R)
        return [pltpu.make_async_copy(a_.at[pl.ds(src, R)], b_.at[pl.ds(n * R, R)], sem_l.at[k, sum(n >= e for e in ends)])
                for k, (a_, b_) in enumerate(((green_h, green), (data_h, data)))]

    small = [pltpu.make_async_copy(src, dst, sem_l.at[i, len(ends)])
             for i, (src, dst) in enumerate(((nb_h, nb), (rw_h, rw)))]
    barrier = pltpu.get_barrier_semaphore()

    def greet(o, q):
        pl.semaphore_signal(barrier, inc=1, device_id=at(o, q), device_id_type=MESH)

    def tell(k):
        pl.semaphore_signal(go.at[k], inc=1, device_id=at(obs, partner), device_id_type=MESH)

    def plane_entered():
        @pl.when(c == 0)
        def _():
            pl.semaphore_wait(barrier, 2 * n_obs - 1)
            tell(0)

        @pl.when(c == 1)
        def _():
            pl.semaphore_wait(go.at[0], 1)

    def line_entered():
        @pl.when(c == 1)
        def _():
            pl.semaphore_wait(barrier, n_patch - 1)
            tell(1)

        @pl.when(c == 0)
        def _():
            pl.semaphore_wait(go.at[1], 1)

    for n in range(2 * nz):
        if n == nz // 2:
            greet(obs, partner)

            @pl.loop(1, n_obs)
            def _(i):
                greet((obs + i) % n_obs, z * 2)

            @pl.loop(1, nz)
            def _(k):
                greet(obs, (z + k) % nz * 2 + 1)

        for copy in load(n):
            copy.start()

    for copy in small:
        copy.start()

    def put_cat(where, value):
        hi, lo = split(value)
        cat_r[where, 0:E] = hi
        cat_r[where, E:2 * E] = lo

    def product(m0, m1, k0, k1):
        y = dot(gthi[m0:m1, k0:k1], cat_r[k0:k1, :])
        y = y[:, :E] + y[:, E:] + dot(gtlo[m0:m1, k0:k1], cat_r[k0:k1, 0:E])
        return y.reshape((m1 - m0) // BR, BR, E)

    def first_product(r0):
        y = product(0, cols, r0, r0 + STEP)
        if r0 == 0:
            bs[0] = y
        else:
            bs[0] += y

    loaded = 0
    for n, r0 in enumerate(range(0, rows, STEP)):
        span = pl.ds(loaded * R, (ends[n] - loaded) * R)
        for k, (a_, b_) in enumerate(((green_h, green), (data_h, data))):
            pltpu.make_async_copy(a_.at[span], b_.at[span], sem_l.at[k, n]).wait()
        loaded = ends[n]
        if r0:
            first_product(r0 - STEP)
        for r in range(r0, r0 + STEP, BAND):
            block = green[r:r + BAND, :]
            hi, lo = split(block)
            ghi[r:r + BAND, :] = hi
            glo[r:r + BAND, :] = lo
            hi, lo = split(block.T)
            gthi[:, r:r + BAND] = hi
            gtlo[:, r:r + BAND] = lo
            put_cat(slice(r, r + BAND), data[r:r + BAND, :])

    first_product(rows - STEP)

    for copy in small:
        copy.wait()
    weight = rw[...]

    zero_h = jnp.zeros((BAND, E), F32)

    @pl.when(pat == 0)
    def _():
        for it in range(ITERS):
            hal[it, 0] = zero_h
        for it in range(ITERS - 1):
            wr[it, 0] = zero_h

    @pl.when(pat == n_patch - 1)
    def _():
        for it in range(ITERS):
            hal[it, 1] = zero_h
        for it in range(ITERS - 1):
            wr[it, 1] = zero_h

    def build_laplace():
        @pl.loop(0, CB + 2)
        def _(j):
            r0 = pl.multiple_of(j * BAND, BAND)
            col = lax.broadcasted_iota(jnp.int32, (BAND, cols), 0) + j * BAND
            own = lax.broadcasted_iota(jnp.int32, (BAND, cols), 1) + BAND
            m = jnp.where(col == own, 4.0, 0.0)
            col = col + (pat * cols - BAND)
            for k in range(3):
                m = m - jnp.where(col == nb[k:k + 1, :], 1.0, 0.0)
            lmt[pl.ds(r0, BAND), :] = m.astype(BF16)
            lm[:, pl.ds(r0, BAND)] = m.T.astype(BF16)

    side = math.isqrt(n_obs)
    steps = sorted(range(side), key=lambda k: -min(k, side - k))
    far_first = sorted([(i, j) for i in steps for j in steps if i or j],
                       key=lambda ij: -sum(min(k, side - k) for k in ij))

    def shifted(i, j):
        return (obs // side + i) % side * side + (obs + j) % side

    def bcopy(b, o, slot):
        return rcopy(bs.at[b, o], br.at[b, slot], pair(sem_b, b), at(o, pat))

    def ball(b):
        return rcopy(bs.at[b, pl.ds(0, n_obs - 1)], br.at[b, pl.ds(0, n_obs - 1)], pair(sem_b, b), at(obs, partner))

    def acopy(b, o, slot):
        piece = ag.at[b, pl.ds(pl.multiple_of(slot * BR, BR), BR)]
        return rcopy(piece, piece, pair(sem_a, b), at(o, pat))

    def aall(b):
        block = ag.at[b, pl.ds(0, (n_obs - 1) * BR)]
        return rcopy(block, block, pair(sem_a, b), at(obs, partner))

    def backward(b, hook):
        if b == 0:
            plane_entered()

            for i, j in far_first:
                bcopy(b, shifted(i, j), obs).start()
        else:
            for i in range(NP, nz - 1):
                gall(b - 1, i, 1).wait_recv()
                icopy(b - 1, i).start()

            icopy(b - 1, NP, NP).wait_recv()

            for h in range(2):
                put_cat(slice(half + h * quarter, half + (h + 1) * quarter), img[b - 1, h, NP:].reshape(quarter, E))
            for i in steps:
                ch = (obs // side + i) % side
                r0 = pl.multiple_of(ch * (per * BR), per * BR)
                y = dot(gthi[pl.ds(r0, per * BR), half:], cat_r[half:, :])
                y = y[:, :E] + y[:, E:] + dot(gtlo[pl.ds(r0, per * BR), half:], cat_r[half:, 0:E])
                bs[b, pl.ds(ch * per, per)] += y.reshape(per, BR, E)
                for j in steps:
                    if i or j:
                        bcopy(b, shifted(i, j), obs).start()

        hook()

        ball(b).wait_recv()
        total = lax.fori_loop(1, n_obs, lambda i, acc: acc + br[b, (obs + i) % n_obs], bs[b, obs])
        ag[b, pl.ds(pl.multiple_of(obs * BR, BR), BR), :] = total

        for i, j in far_first:
            acopy(b, shifted(i, j), obs).start()

        if b == 0:
            line_entered()

        aall(b).wait_recv()

    def backward_end(b):
        ball(b).wait_send()
        aall(b).wait_send()

    def dcopy(it, k):
        return rcopy(pf.at[pl.ds(k * NP, NP)], rd.at[it, k], pair(sem_d, it, k), at(obs, partner))

    turn = 1 - 2 * c

    def zat(k):
        return at(obs, ((z + turn * k + nz) % nz) * 2 + c)

    first_step = ([(-k, -k - Q) for k in reversed(plus)] + [(k, k + Q) for k in reversed(minus)]
                  + [(-k, -k) for k in reversed(minus)] + [(k, k) for k in reversed(minus)])
    n_plus, n_minus = len(plus), len(minus)

    groups = [(0, n_plus), (n_plus, n_minus), (n_plus + n_minus, len(first_step) - n_plus - n_minus)]

    def zcopy(it, slot):
        k, o = first_step[slot]
        group = sum(slot >= first for first, _ in groups)
        return rcopy(s.at[idx(o)], zr.at[it, slot], (sem_z.at[it, 0], sem_z.at[it, group]), zat(k))

    def zall(it, group, first, n):
        block = zr.at[it, pl.ds(first, n)]
        return rcopy(block, block, (sem_z.at[it, 0], sem_z.at[it, group]), at(obs, partner))

    def fcopy(it, slot):
        return rcopy(zrel.at[slot], zfin.at[it, slot], pair(sem_f, it), zat(-Q if slot == 0 else Q))

    def fall(it):
        return rcopy(zrel, zfin.at[it], pair(sem_f, it), at(obs, partner))

    gather = ([(k, 0) for k in (-Q, Q)] + [(sgn * k, 0) for k in reversed(minus) for sgn in (1, -1)]
              + [(k, -Q) for k in reversed(plus)] + [(-k, Q) for k in reversed(minus)])
    n_own = 2 * Q

    def arrival(it, i):
        return sem_g.at[it, 1 if 0 < i < NP - 1 else i - NP + 3]

    def gcopy(it, m):
        k, o = gather[m]
        to = idx(o - k)
        return rcopy(img.at[it, c, idx(o)], img.at[it, c, to], (sem_g.at[it, 0], arrival(it, to)), zat(k))

    def gall(it, i, n):
        block = img.at[it, c, pl.ds(i, n)]
        return rcopy(block, block, (sem_g.at[it, 0], arrival(it, i)), at(obs, partner))

    def icopy(it, i, n=1):
        block = img.at[it, c, pl.ds(i, n)]
        return rcopy(block, block, (sem_i.at[it, 0], sem_i.at[it, 1 + i // NP]), at(obs, partner))

    def fold(acc, it, group):
        first, n = groups[group]
        zall(it, group + 1, first, n).wait_recv()
        for slot in range(first, first + n):
            acc = acc + zr[it, slot]
        return acc

    def hsrc(it):
        return a if it else ag.at[0]

    def hcopy_r(it):
        return rcopy(hsrc(it).at[pl.ds(cols - BAND, BAND)], hal.at[it, 0], pair(sem_h, it, 0), at(obs, pat + 1))

    def hcopy_l(it):
        return rcopy(hsrc(it).at[pl.ds(0, BAND)], hal.at[it, 1], pair(sem_h, it, 1), at(obs, pat - 1))

    def forward(it, hook):
        last = it == ITERS - 1

        hi, lo = split(hsrc(it)[...])
        cat_d[:, 0:E] = hi
        cat_d[:, E:2 * E] = lo

        def part(h, k):
            r0 = pl.multiple_of(k * half + h * quarter, quarter)
            y = dot(ghi[pl.ds(r0, quarter), :], cat_d[...])
            y = y[:, :E] + y[:, E:] + dot(glo[pl.ds(r0, quarter), :], cat_d[:, 0:E])
            return y.reshape(NP, R, E)

        for k in (1, 0):
            pf[k * NP:(k + 1) * NP] = part(other, k)
            dcopy(it, k).start()

        if it:
            dots(it - 1)

        for k in (1, 0):
            s[k * NP:(k + 1) * NP] = part(c, k)

        dcopy(it, 1).wait_recv()
        s[NP:] += rd[it, 1]
        for slot in range(n_plus + n_minus):
            zcopy(it, slot).start()
        dcopy(it, 0).wait_recv()
        s[:NP] += rd[it, 0]

        if it:
            sums_mid(it - 1)

        def halos():
            @pl.when(has_r)
            def _():
                hcopy_r(it).start()

            @pl.when(has_l)
            def _():
                hcopy_l(it).start()

        if last:
            halos()

        direct = range(n_plus + n_minus, len(first_step))
        for slot in direct:
            if abs(first_step[slot][0]) > 1:
                zcopy(it, slot).start()

        zrel[0] = fold(s[idx(-Q)], it, 0)
        fcopy(it, 0).start()
        zrel[1] = fold(s[idx(Q)], it, 1)
        fcopy(it, 1).start()

        for slot in direct:
            if abs(first_step[slot][0]) == 1:
                zcopy(it, slot).start()

        if not last:
            halos()

        scalars = hook()

        total = fold(s[idx(0)], it, 2)
        fall(it).wait_recv()
        total = total + zfin[it, 0] + zfin[it, 1]

        if it:
            step, ratio = scalars
            rest = qg[...] - step * total
            total = rest + ratio * qd[...]
        else:
            rest = total

        if last:
            sq = jnp.sum(total * total, axis=0, keepdims=True)
        else:
            sq = None
            qg[...] = rest
            qd[...] = total
            img[it, c, idx(0)] = total
            for m in range(n_own):
                gcopy(it, m).start()
            icopy(it, 0).start()
            halo_update(it, scalars)
            gall(it, idx(-Q), 1).wait_recv()
            for m in range(n_own, n_own + Q):
                gcopy(it, m).start()
            gall(it, idx(Q), 1).wait_recv()
            for m in range(n_own + Q, len(gather)):
                gcopy(it, m).start()
            icopy(it, idx(Q)).start()
            icopy(it, idx(-Q)).start()
            gall(it, 1, NP - 2).wait_recv()
            icopy(it, 1, NP - 2).start()

            icopy(it, 0, NP).wait_recv()
            for h in range(2):
                put_cat(slice(h * quarter, (h + 1) * quarter), img[it, h, :NP].reshape(quarter, E))

            @pl.loop(0, nch)
            def _(ch):
                r0 = pl.multiple_of(ch * (per * BR), per * BR)
                y = dot(gthi[pl.ds(r0, per * BR), :half], cat_r[:half, :])
                y = y[:, :E] + y[:, E:] + dot(gtlo[pl.ds(r0, per * BR), :half], cat_r[:half, 0:E])
                bs[it + 1, pl.ds(ch * per, per)] = y.reshape(per, BR, E)

        return sq

    def forward_end(it):
        for k in range(2):
            dcopy(it, k).wait_send()
        zall(it, 1, 0, len(first_step)).wait_send()
        fall(it).wait_send()
        if it < ITERS - 1:
            gall(it, 0, nz - 1).wait_send()
            icopy(it, 0, nz).wait_send()

    def halo_wait(it):
        @pl.when(has_l)
        def _():
            hcopy_r(it).wait_recv()

        @pl.when(has_r)
        def _():
            hcopy_l(it).wait_recv()

        @pl.when(has_r)
        def _():
            hcopy_r(it).wait_send()

        @pl.when(has_l)
        def _():
            hcopy_l(it).wait_send()

    def laplace():
        for r0, n, v in ((0, BAND, hd[0]), (BAND, cols, d[...]), (BAND + cols, BAND, hd[1])):
            hi, lo = split(v)
            cat_e[r0:r0 + n, 0:E] = hi
            cat_e[r0:r0 + n, E:2 * E] = lo

    def lap_rows(i):
        r0 = pl.multiple_of(i * BAND, BAND)
        y = dot(lm[pl.ds(r0, BAND), :], cat_e[...])
        return r0, weight * (y[:, :E] + y[:, E:])

    def wcopy_l(it):
        return rcopy(wext.at[pl.ds(0, BAND)], wr.at[it, 1], pair(sem_w, it, 1), at(obs, pat - 1))

    def wcopy_r(it):
        return rcopy(wext.at[pl.ds(BAND + cols, BAND)], wr.at[it, 0], pair(sem_w, it, 0), at(obs, pat + 1))

    def reg_start(it):
        laplace()

        @pl.loop(0, CB)
        def _(i):
            r0, u = lap_rows(i)
            hi, lo = split(u)
            cat_d[pl.ds(r0, BAND), 0:E] = hi
            cat_d[pl.ds(r0, BAND), E:2 * E] = lo

        @pl.loop(0, CB + 2)
        def _(i):
            r0 = pl.multiple_of(i * BAND, BAND)
            y = dot(lmt[pl.ds(r0, BAND), :], cat_d[...])
            wext[pl.ds(r0, BAND), :] = weight * (y[:, :E] + y[:, E:])

        @pl.when(has_l)
        def _():
            wcopy_l(it).start()

        @pl.when(has_r)
        def _():
            wcopy_r(it).start()

    def reg_end(it):
        a[...] = ag[it + 1] + wext[BAND:BAND + cols, :]

        @pl.when(has_l)
        def _():
            wcopy_r(it).wait_recv()

        @pl.when(has_r)
        def _():
            wcopy_l(it).wait_recv()

        a[0:BAND, :] += wr[it, 0]
        a[cols - BAND:cols, :] += wr[it, 1]

    def reg_done(it):
        @pl.when(has_l)
        def _():
            wcopy_l(it).wait_send()

        @pl.when(has_r)
        def _():
            wcopy_r(it).wait_send()

    def ccopy(it):
        return rcopy(scs.at[it], scp.at[it], pair(sem_c, it), at(obs, partner))

    def scopy(it, k, slot):
        return rcopy(scz.at[it], scr.at[it, slot], pair(sem_s, it), zat(k))

    def sall(it):
        block = scr.at[it, pl.ds(0, nz - 1)]
        return rcopy(block, block, pair(sem_s, it), at(obs, partner))

    def tcopy(it):
        return rcopy(tots.at[it], tots.at[it], pair(sem_t, it), at(obs, partner))

    def sums_mid(it):
        @pl.when(c == 1)
        def _():
            ccopy(it).wait_recv()
            both = scs[it] + scp[it]
            scz[it] = both
            scr[it, z] = both

            @pl.loop(1, nz)
            def _(k):
                scopy(it, k, z).start()

    def sums_end(it):
        @pl.when(c == 1)
        def _():
            sall(it).wait_recv()
            tots[it] = jnp.sum(scr[it], axis=0)
            tcopy(it).start()

        @pl.when(c == 0)
        def _():
            tcopy(it).wait_recv()

        return tots[it]

    def sums_done(it):
        @pl.when(c == 0)
        def _():
            ccopy(it).wait_send()

        @pl.when(c == 1)
        def _():
            sall(it).wait_send()
            tcopy(it).wait_send()

    def pcopy(q, slot):
        return rcopy(pls, plr.at[slot], pair(sem_p), at(obs, q))

    def qcopy(o, core, slot):
        return rcopy(qls, qlr.at[slot], pair(sem_q), at(o, 2 * z + core))

    def rows_of(sem, n):
        block = plr.at[pl.ds(0, n)]
        return rcopy(block, block, pair(sem), at(obs, partner))

    def rowsum(x):
        return jnp.sum(x, axis=0, keepdims=True)

    norms, regs = [], []

    def dots(it):
        gv, dv, av = g[...], d[...], a[...]
        scs[it, 0:1, :] = rowsum(gv * gv)
        scs[it, 1:2, :] = rowsum(dv * av)
        scs[it, 2:3, :] = rowsum(gv * av)
        scs[it, 3:4, :] = rowsum(av * av)
        @pl.when(c == 0)
        def _():
            ccopy(it).start()

    def first():
        return None

    def halo_update(it, scalars):
        halo_wait(it)
        if it == 0:
            hg[...] = hal[0]
            hd[...] = hal[0]
        else:
            step, ratio = scalars
            hg[...] = hg[...] - step * hal[it]
            hd[...] = hg[...] + ratio * hd[...]

    def advance(it):
        tot = sums_end(it - 1)
        if it == 1:
            norms.append(tot[0:1])
        norm = norms[-1]
        step = norm / tot[1:2]
        after = norm - 2.0 * step * tot[2:3] + step * step * tot[3:4]
        ratio = after / norm
        norms.append(after)
        if it == 1:
            slip[...] = step * d[...]
        else:
            slip[...] += step * d[...]
        g[...] = g[...] - step * a[...]
        d[...] = g[...] + ratio * d[...]
        if it == ITERS - 1:
            halo_update(it, (step, ratio))
            laplace()

            _, u = lap_rows(jnp.minimum(obs, CB - 1))
            regs.append(jnp.where(obs < CB, rowsum(u * u), 0.0))
            for k, (src, dst) in enumerate(((slip, slip_h), (d, d_h))):
                pltpu.make_async_copy(src, dst, sem_o.at[k]).start()
        return step, ratio

    backward(0, build_laplace)
    g[...] = ag[0]
    d[...] = ag[0]
    forward(0, first)
    for it in range(1, ITERS):
        backward(it, functools.partial(reg_start, it - 1))
        forward_end(it - 1)
        reg_end(it - 1)
        sq = forward(it, functools.partial(advance, it))
        reg_done(it - 1)
    last = ITERS - 1
    norm = norms[-1]
    sq = sq + regs[0]
    pls[...] = sq

    @pl.loop(c, nz)
    def _(k):
        pcopy((z + k) % nz * 2 + 1, pat).start()

    forward_end(last)
    for it in range(ITERS):
        backward_end(it)
    for it in range(ITERS - 1):
        sums_done(it)

    @pl.when(c == 1)
    def _():
        plr[pat] = sq

        rows_of(sem_p, n_patch - 1).wait_recv()

    @pl.when(c == 1)
    def _():
        line = jnp.sum(plr[...], axis=0)
        qls[...] = line
        qlr[obs] = line
        for i, j in far_first:
            for core in range(2):
                qcopy(shifted(i, j), core, obs).start()
        qcopy(obs, 0, obs).start()

    for core in range(2):
        @pl.when(c == core)
        def _():
            rows_of(sem_p, nz - core).wait_send()

    for k, (src, dst) in enumerate(((slip, slip_h), (d, d_h))):
        pltpu.make_async_copy(src, dst, sem_o.at[k]).wait()

    for core in range(2):
        @pl.when(c == core)
        def _():
            rows_of(sem_q, n_obs - core).wait_recv()

    scale[...] = norm / jnp.sum(qlr[...], axis=0)

    @pl.when(c == 1)
    def _():
        rows_of(sem_q, 2 * n_obs - 1).wait_send()


def shards(green, data, neighbours, reg_weight):
    rows, cols = green.shape
    E = data.shape[1]
    n_obs, n_patch = lax.axis_size("obs"), lax.axis_size("patch")
    nz = n_patch // 2
    nd = 2
    R, BR, ext = rows // 2 // nz, cols // n_obs, cols + 2 * BAND
    first = 4 * (nz // 4) - 3
    V = pltpu.VMEM
    D = pltpu.SemaphoreType.DMA
    scratch = [
        V((rows, cols), F32), V((rows, E), F32), V(neighbours.shape, jnp.int32), V((1, E), F32),
        V((rows, cols), BF16), V((rows, cols), BF16),
        V((cols, rows), BF16), V((cols, rows), BF16),
        V((cols, ext), BF16), V((ext, cols), BF16),
        V((cols, 2 * E), BF16), V((rows, 2 * E), BF16), V((ext, 2 * E), BF16),
        V((cols, E), F32), V((cols, E), F32), V((cols, E), F32), V((ext, E), F32), V((cols, E), F32),
        V((2, BAND, E), F32), V((2, BAND, E), F32), V((R, E), F32), V((R, E), F32),
        V((nz, R, E), F32), V((nz, R, E), F32), V((ITERS, nd, nz // nd, R, E), F32),
        V((ITERS, first, R, E), F32), V((2, R, E), F32), V((ITERS, 2, R, E), F32),
        V((ITERS - 1, 2, nz, R, E), F32),
        V((ITERS, n_obs, BR, E), F32), V((ITERS, n_obs, BR, E), F32), V((ITERS, cols, E), F32),
        V((ITERS, 2, BAND, E), F32), V((ITERS - 1, 2, BAND, E), F32),
        V((ITERS - 1, 4, E), F32), V((ITERS - 1, 4, E), F32), V((ITERS - 1, 4, E), F32), V((ITERS - 1, nz, 4, E), F32), V((ITERS - 1, 4, E), F32),
        V((1, E), F32), V((n_patch, 1, E), F32), V((1, E), F32), V((n_obs, 1, E), F32),
        D((2, rows // (2 * BAND) + 1)), D((2,)),
        D((2, ITERS, nd)), D((ITERS, 4)), D((2, ITERS)), D((ITERS - 1, nz - nz // 2 + 3)), D((ITERS - 1, 3)),
        D((2, ITERS)), D((2, ITERS)), D((2, ITERS, 2)), D((2, ITERS - 1, 2)),
        D((2, ITERS - 1)), D((2, ITERS - 1)), D((2, ITERS - 1)), D((2,)), D((2,)), pltpu.SemaphoreType.REGULAR((2,)),
    ]
    anywhere = pl.BlockSpec(memory_space=pl.ANY)
    slip, d, scale = pl.pallas_call(
        functools.partial(kernel, n_obs, n_patch),
        out_shape=[jax.ShapeDtypeStruct((cols, E), F32)] * 2 + [jax.ShapeDtypeStruct((1, E), F32)],
        in_specs=[anywhere] * 4,
        out_specs=[anywhere, anywhere, pl.BlockSpec(memory_space=pltpu.VMEM)],
        scratch_shapes=scratch,
        compiler_params=pltpu.CompilerParams(
            collective_id=0, has_side_effects=True, vmem_limit_bytes=56 * 1024 * 1024),
    )(green, data, neighbours, reg_weight.reshape(1, E))
    return slip + scale * d


def solution(mesh):
    in_specs = (P("obs", "patch"), P("obs", None), P(None, "patch"), P())
    return jax.shard_map(shards, mesh=mesh, in_specs=in_specs, out_specs=P("patch", None), check_vma=False)
```

```python
import functools
import math

import jax
import jax.numpy as jnp
from jax import lax
from jax.experimental import pallas as pl
from jax.experimental.pallas import tpu as pltpu
from jax.sharding import PartitionSpec as P

BAND = 128
ITERS = 3
MESH = pl.DeviceIdType.MESH
F32 = jnp.float32
BF16 = jnp.bfloat16


def dot(a, b):
    return lax.dot_general(a, b, (((1,), (0,)), ((), ())), preferred_element_type=F32)


def split(x):
    hi = x.astype(BF16)
    return hi, (x - hi.astype(F32)).astype(BF16)


def kernel(n_obs, n_patch, green_h, data_h, nb_h, rw_h, slip_h, d_h, scale,
           green, data, nb, rw,
           ghi, glo, gthi, gtlo, lm, lmt, cat_d, cat_r, cat_e,
           d, g, a, wext, slip, hd, hg, qd, qg,
           pf, s, rd, zr, zrel, zfin, img, bs, br, ag, hal, wr, scs, scp, scz, scr, tots, pls, plr, qls, qlr,
           sem_l, sem_o, sem_d, sem_z, sem_f, sem_g, sem_i, sem_b, sem_a, sem_h, sem_w, sem_c, sem_s, sem_t, sem_p, sem_q, go):
    rows, cols = green.shape
    E = data.shape[1]
    nz = n_patch // 2
    R = rows // 2 // nz
    BR = cols // n_obs
    half = rows // 2
    per = nch = math.isqrt(n_obs)
    CB = cols // BAND
    Q = nz // 4
    plus = list(range(1, Q + 1))
    minus = list(range(1, Q))
    near = [0] + [sgn * k for k in minus for sgn in (1, -1)] + [Q]
    far = [2 * Q] + [sgn * k for k in range(2 * Q - 1, Q, -1) for sgn in (1, -1)] + [-Q]
    pieces = near + far
    NP = len(near)
    quarter = half // 2

    def wrapped(o):
        return (o + 2 * Q - 1) % nz - 2 * Q + 1

    def idx(o):
        return pieces.index(wrapped(o))
    obs = lax.axis_index("obs")
    pat = lax.axis_index("patch")
    z = pat // 2
    c = pat % 2
    other = 1 - c
    partner = z * 2 + other
    has_l, has_r = pat > 0, pat < n_patch - 1

    def at(o, q):
        return (o, q)

    def rcopy(src, dst, sems, dev):
        return pltpu.make_async_remote_copy(
            src_ref=src, dst_ref=dst, send_sem=sems[0], recv_sem=sems[1],
            device_id=dev, device_id_type=MESH)

    def pair(sem, *idx):
        return sem.at[(0,) + idx], sem.at[(1,) + idx]

    STEP = 2 * BAND
    ends = [-(-(r0 + STEP) // R) for r0 in range(0, rows, STEP)]

    def load(n):
        part, h, r = n // (2 * NP), n // NP % 2, n % NP
        o = pieces[part * NP + r]
        src = pl.multiple_of(h * half + (z + (1 - 2 * h) * o + nz) % nz * R, R)
        return [pltpu.make_async_copy(a_.at[pl.ds(src, R)], b_.at[pl.ds(n * R, R)], sem_l.at[k, sum(n >= e for e in ends)])
                for k, (a_, b_) in enumerate(((green_h, green), (data_h, data)))]

    small = [pltpu.make_async_copy(src, dst, sem_l.at[i, len(ends)])
             for i, (src, dst) in enumerate(((nb_h, nb), (rw_h, rw)))]
    barrier = pltpu.get_barrier_semaphore()

    def greet(o, q):
        pl.semaphore_signal(barrier, inc=1, device_id=at(o, q), device_id_type=MESH)

    def tell(k):
        pl.semaphore_signal(go.at[k], inc=1, device_id=at(obs, partner), device_id_type=MESH)

    def plane_entered():
        @pl.when(c == 0)
        def _():
            pl.semaphore_wait(barrier, 2 * n_obs - 1)
            tell(0)

        @pl.when(c == 1)
        def _():
            pl.semaphore_wait(go.at[0], 1)

    def line_entered():
        @pl.when(c == 1)
        def _():
            pl.semaphore_wait(barrier, n_patch - 1)
            tell(1)

        @pl.when(c == 0)
        def _():
            pl.semaphore_wait(go.at[1], 1)

    for n in range(2 * nz):
        if n == nz // 2:
            greet(obs, partner)

            @pl.loop(1, n_obs)
            def _(i):
                greet((obs + i) % n_obs, z * 2)

            @pl.loop(1, nz)
            def _(k):
                greet(obs, (z + k) % nz * 2 + 1)

        for copy in load(n):
            copy.start()

    for copy in small:
        copy.start()

    def put_cat(where, value):
        hi, lo = split(value)
        cat_r[where, 0:E] = hi
        cat_r[where, E:2 * E] = lo

    def product(m0, m1, k0, k1):
        y = dot(gthi[m0:m1, k0:k1], cat_r[k0:k1, :])
        y = y[:, :E] + y[:, E:] + dot(gtlo[m0:m1, k0:k1], cat_r[k0:k1, 0:E])
        return y.reshape((m1 - m0) // BR, BR, E)

    def first_product(r0):
        y = product(0, cols, r0, r0 + STEP)
        if r0 == 0:
            bs[0] = y
        else:
            bs[0] += y

    loaded = 0
    for n, r0 in enumerate(range(0, rows, STEP)):
        span = pl.ds(loaded * R, (ends[n] - loaded) * R)
        for k, (a_, b_) in enumerate(((green_h, green), (data_h, data))):
            pltpu.make_async_copy(a_.at[span], b_.at[span], sem_l.at[k, n]).wait()
        loaded = ends[n]
        if r0:
            first_product(r0 - STEP)
        for r in range(r0, r0 + STEP, BAND):
            block = green[r:r + BAND, :]
            hi, lo = split(block)
            ghi[r:r + BAND, :] = hi
            glo[r:r + BAND, :] = lo
            hi, lo = split(block.T)
            gthi[:, r:r + BAND] = hi
            gtlo[:, r:r + BAND] = lo
            put_cat(slice(r, r + BAND), data[r:r + BAND, :])

    first_product(rows - STEP)

    for copy in small:
        copy.wait()
    weight = rw[...]

    zero_h = jnp.zeros((BAND, E), F32)

    @pl.when(pat == 0)
    def _():
        for it in range(ITERS):
            hal[it, 0] = zero_h
        for it in range(ITERS - 1):
            wr[it, 0] = zero_h

    @pl.when(pat == n_patch - 1)
    def _():
        for it in range(ITERS):
            hal[it, 1] = zero_h
        for it in range(ITERS - 1):
            wr[it, 1] = zero_h

    def build_laplace():
        @pl.loop(0, CB + 2)
        def _(j):
            r0 = pl.multiple_of(j * BAND, BAND)
            col = lax.broadcasted_iota(jnp.int32, (BAND, cols), 0) + j * BAND
            own = lax.broadcasted_iota(jnp.int32, (BAND, cols), 1) + BAND
            m = jnp.where(col == own, 4.0, 0.0)
            col = col + (pat * cols - BAND)
            for k in range(3):
                m = m - jnp.where(col == nb[k:k + 1, :], 1.0, 0.0)
            lmt[pl.ds(r0, BAND), :] = m.astype(BF16)
            lm[:, pl.ds(r0, BAND)] = m.T.astype(BF16)

    side = math.isqrt(n_obs)
    steps = sorted(range(side), key=lambda k: -min(k, side - k))
    far_first = sorted([(i, j) for i in steps for j in steps if i or j],
                       key=lambda ij: -sum(min(k, side - k) for k in ij))

    def shifted(i, j):
        return (obs // side + i) % side * side + (obs + j) % side

    def bcopy(b, o, slot):
        return rcopy(bs.at[b, o], br.at[b, slot], pair(sem_b, b), at(o, pat))

    def ball(b):
        return rcopy(bs.at[b, pl.ds(0, n_obs - 1)], br.at[b, pl.ds(0, n_obs - 1)], pair(sem_b, b), at(obs, partner))

    def acopy(b, o, slot):
        piece = ag.at[b, pl.ds(pl.multiple_of(slot * BR, BR), BR)]
        return rcopy(piece, piece, pair(sem_a, b), at(o, pat))

    def aall(b):
        block = ag.at[b, pl.ds(0, (n_obs - 1) * BR)]
        return rcopy(block, block, pair(sem_a, b), at(obs, partner))

    def backward(b, hook):
        if b == 0:
            plane_entered()

            for i, j in far_first:
                bcopy(b, shifted(i, j), obs).start()
        else:
            for i in range(NP, nz - 1):
                gall(b - 1, i, 1).wait_recv()
                icopy(b - 1, i).start()

            icopy(b - 1, NP, NP).wait_recv()

            for h in range(2):
                put_cat(slice(half + h * quarter, half + (h + 1) * quarter), img[b - 1, h, NP:].reshape(quarter, E))
            for i in steps:
                ch = (obs // side + i) % side
                r0 = pl.multiple_of(ch * (per * BR), per * BR)
                y = dot(gthi[pl.ds(r0, per * BR), half:], cat_r[half:, :])
                y = y[:, :E] + y[:, E:] + dot(gtlo[pl.ds(r0, per * BR), half:], cat_r[half:, 0:E])
                bs[b, pl.ds(ch * per, per)] += y.reshape(per, BR, E)
                for j in steps:
                    if i or j:
                        bcopy(b, shifted(i, j), obs).start()

        if b:
            updates.pop()()
        hook()

        ball(b).wait_recv()
        total = lax.fori_loop(1, n_obs, lambda i, acc: acc + br[b, (obs + i) % n_obs], bs[b, obs])
        ag[b, pl.ds(pl.multiple_of(obs * BR, BR), BR), :] = total

        for i, j in far_first:
            acopy(b, shifted(i, j), obs).start()

        if b == 0:
            line_entered()

        aall(b).wait_recv()

    def backward_end(b):
        ball(b).wait_send()
        aall(b).wait_send()

    def dcopy(it, k):
        return rcopy(pf.at[pl.ds(k * NP, NP)], rd.at[it, k], pair(sem_d, it, k), at(obs, partner))

    turn = 1 - 2 * c

    def zat(k):
        return at(obs, ((z + turn * k + nz) % nz) * 2 + c)

    W = Q + 1
    first_step = ([(-k, -k - W) for k in reversed(minus)] + [(1, -Q)] + [(k, k + W) for k in reversed(minus[:-1])] + [(-1, Q)]
                  + [(-k, -k) for k in reversed(minus)] + [(k, k) for k in reversed(minus)])
    n_plus, n_minus = len(plus), len(minus)

    groups = [(0, n_plus), (n_plus, n_minus), (n_plus + n_minus, len(first_step) - n_plus - n_minus)]

    def zcopy(it, slot):
        k, o = first_step[slot]
        group = sum(slot >= first for first, _ in groups)
        return rcopy(s.at[idx(o)], zr.at[it, slot], (sem_z.at[it, 0], sem_z.at[it, group]), zat(k))

    def zall(it, group, first, n):
        block = zr.at[it, pl.ds(first, n)]
        return rcopy(block, block, (sem_z.at[it, 0], sem_z.at[it, group]), at(obs, partner))

    def fcopy(it, slot):
        return rcopy(zrel.at[slot], zfin.at[it, slot], pair(sem_f, it), zat(-W if slot == 0 else W))

    def fall(it):
        return rcopy(zrel, zfin.at[it], pair(sem_f, it), at(obs, partner))

    gather = ([(k, 0) for k in (-Q, Q)] + [(sgn * k, 0) for k in reversed(minus) for sgn in (1, -1)]
              + [(k, -Q) for k in reversed(plus)] + [(-k, Q) for k in reversed(minus)])
    n_own = 2 * Q

    def arrival(it, i):
        return sem_g.at[it, 1 if 0 < i < NP - 1 else i - NP + 3]

    def gcopy(it, m):
        k, o = gather[m]
        to = idx(o - k)
        return rcopy(img.at[it, c, idx(o)], img.at[it, c, to], (sem_g.at[it, 0], arrival(it, to)), zat(k))

    def gall(it, i, n):
        block = img.at[it, c, pl.ds(i, n)]
        return rcopy(block, block, (sem_g.at[it, 0], arrival(it, i)), at(obs, partner))

    def icopy(it, i, n=1):
        block = img.at[it, c, pl.ds(i, n)]
        return rcopy(block, block, (sem_i.at[it, 0], sem_i.at[it, 1 + i // NP]), at(obs, partner))

    def fold(acc, it, group):
        first, n = groups[group]
        zall(it, group + 1, first, n).wait_recv()
        for slot in range(first, first + n):
            acc = acc + zr[it, slot]
        return acc

    def hsrc(it):
        return a if it else ag.at[0]

    def hcopy_r(it):
        return rcopy(hsrc(it).at[pl.ds(cols - BAND, BAND)], hal.at[it, 0], pair(sem_h, it, 0), at(obs, pat + 1))

    def hcopy_l(it):
        return rcopy(hsrc(it).at[pl.ds(0, BAND)], hal.at[it, 1], pair(sem_h, it, 1), at(obs, pat - 1))

    def forward(it, hook):
        last = it == ITERS - 1

        hi, lo = split(hsrc(it)[...])
        cat_d[:, 0:E] = hi
        cat_d[:, E:2 * E] = lo

        def part(h, k):
            r0 = pl.multiple_of(k * half + h * quarter, quarter)
            y = dot(ghi[pl.ds(r0, quarter), :], cat_d[...])
            y = y[:, :E] + y[:, E:] + dot(glo[pl.ds(r0, quarter), :], cat_d[:, 0:E])
            return y.reshape(NP, R, E)

        for k in (1, 0):
            pf[k * NP:(k + 1) * NP] = part(other, k)
            dcopy(it, k).start()

        if it:
            dots(it - 1)

        for k in (1, 0):
            s[k * NP:(k + 1) * NP] = part(c, k)

        dcopy(it, 1).wait_recv()
        s[NP:] += rd[it, 1]
        for slot in range(n_plus + n_minus - 1):
            zcopy(it, slot).start()
        dcopy(it, 0).wait_recv()
        s[:NP] += rd[it, 0]
        zcopy(it, n_plus + n_minus - 1).start()

        if it:
            sums_mid(it - 1)

        def halos():
            @pl.when(has_r)
            def _():
                hcopy_r(it).start()

            @pl.when(has_l)
            def _():
                hcopy_l(it).start()

        if last:
            halos()

        direct = range(n_plus + n_minus, len(first_step))
        for slot in direct:
            if abs(first_step[slot][0]) > 1:
                zcopy(it, slot).start()

        zrel[0] = fold(s[idx(-W)], it, 0)
        fcopy(it, 0).start()
        zrel[1] = fold(s[idx(W)], it, 1)
        fcopy(it, 1).start()

        for slot in direct:
            if abs(first_step[slot][0]) == 1:
                zcopy(it, slot).start()


        scalars = hook()

        total = fold(s[idx(0)], it, 2)
        fall(it).wait_recv()
        total = total + zfin[it, 0] + zfin[it, 1]

        if it:
            step, ratio = scalars
            rest = qg[...] - step * total
            total = rest + ratio * qd[...]
        else:
            rest = total

        if last:
            sq = jnp.sum(total * total, axis=0, keepdims=True)
        else:
            sq = None
            qg[...] = rest
            qd[...] = total
            img[it, c, idx(0)] = total
            for m in range(n_own):
                gcopy(it, m).start()
            icopy(it, 0).start()
            gall(it, idx(-Q), 1).wait_recv()
            for m in range(n_own, n_own + Q):
                gcopy(it, m).start()
            gall(it, idx(Q), 1).wait_recv()
            for m in range(n_own + Q, len(gather)):
                gcopy(it, m).start()
            halos()
            icopy(it, idx(Q)).start()
            icopy(it, idx(-Q)).start()
            gall(it, 1, NP - 2).wait_recv()
            icopy(it, 1, NP - 2).start()

            icopy(it, 0, NP).wait_recv()
            for h in range(2):
                put_cat(slice(h * quarter, (h + 1) * quarter), img[it, h, :NP].reshape(quarter, E))

            @pl.loop(0, nch)
            def _(ch):
                r0 = pl.multiple_of(ch * (per * BR), per * BR)
                y = dot(gthi[pl.ds(r0, per * BR), :half], cat_r[:half, :])
                y = y[:, :E] + y[:, E:] + dot(gtlo[pl.ds(r0, per * BR), :half], cat_r[:half, 0:E])
                bs[it + 1, pl.ds(ch * per, per)] = y.reshape(per, BR, E)

            updates.append(functools.partial(halo_update, it, scalars))

        return sq

    def forward_end(it):
        for k in range(2):
            dcopy(it, k).wait_send()
        zall(it, 1, 0, len(first_step)).wait_send()
        fall(it).wait_send()
        if it < ITERS - 1:
            gall(it, 0, nz - 1).wait_send()
            icopy(it, 0, nz).wait_send()

    def halo_wait(it):
        @pl.when(has_l)
        def _():
            hcopy_r(it).wait_recv()

        @pl.when(has_r)
        def _():
            hcopy_l(it).wait_recv()

        @pl.when(has_r)
        def _():
            hcopy_r(it).wait_send()

        @pl.when(has_l)
        def _():
            hcopy_l(it).wait_send()

    def laplace():
        for r0, n, v in ((0, BAND, hd[0]), (BAND, cols, d[...]), (BAND + cols, BAND, hd[1])):
            hi, lo = split(v)
            cat_e[r0:r0 + n, 0:E] = hi
            cat_e[r0:r0 + n, E:2 * E] = lo

    def lap_rows(i):
        r0 = pl.multiple_of(i * BAND, BAND)
        y = dot(lm[pl.ds(r0, BAND), :], cat_e[...])
        return r0, weight * (y[:, :E] + y[:, E:])

    def wcopy_l(it):
        return rcopy(wext.at[pl.ds(0, BAND)], wr.at[it, 1], pair(sem_w, it, 1), at(obs, pat - 1))

    def wcopy_r(it):
        return rcopy(wext.at[pl.ds(BAND + cols, BAND)], wr.at[it, 0], pair(sem_w, it, 0), at(obs, pat + 1))

    def reg_start(it):
        laplace()

        @pl.loop(0, CB)
        def _(i):
            r0, u = lap_rows(i)
            hi, lo = split(u)
            cat_d[pl.ds(r0, BAND), 0:E] = hi
            cat_d[pl.ds(r0, BAND), E:2 * E] = lo

        @pl.loop(0, CB + 2)
        def _(i):
            r0 = pl.multiple_of(i * BAND, BAND)
            y = dot(lmt[pl.ds(r0, BAND), :], cat_d[...])
            wext[pl.ds(r0, BAND), :] = weight * (y[:, :E] + y[:, E:])

        @pl.when(has_l)
        def _():
            wcopy_l(it).start()

        @pl.when(has_r)
        def _():
            wcopy_r(it).start()

    def reg_end(it):
        a[...] = ag[it + 1] + wext[BAND:BAND + cols, :]

        @pl.when(has_l)
        def _():
            wcopy_r(it).wait_recv()

        @pl.when(has_r)
        def _():
            wcopy_l(it).wait_recv()

        a[0:BAND, :] += wr[it, 0]
        a[cols - BAND:cols, :] += wr[it, 1]

    def reg_done(it):
        @pl.when(has_l)
        def _():
            wcopy_l(it).wait_send()

        @pl.when(has_r)
        def _():
            wcopy_r(it).wait_send()

    def ccopy(it):
        return rcopy(scs.at[it], scp.at[it], pair(sem_c, it), at(obs, partner))

    def scopy(it, k, slot):
        return rcopy(scz.at[it], scr.at[it, slot], pair(sem_s, it), zat(k))

    def sall(it):
        block = scr.at[it, pl.ds(0, nz - 1)]
        return rcopy(block, block, pair(sem_s, it), at(obs, partner))

    def tcopy(it):
        return rcopy(tots.at[it], tots.at[it], pair(sem_t, it), at(obs, partner))

    def sums_mid(it):
        @pl.when(c == 1)
        def _():
            ccopy(it).wait_recv()
            both = scs[it] + scp[it]
            scz[it] = both
            scr[it, z] = both

            @pl.loop(1, nz)
            def _(k):
                scopy(it, k, z).start()

    def sums_end(it):
        @pl.when(c == 1)
        def _():
            sall(it).wait_recv()
            tots[it] = jnp.sum(scr[it], axis=0)
            tcopy(it).start()

        @pl.when(c == 0)
        def _():
            tcopy(it).wait_recv()

        return tots[it]

    def sums_done(it):
        @pl.when(c == 0)
        def _():
            ccopy(it).wait_send()

        @pl.when(c == 1)
        def _():
            sall(it).wait_send()
            tcopy(it).wait_send()

    def pcopy(q, slot):
        return rcopy(pls, plr.at[slot], pair(sem_p), at(obs, q))

    def qcopy(o, core, slot):
        return rcopy(qls, qlr.at[slot], pair(sem_q), at(o, 2 * z + core))

    def rows_of(sem, n):
        block = plr.at[pl.ds(0, n)]
        return rcopy(block, block, pair(sem), at(obs, partner))

    def rowsum(x):
        return jnp.sum(x, axis=0, keepdims=True)

    norms, regs = [], []
    updates = []

    def dots(it):
        gv, dv, av = g[...], d[...], a[...]
        scs[it, 0:1, :] = rowsum(gv * gv)
        scs[it, 1:2, :] = rowsum(dv * av)
        scs[it, 2:3, :] = rowsum(gv * av)
        scs[it, 3:4, :] = rowsum(av * av)
        @pl.when(c == 0)
        def _():
            ccopy(it).start()

    def first():
        return None

    def halo_update(it, scalars):
        halo_wait(it)
        if it == 0:
            hg[...] = hal[0]
            hd[...] = hal[0]
        else:
            step, ratio = scalars
            hg[...] = hg[...] - step * hal[it]
            hd[...] = hg[...] + ratio * hd[...]

    def advance(it):
        tot = sums_end(it - 1)
        if it == 1:
            norms.append(tot[0:1])
        norm = norms[-1]
        step = norm / tot[1:2]
        after = norm - 2.0 * step * tot[2:3] + step * step * tot[3:4]
        ratio = after / norm
        norms.append(after)
        if it == 1:
            slip[...] = step * d[...]
        else:
            slip[...] += step * d[...]
        g[...] = g[...] - step * a[...]
        d[...] = g[...] + ratio * d[...]
        if it == ITERS - 1:
            halo_update(it, (step, ratio))
            laplace()

            _, u = lap_rows(jnp.minimum(obs, CB - 1))
            regs.append(jnp.where(obs < CB, rowsum(u * u), 0.0))
            for k, (src, dst) in enumerate(((slip, slip_h), (d, d_h))):
                pltpu.make_async_copy(src, dst, sem_o.at[k]).start()
        return step, ratio

    backward(0, build_laplace)
    g[...] = ag[0]
    d[...] = ag[0]
    forward(0, first)
    for it in range(1, ITERS):
        backward(it, functools.partial(reg_start, it - 1))
        forward_end(it - 1)
        reg_end(it - 1)
        sq = forward(it, functools.partial(advance, it))
        reg_done(it - 1)
    last = ITERS - 1
    norm = norms[-1]
    sq = sq + regs[0]
    pls[...] = sq

    @pl.loop(c, nz)
    def _(k):
        pcopy((z + k) % nz * 2 + 1, pat).start()

    forward_end(last)
    for it in range(ITERS):
        backward_end(it)
    for it in range(ITERS - 1):
        sums_done(it)

    @pl.when(c == 1)
    def _():
        plr[pat] = sq

        rows_of(sem_p, n_patch - 1).wait_recv()

    @pl.when(c == 1)
    def _():
        line = jnp.sum(plr[...], axis=0)
        qls[...] = line
        qlr[obs] = line
        for i, j in far_first:
            for core in range(2):
                qcopy(shifted(i, j), core, obs).start()
        qcopy(obs, 0, obs).start()

    for core in range(2):
        @pl.when(c == core)
        def _():
            rows_of(sem_p, nz - core).wait_send()

    for k, (src, dst) in enumerate(((slip, slip_h), (d, d_h))):
        pltpu.make_async_copy(src, dst, sem_o.at[k]).wait()

    for core in range(2):
        @pl.when(c == core)
        def _():
            rows_of(sem_q, n_obs - core).wait_recv()

    scale[...] = norm / jnp.sum(qlr[...], axis=0)

    @pl.when(c == 1)
    def _():
        rows_of(sem_q, 2 * n_obs - 1).wait_send()


def shards(green, data, neighbours, reg_weight):
    rows, cols = green.shape
    E = data.shape[1]
    n_obs, n_patch = lax.axis_size("obs"), lax.axis_size("patch")
    nz = n_patch // 2
    nd = 2
    R, BR, ext = rows // 2 // nz, cols // n_obs, cols + 2 * BAND
    first = 4 * (nz // 4) - 3
    V = pltpu.VMEM
    D = pltpu.SemaphoreType.DMA
    scratch = [
        V((rows, cols), F32), V((rows, E), F32), V(neighbours.shape, jnp.int32), V((1, E), F32),
        V((rows, cols), BF16), V((rows, cols), BF16),
        V((cols, rows), BF16), V((cols, rows), BF16),
        V((cols, ext), BF16), V((ext, cols), BF16),
        V((cols, 2 * E), BF16), V((rows, 2 * E), BF16), V((ext, 2 * E), BF16),
        V((cols, E), F32), V((cols, E), F32), V((cols, E), F32), V((ext, E), F32), V((cols, E), F32),
        V((2, BAND, E), F32), V((2, BAND, E), F32), V((R, E), F32), V((R, E), F32),
        V((nz, R, E), F32), V((nz, R, E), F32), V((ITERS, nd, nz // nd, R, E), F32),
        V((ITERS, first, R, E), F32), V((2, R, E), F32), V((ITERS, 2, R, E), F32),
        V((ITERS - 1, 2, nz, R, E), F32),
        V((ITERS, n_obs, BR, E), F32), V((ITERS, n_obs, BR, E), F32), V((ITERS, cols, E), F32),
        V((ITERS, 2, BAND, E), F32), V((ITERS - 1, 2, BAND, E), F32),
        V((ITERS - 1, 4, E), F32), V((ITERS - 1, 4, E), F32), V((ITERS - 1, 4, E), F32), V((ITERS - 1, nz, 4, E), F32), V((ITERS - 1, 4, E), F32),
        V((1, E), F32), V((n_patch, 1, E), F32), V((1, E), F32), V((n_obs, 1, E), F32),
        D((2, rows // (2 * BAND) + 1)), D((2,)),
        D((2, ITERS, nd)), D((ITERS, 4)), D((2, ITERS)), D((ITERS - 1, nz - nz // 2 + 3)), D((ITERS - 1, 3)),
        D((2, ITERS)), D((2, ITERS)), D((2, ITERS, 2)), D((2, ITERS - 1, 2)),
        D((2, ITERS - 1)), D((2, ITERS - 1)), D((2, ITERS - 1)), D((2,)), D((2,)), pltpu.SemaphoreType.REGULAR((2,)),
    ]
    anywhere = pl.BlockSpec(memory_space=pl.ANY)
    slip, d, scale = pl.pallas_call(
        functools.partial(kernel, n_obs, n_patch),
        out_shape=[jax.ShapeDtypeStruct((cols, E), F32)] * 2 + [jax.ShapeDtypeStruct((1, E), F32)],
        in_specs=[anywhere] * 4,
        out_specs=[anywhere, anywhere, pl.BlockSpec(memory_space=pltpu.VMEM)],
        scratch_shapes=scratch,
        compiler_params=pltpu.CompilerParams(
            collective_id=0, has_side_effects=True, vmem_limit_bytes=56 * 1024 * 1024),
    )(green, data, neighbours, reg_weight.reshape(1, E))
    return slip + scale * d


def solution(mesh):
    in_specs = (P("obs", "patch"), P("obs", None), P(None, "patch"), P())
    return jax.shard_map(shards, mesh=mesh, in_specs=in_specs, out_specs=P("patch", None), check_vma=False)
```

```python
import functools
import math

import jax
import jax.numpy as jnp
from jax import lax
from jax.experimental import pallas as pl
from jax.experimental.pallas import tpu as pltpu
from jax.sharding import PartitionSpec as P

BAND = 128
ITERS = 3
MESH = pl.DeviceIdType.MESH
F32 = jnp.float32
BF16 = jnp.bfloat16


def dot(a, b):
    return lax.dot_general(a, b, (((1,), (0,)), ((), ())), preferred_element_type=F32)


def split(x):
    hi = x.astype(BF16)
    return hi, (x - hi.astype(F32)).astype(BF16)


def kernel(n_obs, n_patch, green_h, data_h, nb_h, rw_h, slip_h, d_h, scale,
           green, data, line_up, nb, rw,
           ghi, glo, gthi, gtlo, lm, lmt, cat_d, cat_r, cat_e,
           d, g, a, wext, slip, hd, hg, qd, qg,
           pf, s, rd, zr, zrel, zfin, img, bs, br, ag, hal, wr, scs, scp, scz, scr, tots, pls, plr, qls, qlr,
           sem_l, sem_o, sem_d, sem_z, sem_f, sem_g, sem_i, sem_b, sem_a, sem_h, sem_w, sem_c, sem_s, sem_t, sem_p, sem_q, go):
    rows, cols = green.shape
    E = data.shape[1]
    nz = n_patch // 2
    R = rows // 2 // nz
    BR = cols // n_obs
    half = rows // 2
    per = nch = math.isqrt(n_obs)
    CB = cols // BAND
    Q = nz // 4
    plus = list(range(1, Q + 1))
    minus = list(range(1, Q))
    near = [0] + [sgn * k for k in minus for sgn in (1, -1)] + [Q]
    far = [2 * Q] + [sgn * k for k in range(2 * Q - 1, Q, -1) for sgn in (1, -1)] + [-Q]
    pieces = near + far
    NP = len(near)
    quarter = half // 2

    def wrapped(o):
        return (o + 2 * Q - 1) % nz - 2 * Q + 1

    def idx(o):
        return pieces.index(wrapped(o))
    obs = lax.axis_index("obs")
    pat = lax.axis_index("patch")
    z = pat // 2
    c = pat % 2
    other = 1 - c
    partner = z * 2 + other
    has_l, has_r = pat > 0, pat < n_patch - 1

    def at(o, q):
        return (o, q)

    def rcopy(src, dst, sems, dev):
        return pltpu.make_async_remote_copy(
            src_ref=src, dst_ref=dst, send_sem=sems[0], recv_sem=sems[1],
            device_id=dev, device_id_type=MESH)

    def pair(sem, *idx):
        return sem.at[(0,) + idx], sem.at[(1,) + idx]

    STEP = 2 * BAND
    ends = [-(-(r0 + STEP) // R) for r0 in range(0, rows, STEP)]

    def load(n):
        part, h, r = n // (2 * NP), n // NP % 2, n % NP
        o = pieces[part * NP + r]
        src = pl.multiple_of(h * half + (z + (1 - 2 * h) * o + nz) % nz * R, R)
        return src, pltpu.make_async_copy(green_h.at[pl.ds(src, R)], green.at[pl.ds(n * R, R)],
                                          sem_l.at[0, sum(n >= e for e in ends)])

    small = [pltpu.make_async_copy(src, dst, sem_l.at[i, len(ends)])
             for i, (src, dst) in enumerate(((nb_h, nb), (rw_h, rw)))]
    fields = pltpu.make_async_copy(data_h, data, sem_l.at[1, 0])
    barrier = pltpu.get_barrier_semaphore()

    def greet(o, q):
        pl.semaphore_signal(barrier, inc=1, device_id=at(o, q), device_id_type=MESH)

    def tell(k):
        pl.semaphore_signal(go.at[k], inc=1, device_id=at(obs, partner), device_id_type=MESH)

    def plane_entered():
        @pl.when(c == 0)
        def _():
            pl.semaphore_wait(barrier, 2 * n_obs - 1)
            tell(0)

        @pl.when(c == 1)
        def _():
            pl.semaphore_wait(go.at[0], 1)

    def line_entered():
        @pl.when(c == 1)
        def _():
            pl.semaphore_wait(barrier, n_patch - 1)
            tell(1)

        @pl.when(c == 0)
        def _():
            pl.semaphore_wait(go.at[1], 1)

    for n in range(2 * nz):
        load(n)[1].start()
        if n == nz // 4:
            fields.start()

    for copy in small:
        copy.start()

    greet(obs, partner)

    @pl.loop(1, n_obs)
    def _(i):
        greet((obs + i) % n_obs, z * 2)

    @pl.loop(1, nz)
    def _(k):
        greet(obs, (z + k) % nz * 2 + 1)

    def put_cat(where, value):
        hi, lo = split(value)
        cat_r[where, 0:E] = hi
        cat_r[where, E:2 * E] = lo

    def product(m0, m1, k0, k1):
        y = dot(gthi[m0:m1, k0:k1], cat_r[k0:k1, :])
        y = y[:, :E] + y[:, E:] + dot(gtlo[m0:m1, k0:k1], cat_r[k0:k1, 0:E])
        return y.reshape((m1 - m0) // BR, BR, E)

    def first_product(r0):
        y = product(0, cols, r0, r0 + STEP)
        if r0 == 0:
            bs[0] = y
        else:
            bs[0] += y

    loaded = 0
    for n, r0 in enumerate(range(0, rows, STEP)):
        span = pl.ds(loaded * R, (ends[n] - loaded) * R)
        pltpu.make_async_copy(green_h.at[span], green.at[span], sem_l.at[0, n]).wait()
        if n == 0:
            fields.wait()
        for m in range(loaded, ends[n]):
            line_up[m * R:(m + 1) * R, :] = data[pl.ds(load(m)[0], R), :]
        loaded = ends[n]
        if r0:
            first_product(r0 - STEP)
        for r in range(r0, r0 + STEP, BAND):
            block = green[r:r + BAND, :]
            hi, lo = split(block)
            ghi[r:r + BAND, :] = hi
            glo[r:r + BAND, :] = lo
            hi, lo = split(block.T)
            gthi[:, r:r + BAND] = hi
            gtlo[:, r:r + BAND] = lo
            put_cat(slice(r, r + BAND), line_up[r:r + BAND, :])

    first_product(rows - STEP)

    for copy in small:
        copy.wait()
    weight = rw[...]

    zero_h = jnp.zeros((BAND, E), F32)

    @pl.when(pat == 0)
    def _():
        for it in range(ITERS):
            hal[it, 0] = zero_h
        for it in range(ITERS - 1):
            wr[it, 0] = zero_h

    @pl.when(pat == n_patch - 1)
    def _():
        for it in range(ITERS):
            hal[it, 1] = zero_h
        for it in range(ITERS - 1):
            wr[it, 1] = zero_h

    def build_laplace():
        @pl.loop(0, CB + 2)
        def _(j):
            r0 = pl.multiple_of(j * BAND, BAND)
            col = lax.broadcasted_iota(jnp.int32, (BAND, cols), 0) + j * BAND
            own = lax.broadcasted_iota(jnp.int32, (BAND, cols), 1) + BAND
            m = jnp.where(col == own, 4.0, 0.0)
            col = col + (pat * cols - BAND)
            for k in range(3):
                m = m - jnp.where(col == nb[k:k + 1, :], 1.0, 0.0)
            lmt[pl.ds(r0, BAND), :] = m.astype(BF16)
            lm[:, pl.ds(r0, BAND)] = m.T.astype(BF16)

    side = math.isqrt(n_obs)
    steps = sorted(range(side), key=lambda k: -min(k, side - k))
    far_first = sorted([(i, j) for i in steps for j in steps if i or j],
                       key=lambda ij: -sum(min(k, side - k) for k in ij))

    def shifted(i, j):
        return (obs // side + (1 - 2 * c) * i + side) % side * side + (obs + (1 - 2 * c) * j + side) % side

    def crossed(i, j):
        return shifted(i + c * (j - i), j + c * (i - j))

    def bcopy(b, o, slot):
        return rcopy(bs.at[b, o], br.at[b, slot], pair(sem_b), at(o, pat))

    def ball(b):
        return rcopy(bs.at[b, pl.ds(0, n_obs - 1)], br.at[b, pl.ds(0, n_obs - 1)], pair(sem_b), at(obs, partner))

    def acopy(b, o, slot):
        piece = ag.at[b, pl.ds(pl.multiple_of(slot * BR, BR), BR)]
        return rcopy(piece, piece, pair(sem_a), at(o, pat))

    def aall(b):
        block = ag.at[b, pl.ds(0, (n_obs - 1) * BR)]
        return rcopy(block, block, pair(sem_a), at(obs, partner))

    def backward(b, hook):
        if b == 0:
            plane_entered()

            for i, j in far_first:
                bcopy(b, crossed(i, j), obs).start()
        else:
            for i in range(NP, nz - 1):
                gall(b - 1, i, 1).wait_recv()
                icopy(b - 1, i).start()

            icopy(b - 1, NP, NP).wait_recv()

            for h in range(2):
                put_cat(slice(half + h * quarter, half + (h + 1) * quarter), img[b - 1, h, NP:].reshape(quarter, E))
            for i in steps:
                ch = (obs // side + (1 - 2 * c) * i + side) % side
                r0 = pl.multiple_of(ch * (per * BR), per * BR)
                y = dot(gthi[pl.ds(r0, per * BR), half:], cat_r[half:, :])
                y = y[:, :E] + y[:, E:] + dot(gtlo[pl.ds(r0, per * BR), half:], cat_r[half:, 0:E])
                bs[b, pl.ds(ch * per, per)] += y.reshape(per, BR, E)
                for j in steps:
                    if i or j:
                        bcopy(b, shifted(i, j), obs).start()

        if b:
            updates.pop()()
        hook()

        ball(b).wait_recv()
        total = lax.fori_loop(1, n_obs, lambda i, acc: acc + br[b, (obs + i) % n_obs], bs[b, obs])
        ag[b, pl.ds(pl.multiple_of(obs * BR, BR), BR), :] = total

        for i, j in far_first:
            acopy(b, crossed(i, j), obs).start()

        if b == 0:
            line_entered()

        aall(b).wait_recv()

    def backward_end(b):
        ball(b).wait_send()
        aall(b).wait_send()

    def dcopy(it, k):
        return rcopy(pf.at[pl.ds(k * NP, NP)], rd.at[it, k], pair(sem_d, k), at(obs, partner))

    turn = 1 - 2 * c

    def zat(k):
        return at(obs, ((z + turn * k + nz) % nz) * 2 + c)

    W = Q + 1
    first_step = ([(-k, -k - W) for k in reversed(minus)] + [(1, -Q)] + [(k, k + W) for k in reversed(minus[:-1])] + [(-1, Q)]
                  + [(-k, -k) for k in reversed(minus)] + [(k, k) for k in reversed(minus)])
    n_plus, n_minus = len(plus), len(minus)

    groups = [(0, n_plus), (n_plus, n_minus), (n_plus + n_minus, len(first_step) - n_plus - n_minus)]

    def zcopy(it, slot):
        k, o = first_step[slot]
        group = sum(slot >= first for first, _ in groups)
        return rcopy(s.at[idx(o)], zr.at[it, slot], (sem_z.at[0], sem_z.at[group]), zat(k))

    def zall(it, group, first, n):
        block = zr.at[it, pl.ds(first, n)]
        return rcopy(block, block, (sem_z.at[0], sem_z.at[group]), at(obs, partner))

    def fcopy(it, slot):
        return rcopy(zrel.at[slot], zfin.at[it, slot], pair(sem_f), zat(-W if slot == 0 else W))

    def fall(it):
        return rcopy(zrel, zfin.at[it], pair(sem_f), at(obs, partner))

    gather = ([(k, 0) for k in (-Q, Q)] + [(sgn * k, 0) for k in reversed(minus) for sgn in (1, -1)]
              + [(k, -Q) for k in reversed(plus)] + [(-k, Q) for k in reversed(minus)])
    n_own = 2 * Q

    def arrival(it, i):
        return sem_g.at[1 if 0 < i < NP - 1 else i - NP + 3]

    def gcopy(it, m):
        k, o = gather[m]
        to = idx(o - k)
        return rcopy(img.at[it, c, idx(o)], img.at[it, c, to], (sem_g.at[0], arrival(it, to)), zat(k))

    def gall(it, i, n):
        block = img.at[it, c, pl.ds(i, n)]
        return rcopy(block, block, (sem_g.at[0], arrival(it, i)), at(obs, partner))

    def icopy(it, i, n=1):
        block = img.at[it, c, pl.ds(i, n)]
        return rcopy(block, block, (sem_i.at[0], sem_i.at[1 + i // NP]), at(obs, partner))

    def fold(acc, it, group):
        first, n = groups[group]
        zall(it, group + 1, first, n).wait_recv()
        for slot in range(first, first + n):
            acc = acc + zr[it, slot]
        return acc

    def hsrc(it):
        return a if it else ag.at[0]

    def hcopy_r(it):
        return rcopy(hsrc(it).at[pl.ds(cols - BAND, BAND)], hal.at[it, 0], pair(sem_h, it, 0), at(obs, pat + 1))

    def hcopy_l(it):
        return rcopy(hsrc(it).at[pl.ds(0, BAND)], hal.at[it, 1], pair(sem_h, it, 1), at(obs, pat - 1))

    def forward(it, hook):
        last = it == ITERS - 1

        hi, lo = split(hsrc(it)[...])
        cat_d[:, 0:E] = hi
        cat_d[:, E:2 * E] = lo

        def part(h, k):
            r0 = pl.multiple_of(k * half + h * quarter, quarter)
            y = dot(ghi[pl.ds(r0, quarter), :], cat_d[...])
            y = y[:, :E] + y[:, E:] + dot(glo[pl.ds(r0, quarter), :], cat_d[:, 0:E])
            return y.reshape(NP, R, E)

        for k in (1, 0):
            pf[k * NP:(k + 1) * NP] = part(other, k)
            dcopy(it, k).start()

        if it:
            dots(it - 1)

        for k in (1, 0):
            s[k * NP:(k + 1) * NP] = part(c, k)

        dcopy(it, 1).wait_recv()
        s[NP:] += rd[it, 1]
        for slot in range(n_plus + n_minus - 1):
            zcopy(it, slot).start()
        dcopy(it, 0).wait_recv()
        s[:NP] += rd[it, 0]
        zcopy(it, n_plus + n_minus - 1).start()

        if it:
            sums_mid(it - 1)

        def halos():
            @pl.when(has_r)
            def _():
                hcopy_r(it).start()

            @pl.when(has_l)
            def _():
                hcopy_l(it).start()

        if last:
            halos()

        direct = range(n_plus + n_minus, len(first_step))
        for slot in direct:
            if abs(first_step[slot][0]) > 1:
                zcopy(it, slot).start()

        zrel[0] = fold(s[idx(-W)], it, 0)
        fcopy(it, 0).start()
        zrel[1] = fold(s[idx(W)], it, 1)
        fcopy(it, 1).start()

        for slot in direct:
            if abs(first_step[slot][0]) == 1:
                zcopy(it, slot).start()


        scalars = hook()

        total = fold(s[idx(0)], it, 2)
        fall(it).wait_recv()
        total = total + zfin[it, 0] + zfin[it, 1]

        if it:
            step, ratio = scalars
            rest = qg[...] - step * total
            total = rest + ratio * qd[...]
        else:
            rest = total

        if last:
            sq = jnp.sum(total * total, axis=0, keepdims=True)
        else:
            sq = None
            qg[...] = rest
            qd[...] = total
            img[it, c, idx(0)] = total
            for m in range(n_own):
                gcopy(it, m).start()
            icopy(it, 0).start()
            gall(it, idx(-Q), 1).wait_recv()
            for m in range(n_own, n_own + Q):
                gcopy(it, m).start()
            gall(it, idx(Q), 1).wait_recv()
            for m in range(n_own + Q, len(gather)):
                gcopy(it, m).start()
            halos()
            icopy(it, idx(Q)).start()
            icopy(it, idx(-Q)).start()
            gall(it, 1, NP - 2).wait_recv()
            icopy(it, 1, NP - 2).start()

            icopy(it, 0, NP).wait_recv()
            for h in range(2):
                put_cat(slice(h * quarter, (h + 1) * quarter), img[it, h, :NP].reshape(quarter, E))

            @pl.loop(0, nch)
            def _(ch):
                r0 = pl.multiple_of(ch * (per * BR), per * BR)
                y = dot(gthi[pl.ds(r0, per * BR), :half], cat_r[:half, :])
                y = y[:, :E] + y[:, E:] + dot(gtlo[pl.ds(r0, per * BR), :half], cat_r[:half, 0:E])
                bs[it + 1, pl.ds(ch * per, per)] = y.reshape(per, BR, E)

            updates.append(functools.partial(halo_update, it, scalars))

        return sq

    def forward_end(it):
        for k in range(2):
            dcopy(it, k).wait_send()
        zall(it, 1, 0, len(first_step)).wait_send()
        fall(it).wait_send()
        if it < ITERS - 1:
            gall(it, 0, nz - 1).wait_send()
            icopy(it, 0, nz).wait_send()

    def halo_wait(it):
        @pl.when(has_l)
        def _():
            hcopy_r(it).wait_recv()

        @pl.when(has_r)
        def _():
            hcopy_l(it).wait_recv()

        @pl.when(has_r)
        def _():
            hcopy_r(it).wait_send()

        @pl.when(has_l)
        def _():
            hcopy_l(it).wait_send()

    def laplace():
        for r0, n, v in ((0, BAND, hd[0]), (BAND, cols, d[...]), (BAND + cols, BAND, hd[1])):
            hi, lo = split(v)
            cat_e[r0:r0 + n, 0:E] = hi
            cat_e[r0:r0 + n, E:2 * E] = lo

    def lap_rows(i):
        r0 = pl.multiple_of(i * BAND, BAND)
        y = dot(lm[pl.ds(r0, BAND), :], cat_e[...])
        return r0, weight * (y[:, :E] + y[:, E:])

    def wcopy_l(it):
        return rcopy(wext.at[pl.ds(0, BAND)], wr.at[it, 1], pair(sem_w, it, 1), at(obs, pat - 1))

    def wcopy_r(it):
        return rcopy(wext.at[pl.ds(BAND + cols, BAND)], wr.at[it, 0], pair(sem_w, it, 0), at(obs, pat + 1))

    def reg_start(it):
        laplace()

        @pl.loop(0, CB)
        def _(i):
            r0, u = lap_rows(i)
            hi, lo = split(u)
            cat_d[pl.ds(r0, BAND), 0:E] = hi
            cat_d[pl.ds(r0, BAND), E:2 * E] = lo

        @pl.loop(0, CB + 2)
        def _(i):
            r0 = pl.multiple_of(i * BAND, BAND)
            y = dot(lmt[pl.ds(r0, BAND), :], cat_d[...])
            wext[pl.ds(r0, BAND), :] = weight * (y[:, :E] + y[:, E:])

        @pl.when(has_l)
        def _():
            wcopy_l(it).start()

        @pl.when(has_r)
        def _():
            wcopy_r(it).start()

    def reg_end(it):
        a[...] = ag[it + 1] + wext[BAND:BAND + cols, :]

        @pl.when(has_l)
        def _():
            wcopy_r(it).wait_recv()

        @pl.when(has_r)
        def _():
            wcopy_l(it).wait_recv()

        a[0:BAND, :] += wr[it, 0]
        a[cols - BAND:cols, :] += wr[it, 1]

    def reg_done(it):
        @pl.when(has_l)
        def _():
            wcopy_l(it).wait_send()

        @pl.when(has_r)
        def _():
            wcopy_r(it).wait_send()

    def ccopy(it):
        return rcopy(scs.at[it], scp.at[it], pair(sem_c, it), at(obs, partner))

    def scopy(it, k, slot):
        return rcopy(scz.at[it], scr.at[it, slot], pair(sem_s, it), zat(k))

    def sall(it):
        block = scr.at[it, pl.ds(0, nz - 1)]
        return rcopy(block, block, pair(sem_s, it), at(obs, partner))

    def tcopy(it):
        return rcopy(tots.at[it], tots.at[it], pair(sem_t, it), at(obs, partner))

    def sums_mid(it):
        @pl.when(c == 1)
        def _():
            ccopy(it).wait_recv()
            both = scs[it] + scp[it]
            scz[it] = both
            scr[it, z] = both

            @pl.loop(1, nz)
            def _(k):
                scopy(it, k, z).start()

    def sums_end(it):
        @pl.when(c == 1)
        def _():
            sall(it).wait_recv()
            tots[it] = jnp.sum(scr[it], axis=0)
            tcopy(it).start()

        @pl.when(c == 0)
        def _():
            tcopy(it).wait_recv()

        return tots[it]

    def sums_done(it):
        @pl.when(c == 0)
        def _():
            ccopy(it).wait_send()

        @pl.when(c == 1)
        def _():
            sall(it).wait_send()
            tcopy(it).wait_send()

    def pcopy(q, slot):
        return rcopy(pls, plr.at[slot], pair(sem_p), at(obs, q))

    def qcopy(o, core, slot):
        return rcopy(qls, qlr.at[slot], pair(sem_q), at(o, 2 * z + core))

    def rows_of(sem, n):
        block = plr.at[pl.ds(0, n)]
        return rcopy(block, block, pair(sem), at(obs, partner))

    def rowsum(x):
        return jnp.sum(x, axis=0, keepdims=True)

    norms, regs = [], []
    updates = []

    def dots(it):
        gv, dv, av = g[...], d[...], a[...]
        scs[it, 0:1, :] = rowsum(gv * gv)
        scs[it, 1:2, :] = rowsum(dv * av)
        scs[it, 2:3, :] = rowsum(gv * av)
        scs[it, 3:4, :] = rowsum(av * av)
        @pl.when(c == 0)
        def _():
            ccopy(it).start()

    def first():
        return None

    def halo_update(it, scalars):
        halo_wait(it)
        if it == 0:
            hg[...] = hal[0]
            hd[...] = hal[0]
        else:
            step, ratio = scalars
            hg[...] = hg[...] - step * hal[it]
            hd[...] = hg[...] + ratio * hd[...]

    def advance(it):
        tot = sums_end(it - 1)
        if it == 1:
            norms.append(tot[0:1])
        norm = norms[-1]
        step = norm / tot[1:2]
        after = norm - 2.0 * step * tot[2:3] + step * step * tot[3:4]
        ratio = after / norm
        norms.append(after)
        if it == 1:
            slip[...] = step * d[...]
        else:
            slip[...] += step * d[...]
        g[...] = g[...] - step * a[...]
        d[...] = g[...] + ratio * d[...]
        if it == ITERS - 1:
            halo_update(it, (step, ratio))
            laplace()

            _, u = lap_rows(jnp.minimum(obs, CB - 1))
            regs.append(jnp.where(obs < CB, rowsum(u * u), 0.0))
            for k, (src, dst) in enumerate(((slip, slip_h), (d, d_h))):
                pltpu.make_async_copy(src, dst, sem_o.at[k]).start()
        return step, ratio

    backward(0, build_laplace)
    g[...] = ag[0]
    d[...] = ag[0]
    forward(0, first)
    for it in range(1, ITERS):
        backward_end(it - 1)
        backward(it, functools.partial(reg_start, it - 1))
        forward_end(it - 1)
        reg_end(it - 1)
        sq = forward(it, functools.partial(advance, it))
        reg_done(it - 1)
    last = ITERS - 1
    norm = norms[-1]
    sq = sq + regs[0]
    pls[...] = sq

    @pl.loop(c, nz)
    def _(k):
        pcopy((z + k) % nz * 2 + 1, pat).start()

    forward_end(last)
    backward_end(last)
    for it in range(ITERS - 1):
        sums_done(it)

    @pl.when(c == 1)
    def _():
        plr[pat] = sq

        rows_of(sem_p, n_patch - 1).wait_recv()

    @pl.when(c == 1)
    def _():
        line = jnp.sum(plr[...], axis=0)
        qls[...] = line
        qlr[obs] = line
        for i, j in far_first:
            for core in range(2):
                qcopy(shifted(i, j), core, obs).start()
        qcopy(obs, 0, obs).start()

    for core in range(2):
        @pl.when(c == core)
        def _():
            rows_of(sem_p, nz - core).wait_send()

    for k, (src, dst) in enumerate(((slip, slip_h), (d, d_h))):
        pltpu.make_async_copy(src, dst, sem_o.at[k]).wait()

    for core in range(2):
        @pl.when(c == core)
        def _():
            rows_of(sem_q, n_obs - core).wait_recv()

    scale[...] = norm / jnp.sum(qlr[...], axis=0)

    @pl.when(c == 1)
    def _():
        rows_of(sem_q, 2 * n_obs - 1).wait_send()


def shards(green, data, neighbours, reg_weight):
    rows, cols = green.shape
    E = data.shape[1]
    n_obs, n_patch = lax.axis_size("obs"), lax.axis_size("patch")
    nz = n_patch // 2
    nd = 2
    R, BR, ext = rows // 2 // nz, cols // n_obs, cols + 2 * BAND
    first = 4 * (nz // 4) - 3
    V = pltpu.VMEM
    D = pltpu.SemaphoreType.DMA
    scratch = [
        V((rows, cols), F32), V((rows, E), F32), V((rows, E), F32), V(neighbours.shape, jnp.int32), V((1, E), F32),
        V((rows, cols), BF16), V((rows, cols), BF16),
        V((cols, rows), BF16), V((cols, rows), BF16),
        V((cols, ext), BF16), V((ext, cols), BF16),
        V((cols, 2 * E), BF16), V((rows, 2 * E), BF16), V((ext, 2 * E), BF16),
        V((cols, E), F32), V((cols, E), F32), V((cols, E), F32), V((ext, E), F32), V((cols, E), F32),
        V((2, BAND, E), F32), V((2, BAND, E), F32), V((R, E), F32), V((R, E), F32),
        V((nz, R, E), F32), V((nz, R, E), F32), V((ITERS, nd, nz // nd, R, E), F32),
        V((ITERS, first, R, E), F32), V((2, R, E), F32), V((ITERS, 2, R, E), F32),
        V((ITERS - 1, 2, nz, R, E), F32),
        V((ITERS, n_obs, BR, E), F32), V((ITERS, n_obs, BR, E), F32), V((ITERS, cols, E), F32),
        V((ITERS, 2, BAND, E), F32), V((ITERS - 1, 2, BAND, E), F32),
        V((ITERS - 1, 4, E), F32), V((ITERS - 1, 4, E), F32), V((ITERS - 1, 4, E), F32), V((ITERS - 1, nz, 4, E), F32), V((ITERS - 1, 4, E), F32),
        V((1, E), F32), V((n_patch, 1, E), F32), V((1, E), F32), V((n_obs, 1, E), F32),
        D((2, rows // (2 * BAND) + 1)), D((2,)),
        D((2, nd)), D((4,)), D((2,)), D((nz - nz // 2 + 3,)), D((3,)),
        D((2,)), D((2,)), D((2, ITERS, 2)), D((2, ITERS - 1, 2)),
        D((2, ITERS - 1)), D((2, ITERS - 1)), D((2, ITERS - 1)), D((2,)), D((2,)), pltpu.SemaphoreType.REGULAR((2,)),
    ]
    anywhere = pl.BlockSpec(memory_space=pl.ANY)
    slip, d, scale = pl.pallas_call(
        functools.partial(kernel, n_obs, n_patch),
        out_shape=[jax.ShapeDtypeStruct((cols, E), F32)] * 2 + [jax.ShapeDtypeStruct((1, E), F32)],
        in_specs=[anywhere] * 4,
        out_specs=[anywhere, anywhere, pl.BlockSpec(memory_space=pltpu.VMEM)],
        scratch_shapes=scratch,
        compiler_params=pltpu.CompilerParams(
            collective_id=0, has_side_effects=True, vmem_limit_bytes=56 * 1024 * 1024),
    )(green, data, neighbours, reg_weight.reshape(1, E))
    return slip + scale * d


def solution(mesh):
    in_specs = (P("obs", "patch"), P("obs", None), P(None, "patch"), P())
    return jax.shard_map(shards, mesh=mesh, in_specs=in_specs, out_specs=P("patch", None), check_vma=False)
```

```python
import functools
import math

import jax
import jax.numpy as jnp
from jax import lax
from jax.experimental import pallas as pl
from jax.experimental.pallas import tpu as pltpu
from jax.sharding import PartitionSpec as P

BAND = 128
ITERS = 3
MESH = pl.DeviceIdType.MESH
F32 = jnp.float32
BF16 = jnp.bfloat16


def dot(a, b):
    return lax.dot_general(a, b, (((1,), (0,)), ((), ())), preferred_element_type=F32)


def split(x):
    hi = x.astype(BF16)
    return hi, (x - hi.astype(F32)).astype(BF16)


def kernel(n_obs, n_patch, green_h, data_h, nb_h, rw_h, slip_h, d_h, scale,
           green, data, line_up, nb, rw,
           ghi, glo, gthi, gtlo, lm, lmt, cat_d, cat_r, cat_e,
           d, g, a, wext, slip, hd, hg, qd, qg,
           pf, s, rd, zr, zrel, zfin, img, bs, br, ag, hal, wr, scs, scp, scz, scr, tots, pls, plr, qls, qlr,
           sem_l, sem_o, sem_d, sem_z, sem_f, sem_g, sem_i, sem_b, sem_a, sem_h, sem_w, sem_c, sem_s, sem_t, sem_p, sem_q, go):
    rows, cols = green.shape
    E = data.shape[1]
    nz = n_patch // 2
    R = rows // 2 // nz
    BR = cols // n_obs
    half = rows // 2
    per = nch = math.isqrt(n_obs)
    CB = cols // BAND
    Q = nz // 4
    plus = list(range(1, Q + 1))
    minus = list(range(1, Q))
    near = [0] + [sgn * k for k in minus for sgn in (1, -1)] + [Q]
    far = [2 * Q] + [sgn * k for k in range(2 * Q - 1, Q, -1) for sgn in (1, -1)] + [-Q]
    pieces = near + far
    NP = len(near)
    quarter = half // 2

    def wrapped(o):
        return (o + 2 * Q - 1) % nz - 2 * Q + 1

    def idx(o):
        return pieces.index(wrapped(o))
    obs = lax.axis_index("obs")
    pat = lax.axis_index("patch")
    z = pat // 2
    c = pat % 2
    other = 1 - c
    partner = z * 2 + other
    has_l, has_r = pat > 0, pat < n_patch - 1

    def at(o, q):
        return (o, q)

    def rcopy(src, dst, sems, dev):
        return pltpu.make_async_remote_copy(
            src_ref=src, dst_ref=dst, send_sem=sems[0], recv_sem=sems[1],
            device_id=dev, device_id_type=MESH)

    def pair(sem, *idx):
        return sem.at[(0,) + idx], sem.at[(1,) + idx]

    STEP = 2 * BAND
    ends = [-(-(r0 + STEP) // R) for r0 in range(0, rows, STEP)]

    def load(n):
        part, h, r = n // (2 * NP), n // NP % 2, n % NP
        o = pieces[part * NP + r]
        src = pl.multiple_of(h * half + (z + (1 - 2 * h) * o + nz) % nz * R, R)
        return src, pltpu.make_async_copy(green_h.at[pl.ds(src, R)], green.at[pl.ds(n * R, R)],
                                          sem_l.at[0, sum(n >= e for e in ends)])

    small = [pltpu.make_async_copy(src, dst, sem_l.at[i, len(ends)])
             for i, (src, dst) in enumerate(((nb_h, nb), (rw_h, rw)))]
    fields = pltpu.make_async_copy(data_h, data, sem_l.at[1, 0])
    barrier = pltpu.get_barrier_semaphore()

    def greet(o, q):
        pl.semaphore_signal(barrier, inc=1, device_id=at(o, q), device_id_type=MESH)

    def tell(k):
        pl.semaphore_signal(go.at[k], inc=1, device_id=at(obs, partner), device_id_type=MESH)

    def plane_entered():
        @pl.when(c == 0)
        def _():
            pl.semaphore_wait(barrier, 2 * n_obs - 1)
            tell(0)

        @pl.when(c == 1)
        def _():
            pl.semaphore_wait(go.at[0], 1)

    def line_entered():
        @pl.when(c == 1)
        def _():
            pl.semaphore_wait(barrier, n_patch - 1)
            tell(1)

        @pl.when(c == 0)
        def _():
            pl.semaphore_wait(go.at[1], 1)

    for n in range(2 * nz):
        load(n)[1].start()
        if n == nz // 4:
            fields.start()

    for copy in small:
        copy.start()

    greet(obs, partner)

    @pl.loop(1, n_obs)
    def _(i):
        greet((obs + i) % n_obs, z * 2)

    @pl.loop(1, nz)
    def _(k):
        greet(obs, (z + k) % nz * 2 + 1)

    def put_cat(where, value):
        hi, lo = split(value)
        cat_r[where, 0:E] = hi
        cat_r[where, E:2 * E] = lo

    def product(m0, m1, k0, k1):
        y = dot(gthi[m0:m1, k0:k1], cat_r[k0:k1, :])
        y = y[:, :E] + y[:, E:] + dot(gtlo[m0:m1, k0:k1], cat_r[k0:k1, 0:E])
        return y.reshape((m1 - m0) // BR, BR, E)

    def first_product(r0):
        y = product(0, cols, r0, r0 + STEP)
        if r0 == 0:
            bs[0] = y
        else:
            bs[0] += y

    loaded = 0
    for n, r0 in enumerate(range(0, rows, STEP)):
        span = pl.ds(loaded * R, (ends[n] - loaded) * R)
        pltpu.make_async_copy(green_h.at[span], green.at[span], sem_l.at[0, n]).wait()
        if n == 0:
            fields.wait()
        for m in range(loaded, ends[n]):
            line_up[m * R:(m + 1) * R, :] = data[pl.ds(load(m)[0], R), :]
        loaded = ends[n]
        if r0:
            first_product(r0 - STEP)
        for r in range(r0, r0 + STEP, BAND):
            block = green[r:r + BAND, :]
            hi, lo = split(block)
            ghi[r:r + BAND, :] = hi
            glo[r:r + BAND, :] = lo
            hi, lo = split(block.T)
            gthi[:, r:r + BAND] = hi
            gtlo[:, r:r + BAND] = lo
            put_cat(slice(r, r + BAND), line_up[r:r + BAND, :])

    first_product(rows - STEP)

    for copy in small:
        copy.wait()
    weight = rw[...]

    zero_h = jnp.zeros((BAND, E), F32)

    @pl.when(pat == 0)
    def _():
        for it in range(ITERS):
            hal[it, 0] = zero_h
        for it in range(ITERS - 1):
            wr[it, 0] = zero_h

    @pl.when(pat == n_patch - 1)
    def _():
        for it in range(ITERS):
            hal[it, 1] = zero_h
        for it in range(ITERS - 1):
            wr[it, 1] = zero_h

    def build_laplace():
        @pl.loop(0, CB + 2)
        def _(j):
            r0 = pl.multiple_of(j * BAND, BAND)
            col = lax.broadcasted_iota(jnp.int32, (BAND, cols), 0) + j * BAND
            own = lax.broadcasted_iota(jnp.int32, (BAND, cols), 1) + BAND
            m = jnp.where(col == own, 4.0, 0.0)
            col = col + (pat * cols - BAND)
            for k in range(3):
                m = m - jnp.where(col == nb[k:k + 1, :], 1.0, 0.0)
            lmt[pl.ds(r0, BAND), :] = m.astype(BF16)
            lm[:, pl.ds(r0, BAND)] = m.T.astype(BF16)

    side = math.isqrt(n_obs)
    steps = sorted(range(side), key=lambda k: -min(k, side - k))
    far_first = sorted([(i, j) for i in steps for j in steps if i or j],
                       key=lambda ij: -sum(min(k, side - k) for k in ij))

    def shifted(i, j):
        return (obs // side + (1 - 2 * c) * i + side) % side * side + (obs + (1 - 2 * c) * j + side) % side

    def crossed(i, j):
        return shifted(i + c * (j - i), j + c * (i - j))

    def bcopy(b, o, slot):
        return rcopy(bs.at[b, o], br.at[b, slot], pair(sem_b), at(o, pat))

    def ball(b):
        return rcopy(bs.at[b, pl.ds(0, n_obs - 1)], br.at[b, pl.ds(0, n_obs - 1)], pair(sem_b), at(obs, partner))

    def acopy(b, o, slot):
        piece = ag.at[b, pl.ds(pl.multiple_of(slot * BR, BR), BR)]
        return rcopy(piece, piece, pair(sem_a), at(o, pat))

    def aall(b):
        block = ag.at[b, pl.ds(0, (n_obs - 1) * BR)]
        return rcopy(block, block, pair(sem_a), at(obs, partner))

    def backward(b, hook):
        if b == 0:
            plane_entered()

            for i, j in far_first:
                bcopy(b, crossed(i, j), obs).start()
        else:
            for i in range(NP, nz - 1):
                gall(b - 1, i, 1).wait_recv()
                icopy(b - 1, i).start()

            icopy(b - 1, NP, NP).wait_recv()

            for h in range(2):
                put_cat(slice(half + h * quarter, half + (h + 1) * quarter), img[b - 1, h, NP:].reshape(quarter, E))
            for i in steps:
                ch = (obs // side + (1 - 2 * c) * i + side) % side
                r0 = pl.multiple_of(ch * (per * BR), per * BR)
                y = dot(gthi[pl.ds(r0, per * BR), half:], cat_r[half:, :])
                y = y[:, :E] + y[:, E:] + dot(gtlo[pl.ds(r0, per * BR), half:], cat_r[half:, 0:E])
                bs[b, pl.ds(ch * per, per)] += y.reshape(per, BR, E)
                for j in steps:
                    if i or j:
                        bcopy(b, shifted(i, j), obs).start()

        if b:
            updates.pop()()
        hook()

        ball(b).wait_recv()
        total = lax.fori_loop(1, n_obs, lambda i, acc: acc + br[b, (obs + i) % n_obs], bs[b, obs])
        ag[b, pl.ds(pl.multiple_of(obs * BR, BR), BR), :] = total

        for i, j in far_first:
            acopy(b, crossed(i, j), obs).start()

        if b == 0:
            line_entered()

        aall(b).wait_recv()

    def backward_end(b):
        ball(b).wait_send()
        aall(b).wait_send()

    def dcopy(it, k):
        return rcopy(pf.at[pl.ds(k * NP, NP)], rd.at[it, k], pair(sem_d, k), at(obs, partner))

    turn = 1 - 2 * c

    def zat(k):
        return at(obs, ((z + turn * k + nz) % nz) * 2 + c)

    W = Q + 1
    first_step = ([(-k, -k - W) for k in reversed(minus)] + [(1, -Q)] + [(k, k + W) for k in reversed(minus[:-1])] + [(-1, Q)]
                  + [(-k, -k) for k in reversed(minus)] + [(k, k) for k in reversed(minus)])
    n_plus, n_minus = len(plus), len(minus)

    groups = [(0, n_plus), (n_plus, n_minus), (n_plus + n_minus, len(first_step) - n_plus - n_minus)]

    def zcopy(it, slot):
        k, o = first_step[slot]
        group = sum(slot >= first for first, _ in groups)
        return rcopy(s.at[idx(o)], zr.at[it, slot], (sem_z.at[0], sem_z.at[group]), zat(k))

    def zall(it, group, first, n):
        block = zr.at[it, pl.ds(first, n)]
        return rcopy(block, block, (sem_z.at[0], sem_z.at[group]), at(obs, partner))

    def fcopy(it, slot):
        return rcopy(zrel.at[slot], zfin.at[it, slot], pair(sem_f), zat(-W if slot == 0 else W))

    def fall(it):
        return rcopy(zrel, zfin.at[it], pair(sem_f), at(obs, partner))

    gather = ([(k, 0) for k in (-Q, Q)] + [(sgn * k, 0) for k in reversed(minus) for sgn in (1, -1)]
              + [(k, -Q) for k in reversed(plus)] + [(-k, Q) for k in reversed(minus)])
    n_own = 2 * Q

    def arrival(it, i):
        return sem_g.at[1 if 0 < i < NP - 1 else i - NP + 3]

    def gcopy(it, m):
        k, o = gather[m]
        to = idx(o - k)
        return rcopy(img.at[it, c, idx(o)], img.at[it, c, to], (sem_g.at[0], arrival(it, to)), zat(k))

    def gall(it, i, n):
        block = img.at[it, c, pl.ds(i, n)]
        return rcopy(block, block, (sem_g.at[0], arrival(it, i)), at(obs, partner))

    def icopy(it, i, n=1):
        block = img.at[it, c, pl.ds(i, n)]
        return rcopy(block, block, (sem_i.at[0], sem_i.at[1 + i // NP]), at(obs, partner))

    def fold(acc, it, group):
        first, n = groups[group]
        zall(it, group + 1, first, n).wait_recv()
        for slot in range(first, first + n):
            acc = acc + zr[it, slot]
        return acc

    def hsrc(it):
        return a if it else ag.at[0]

    def hcopy_r(it):
        return rcopy(hsrc(it).at[pl.ds(cols - BAND, BAND)], hal.at[it, 0], pair(sem_h, it, 0), at(obs, pat + 1))

    def hcopy_l(it):
        return rcopy(hsrc(it).at[pl.ds(0, BAND)], hal.at[it, 1], pair(sem_h, it, 1), at(obs, pat - 1))

    def forward(it, hook):
        last = it == ITERS - 1

        hi, lo = split(hsrc(it)[...])
        cat_d[:, 0:E] = hi
        cat_d[:, E:2 * E] = lo

        def part(h, k):
            r0 = pl.multiple_of(k * half + h * quarter, quarter)
            y = dot(ghi[pl.ds(r0, quarter), :], cat_d[...])
            y = y[:, :E] + y[:, E:] + dot(glo[pl.ds(r0, quarter), :], cat_d[:, 0:E])
            return y.reshape(NP, R, E)

        for k in (1, 0):
            pf[k * NP:(k + 1) * NP] = part(other, k)
            dcopy(it, k).start()

        if it:
            dots(it - 1)

        for k in (1, 0):
            s[k * NP:(k + 1) * NP] = part(c, k)

        dcopy(it, 1).wait_recv()
        s[NP:] += rd[it, 1]
        for slot in range(n_plus + n_minus - 1):
            zcopy(it, slot).start()
        dcopy(it, 0).wait_recv()
        s[:NP] += rd[it, 0]
        zcopy(it, n_plus + n_minus - 1).start()

        if it:
            sums_mid(it - 1)

        def halos():
            @pl.when(has_r)
            def _():
                hcopy_r(it).start()

            @pl.when(has_l)
            def _():
                hcopy_l(it).start()

        if last:
            halos()

        direct = range(n_plus + n_minus, len(first_step))
        for slot in direct:
            if abs(first_step[slot][0]) > 1:
                zcopy(it, slot).start()

        zrel[1] = fold(s[idx(W)], it, 1)
        fcopy(it, 1).start()
        zrel[0] = fold(s[idx(-W)], it, 0)
        fcopy(it, 0).start()

        for slot in direct:
            if abs(first_step[slot][0]) == 1:
                zcopy(it, slot).start()


        scalars = hook()

        total = fold(s[idx(0)], it, 2)
        fall(it).wait_recv()
        total = total + zfin[it, 0] + zfin[it, 1]

        if it:
            step, ratio = scalars
            rest = qg[...] - step * total
            total = rest + ratio * qd[...]
        else:
            rest = total

        if last:
            sq = jnp.sum(total * total, axis=0, keepdims=True)
        else:
            sq = None
            qg[...] = rest
            qd[...] = total
            img[it, c, idx(0)] = total
            for m in range(n_own):
                gcopy(it, m).start()
            icopy(it, 0).start()
            gall(it, idx(-Q), 1).wait_recv()
            for m in range(n_own, n_own + Q):
                gcopy(it, m).start()
            gall(it, idx(Q), 1).wait_recv()
            for m in range(n_own + Q, len(gather)):
                gcopy(it, m).start()
            halos()
            icopy(it, idx(Q)).start()
            icopy(it, idx(-Q)).start()
            gall(it, 1, NP - 2).wait_recv()
            icopy(it, 1, NP - 2).start()

            icopy(it, 0, NP).wait_recv()
            for h in range(2):
                put_cat(slice(h * quarter, (h + 1) * quarter), img[it, h, :NP].reshape(quarter, E))

            @pl.loop(0, nch)
            def _(ch):
                r0 = pl.multiple_of(ch * (per * BR), per * BR)
                y = dot(gthi[pl.ds(r0, per * BR), :half], cat_r[:half, :])
                y = y[:, :E] + y[:, E:] + dot(gtlo[pl.ds(r0, per * BR), :half], cat_r[:half, 0:E])
                bs[it + 1, pl.ds(ch * per, per)] = y.reshape(per, BR, E)

            updates.append(functools.partial(halo_update, it, scalars))

        return sq

    def forward_end(it):
        for k in range(2):
            dcopy(it, k).wait_send()
        zall(it, 1, 0, len(first_step)).wait_send()
        fall(it).wait_send()
        if it < ITERS - 1:
            gall(it, 0, nz - 1).wait_send()
            icopy(it, 0, nz).wait_send()

    def halo_wait(it):
        @pl.when(has_l)
        def _():
            hcopy_r(it).wait_recv()

        @pl.when(has_r)
        def _():
            hcopy_l(it).wait_recv()

        @pl.when(has_r)
        def _():
            hcopy_r(it).wait_send()

        @pl.when(has_l)
        def _():
            hcopy_l(it).wait_send()

    def laplace():
        for r0, n, v in ((0, BAND, hd[0]), (BAND, cols, d[...]), (BAND + cols, BAND, hd[1])):
            hi, lo = split(v)
            cat_e[r0:r0 + n, 0:E] = hi
            cat_e[r0:r0 + n, E:2 * E] = lo

    def lap_rows(i):
        r0 = pl.multiple_of(i * BAND, BAND)
        y = dot(lm[pl.ds(r0, BAND), :], cat_e[...])
        return r0, weight * (y[:, :E] + y[:, E:])

    def wcopy_l(it):
        return rcopy(wext.at[pl.ds(0, BAND)], wr.at[it, 1], pair(sem_w, it, 1), at(obs, pat - 1))

    def wcopy_r(it):
        return rcopy(wext.at[pl.ds(BAND + cols, BAND)], wr.at[it, 0], pair(sem_w, it, 0), at(obs, pat + 1))

    def reg_start(it):
        laplace()

        @pl.loop(0, CB)
        def _(i):
            r0, u = lap_rows(i)
            hi, lo = split(u)
            cat_d[pl.ds(r0, BAND), 0:E] = hi
            cat_d[pl.ds(r0, BAND), E:2 * E] = lo

        @pl.loop(0, CB + 2)
        def _(i):
            r0 = pl.multiple_of(i * BAND, BAND)
            y = dot(lmt[pl.ds(r0, BAND), :], cat_d[...])
            wext[pl.ds(r0, BAND), :] = weight * (y[:, :E] + y[:, E:])

        @pl.when(has_l)
        def _():
            wcopy_l(it).start()

        @pl.when(has_r)
        def _():
            wcopy_r(it).start()

    def reg_end(it):
        a[...] = ag[it + 1] + wext[BAND:BAND + cols, :]

        @pl.when(has_l)
        def _():
            wcopy_r(it).wait_recv()

        @pl.when(has_r)
        def _():
            wcopy_l(it).wait_recv()

        a[0:BAND, :] += wr[it, 0]
        a[cols - BAND:cols, :] += wr[it, 1]

    def reg_done(it):
        @pl.when(has_l)
        def _():
            wcopy_l(it).wait_send()

        @pl.when(has_r)
        def _():
            wcopy_r(it).wait_send()

    def ccopy(it):
        return rcopy(scs.at[it], scp.at[it], pair(sem_c, it), at(obs, partner))

    def scopy(it, k, slot):
        return rcopy(scz.at[it], scr.at[it, slot], pair(sem_s, it), zat(k))

    def sall(it):
        block = scr.at[it, pl.ds(0, nz - 1)]
        return rcopy(block, block, pair(sem_s, it), at(obs, partner))

    def tcopy(it):
        return rcopy(tots.at[it], tots.at[it], pair(sem_t, it), at(obs, partner))

    def sums_mid(it):
        @pl.when(c == 1)
        def _():
            ccopy(it).wait_recv()
            both = scs[it] + scp[it]
            scz[it] = both
            scr[it, z] = both

            @pl.loop(1, nz)
            def _(k):
                scopy(it, k, z).start()

    def sums_end(it):
        @pl.when(c == 1)
        def _():
            sall(it).wait_recv()
            tots[it] = jnp.sum(scr[it], axis=0)
            tcopy(it).start()

        @pl.when(c == 0)
        def _():
            tcopy(it).wait_recv()

        return tots[it]

    def sums_done(it):
        @pl.when(c == 0)
        def _():
            ccopy(it).wait_send()

        @pl.when(c == 1)
        def _():
            sall(it).wait_send()
            tcopy(it).wait_send()

    def pcopy(q, slot):
        return rcopy(pls, plr.at[slot], pair(sem_p), at(obs, q))

    def qcopy(o, core, slot):
        return rcopy(qls, qlr.at[slot], pair(sem_q), at(o, 2 * z + core))

    def rows_of(sem, n):
        block = plr.at[pl.ds(0, n)]
        return rcopy(block, block, pair(sem), at(obs, partner))

    def rowsum(x):
        return jnp.sum(x, axis=0, keepdims=True)

    norms, regs = [], []
    updates = []

    def dots(it):
        gv, dv, av = g[...], d[...], a[...]
        scs[it, 0:1, :] = rowsum(gv * gv)
        scs[it, 1:2, :] = rowsum(dv * av)
        scs[it, 2:3, :] = rowsum(gv * av)
        scs[it, 3:4, :] = rowsum(av * av)
        @pl.when(c == 0)
        def _():
            ccopy(it).start()

    def first():
        return None

    def halo_update(it, scalars):
        halo_wait(it)
        if it == 0:
            hg[...] = hal[0]
            hd[...] = hal[0]
        else:
            step, ratio = scalars
            hg[...] = hg[...] - step * hal[it]
            hd[...] = hg[...] + ratio * hd[...]

    def advance(it):
        tot = sums_end(it - 1)
        if it == 1:
            norms.append(tot[0:1])
        norm = norms[-1]
        step = norm / tot[1:2]
        after = norm - 2.0 * step * tot[2:3] + step * step * tot[3:4]
        ratio = after / norm
        norms.append(after)
        if it == 1:
            slip[...] = step * d[...]
        else:
            slip[...] += step * d[...]
        g[...] = g[...] - step * a[...]
        d[...] = g[...] + ratio * d[...]
        if it == ITERS - 1:
            halo_update(it, (step, ratio))
            laplace()

            _, u = lap_rows(jnp.minimum(obs, CB - 1))
            regs.append(jnp.where(obs < CB, rowsum(u * u), 0.0))
            for k, (src, dst) in enumerate(((slip, slip_h), (d, d_h))):
                pltpu.make_async_copy(src, dst, sem_o.at[k]).start()
        return step, ratio

    backward(0, build_laplace)
    g[...] = ag[0]
    d[...] = ag[0]
    forward(0, first)
    for it in range(1, ITERS):
        backward_end(it - 1)
        backward(it, functools.partial(reg_start, it - 1))
        forward_end(it - 1)
        reg_end(it - 1)
        sq = forward(it, functools.partial(advance, it))
        reg_done(it - 1)
    last = ITERS - 1
    norm = norms[-1]
    sq = sq + regs[0]
    pls[...] = sq

    @pl.loop(0, nz - c)
    def _(k):
        pcopy((z + (nz // 2 + k + c * (k // (nz // 2))) % nz) % nz * 2 + 1, pat).start()

    forward_end(last)
    backward_end(last)
    for it in range(ITERS - 1):
        sums_done(it)

    @pl.when(c == 1)
    def _():
        plr[pat] = sq

        rows_of(sem_p, n_patch - 1).wait_recv()

    @pl.when(c == 1)
    def _():
        line = jnp.sum(plr[...], axis=0)
        qls[...] = line
        qlr[obs] = line
        for i, j in far_first:
            for core in range(2):
                qcopy(shifted(i, j), core, obs).start()
        qcopy(obs, 0, obs).start()

    for core in range(2):
        @pl.when(c == core)
        def _():
            rows_of(sem_p, nz - core).wait_send()

    for k, (src, dst) in enumerate(((slip, slip_h), (d, d_h))):
        pltpu.make_async_copy(src, dst, sem_o.at[k]).wait()

    for core in range(2):
        @pl.when(c == core)
        def _():
            rows_of(sem_q, n_obs - core).wait_recv()

    scale[...] = norm / jnp.sum(qlr[...], axis=0)

    @pl.when(c == 1)
    def _():
        rows_of(sem_q, 2 * n_obs - 1).wait_send()


def shards(green, data, neighbours, reg_weight):
    rows, cols = green.shape
    E = data.shape[1]
    n_obs, n_patch = lax.axis_size("obs"), lax.axis_size("patch")
    nz = n_patch // 2
    nd = 2
    R, BR, ext = rows // 2 // nz, cols // n_obs, cols + 2 * BAND
    first = 4 * (nz // 4) - 3
    V = pltpu.VMEM
    D = pltpu.SemaphoreType.DMA
    scratch = [
        V((rows, cols), F32), V((rows, E), F32), V((rows, E), F32), V(neighbours.shape, jnp.int32), V((1, E), F32),
        V((rows, cols), BF16), V((rows, cols), BF16),
        V((cols, rows), BF16), V((cols, rows), BF16),
        V((cols, ext), BF16), V((ext, cols), BF16),
        V((cols, 2 * E), BF16), V((rows, 2 * E), BF16), V((ext, 2 * E), BF16),
        V((cols, E), F32), V((cols, E), F32), V((cols, E), F32), V((ext, E), F32), V((cols, E), F32),
        V((2, BAND, E), F32), V((2, BAND, E), F32), V((R, E), F32), V((R, E), F32),
        V((nz, R, E), F32), V((nz, R, E), F32), V((ITERS, nd, nz // nd, R, E), F32),
        V((ITERS, first, R, E), F32), V((2, R, E), F32), V((ITERS, 2, R, E), F32),
        V((ITERS - 1, 2, nz, R, E), F32),
        V((ITERS, n_obs, BR, E), F32), V((ITERS, n_obs, BR, E), F32), V((ITERS, cols, E), F32),
        V((ITERS, 2, BAND, E), F32), V((ITERS - 1, 2, BAND, E), F32),
        V((ITERS - 1, 4, E), F32), V((ITERS - 1, 4, E), F32), V((ITERS - 1, 4, E), F32), V((ITERS - 1, nz, 4, E), F32), V((ITERS - 1, 4, E), F32),
        V((1, E), F32), V((n_patch, 1, E), F32), V((1, E), F32), V((n_obs, 1, E), F32),
        D((2, rows // (2 * BAND) + 1)), D((2,)),
        D((2, nd)), D((4,)), D((2,)), D((nz - nz // 2 + 3,)), D((3,)),
        D((2,)), D((2,)), D((2, ITERS, 2)), D((2, ITERS - 1, 2)),
        D((2, ITERS - 1)), D((2, ITERS - 1)), D((2, ITERS - 1)), D((2,)), D((2,)), pltpu.SemaphoreType.REGULAR((2,)),
    ]
    anywhere = pl.BlockSpec(memory_space=pl.ANY)
    slip, d, scale = pl.pallas_call(
        functools.partial(kernel, n_obs, n_patch),
        out_shape=[jax.ShapeDtypeStruct((cols, E), F32)] * 2 + [jax.ShapeDtypeStruct((1, E), F32)],
        in_specs=[anywhere] * 4,
        out_specs=[anywhere, anywhere, pl.BlockSpec(memory_space=pltpu.VMEM)],
        scratch_shapes=scratch,
        compiler_params=pltpu.CompilerParams(
            collective_id=0, has_side_effects=True, vmem_limit_bytes=56 * 1024 * 1024),
    )(green, data, neighbours, reg_weight.reshape(1, E))
    return slip + scale * d


def solution(mesh):
    in_specs = (P("obs", "patch"), P("obs", None), P(None, "patch"), P())
    return jax.shard_map(shards, mesh=mesh, in_specs=in_specs, out_specs=P("patch", None), check_vma=False)
```
